8 devices in a mesh: dp: 1 (over z), kv: 8 (over y, x, core).
Axes of the slice: x: 2, y: 2, z: 1, core: 2. Of those that a mesh axis runs over, the one named last changes fastest.
Arguments:
- x_in: bfloat16 [512, 1152], P('dp')
- positions: int32 [512], P('dp')
- k_cache: bfloat16 [512, 512, 256], P('dp', 'kv')
- v_cache: bfloat16 [512, 512, 256], P('dp', 'kv')
- slot_pos: int32 [512, 512], P('dp', 'kv')
- norm_scale: bfloat16 [1152], replicated
- w_q: bfloat16 [1152, 1024], replicated
- w_k: bfloat16 [1152, 256], replicated
- w_v: bfloat16 [1152, 256], replicated
- w_o: bfloat16 [1024, 1152], replicated
- b_o: bfloat16 [1152], replicated
Outputs:
- output 1: bfloat16 [512, 1152], P('dp')
- output 2: bfloat16 [512, 512, 256], P('dp', 'kv')
- output 3: bfloat16 [512, 512, 256], P('dp', 'kv')
- output 4: int32 [512, 512], P('dp', 'kv')
All inputs are finite; a program needn't handle non-finite values.
Results may differ from the reference program's by a relative error of at most 0.00589974.
Values sent between devices are 32-bit elements.
A program may use at most 1 GiB of HBM per device.

```python
import math
import jax
import jax.numpy as jnp
from jax import lax

BATCH = 512
D_MODEL = 1152
HEADS = 4
WINDOW = 512
HEAD_DIM = 256
ROPE_DIM = 128
ROW_BLOCK = 8
POS_SPAN = 8
MAX_POS = POS_SPAN * WINDOW
ROPE_BASE = 10000.0
EPS = 1e-6
SCORE_SCALE = HEAD_DIM ** -0.5


def draw_positions(pos_key):
    key_young, key_old, key_bits = jax.random.split(pos_key, 3)
    row_ids = jnp.arange(BATCH)
    log_window = int(math.log2(WINDOW))
    shift_bits = jax.random.randint(key_bits, (BATCH,), 3, log_window + 1)
    young_cap = jnp.minimum(jnp.left_shift(jnp.ones((BATCH,), jnp.int32), shift_bits), WINDOW)
    young_pos = jax.random.randint(key_young, (BATCH,), 0, young_cap)
    old_pos = jax.random.randint(key_old, (BATCH,), WINDOW, MAX_POS)
    positions = jnp.where(row_ids % 2 == 0, young_pos, old_pos)
    positions = jnp.where(row_ids == 0, 0, positions)
    positions = jnp.where(row_ids == 1, MAX_POS - 1, positions)
    return positions.astype(jnp.int32)


def slot_history(positions):
    slot_index = jnp.arange(WINDOW, dtype=jnp.int32)
    last_pos = positions[:, None] - 1
    latest = last_pos - jnp.mod(last_pos - slot_index[None, :], WINDOW)
    return jnp.where(latest >= 0, latest, -1).astype(jnp.int32)


def slot_waves():
    slot_index = jnp.arange(WINDOW, dtype=jnp.float32)
    harmonic = jnp.arange(1.0, 4.0, dtype=jnp.float32)
    angles = 2.0 * math.pi * harmonic[:, None] * slot_index[None, :] / WINDOW
    return jnp.concatenate([jnp.cos(angles), jnp.sin(angles)], axis=0)


def setup_inputs(seed: int = 0, part: int = 0) -> dict:
    part_key = jax.random.fold_in(jax.random.key(seed), part)
    key_list = jax.random.split(part_key, 8)
    shared = jax.random.split(jax.random.key(seed + 1), 7)
    positions = draw_positions(key_list[0])
    slot_pos = slot_history(positions)
    wave_table = slot_waves()
    k_coeffs = jax.random.normal(key_list[1], (BATCH, 6, HEAD_DIM), jnp.float32)
    k_noise = jax.random.normal(key_list[2], (BATCH, WINDOW, HEAD_DIM), jnp.float32)
    k_cache = 0.5 * jnp.einsum('bjd,js->bsd', k_coeffs, wave_table) + 0.8 * k_noise
    v_coeffs = jax.random.normal(key_list[3], (BATCH, 6, HEAD_DIM), jnp.float32)
    v_mean = jax.random.normal(key_list[4], (BATCH, 1, HEAD_DIM), jnp.float32)
    v_noise = jax.random.normal(key_list[5], (BATCH, WINDOW, HEAD_DIM), jnp.float32)
    v_cache = 0.7 * jnp.einsum('bjd,js->bsd', v_coeffs, wave_table) + 0.3 * v_mean + 0.5 * v_noise
    x_in = jax.random.normal(key_list[6], (BATCH, D_MODEL), jnp.float32)
    q_width = HEADS * HEAD_DIM
    norm_scale = 0.3 * jax.random.normal(shared[0], (D_MODEL,), jnp.float32)
    w_q = jax.random.normal(shared[1], (D_MODEL, q_width), jnp.float32) * D_MODEL ** -0.5
    w_k = jax.random.normal(shared[2], (D_MODEL, HEAD_DIM), jnp.float32) * D_MODEL ** -0.5
    w_v = jax.random.normal(shared[3], (D_MODEL, HEAD_DIM), jnp.float32) * D_MODEL ** -0.5
    w_o = jax.random.normal(shared[4], (q_width, D_MODEL), jnp.float32) * 2.0 * q_width ** -0.5
    b_o = 0.3 * jax.random.normal(shared[5], (D_MODEL,), jnp.float32)
    return {
        'x_in': x_in.astype(jnp.bfloat16),
        'positions': positions,
        'k_cache': k_cache.astype(jnp.bfloat16),
        'v_cache': v_cache.astype(jnp.bfloat16),
        'slot_pos': slot_pos,
        'norm_scale': norm_scale.astype(jnp.bfloat16),
        'w_q': w_q.astype(jnp.bfloat16),
        'w_k': w_k.astype(jnp.bfloat16),
        'w_v': w_v.astype(jnp.bfloat16),
        'w_o': w_o.astype(jnp.bfloat16),
        'b_o': b_o.astype(jnp.bfloat16),
    }


def rms_norm(x_in, norm_scale):
    x_f32 = x_in.astype(jnp.float32)
    mean_sq = jnp.mean(x_f32 * x_f32, axis=-1, keepdims=True)
    return (x_f32 * lax.rsqrt(mean_sq + EPS) * (1.0 + norm_scale.astype(jnp.float32))).astype(jnp.bfloat16)


def rope_tables(positions):
    rope_half = ROPE_DIM // 2
    inv_freq = ROPE_BASE ** (-jnp.arange(rope_half, dtype=jnp.float32) / rope_half)
    angles = positions.astype(jnp.float32)[:, None] * inv_freq[None, :]
    return jnp.cos(angles), jnp.sin(angles)


def rotate(tensor, cos_t, sin_t):
    rope_half = ROPE_DIM // 2
    rot_first = tensor[..., :rope_half]
    rot_second = tensor[..., rope_half:ROPE_DIM]
    return jnp.concatenate([rot_first * cos_t - rot_second * sin_t, rot_second * cos_t + rot_first * sin_t, tensor[..., ROPE_DIM:]], axis=-1)


def reference(x_in, positions, k_cache, v_cache, slot_pos, norm_scale, w_q, w_k, w_v, w_o, b_o):
    normed = rms_norm(x_in, norm_scale)
    cos_t, sin_t = rope_tables(positions)
    q_full = jnp.dot(normed, w_q, preferred_element_type=jnp.float32).reshape(BATCH, HEADS, HEAD_DIM)
    q_rot = rotate(q_full, cos_t[:, None, :], sin_t[:, None, :]).astype(jnp.bfloat16)
    k_new = rotate(jnp.dot(normed, w_k, preferred_element_type=jnp.float32), cos_t, sin_t).astype(jnp.bfloat16)
    v_new = jnp.dot(normed, w_v, preferred_element_type=jnp.float32).astype(jnp.bfloat16)
    row_ids = jnp.arange(BATCH)
    slot_now = jnp.mod(positions, WINDOW)
    k_out = k_cache.at[row_ids, slot_now].set(k_new)
    v_out = v_cache.at[row_ids, slot_now].set(v_new)
    slot_pos_out = slot_pos.at[row_ids, slot_now].set(positions)
    slot_age = positions[:, None] - slot_pos_out
    usable = (slot_pos_out >= 0) & (slot_age >= 0) & (slot_age < WINDOW)
    num_blocks = BATCH // ROW_BLOCK

    def attend(block_in):
        q_block, k_block, v_block, mask_block = block_in
        scores = jnp.einsum('bhd,bsd->bhs', q_block.astype(jnp.float32), k_block.astype(jnp.float32)) * SCORE_SCALE
        scores = jnp.where(mask_block[:, None, :], scores, -jnp.inf)
        attn_probs = jax.nn.softmax(scores, axis=-1)
        return jnp.einsum('bhs,bsd->bhd', attn_probs, v_block.astype(jnp.float32))

    attended = lax.map(attend, (
        q_rot.reshape(num_blocks, ROW_BLOCK, HEADS, HEAD_DIM),
        k_out.reshape(num_blocks, ROW_BLOCK, WINDOW, HEAD_DIM),
        v_out.reshape(num_blocks, ROW_BLOCK, WINDOW, HEAD_DIM),
        usable.reshape(num_blocks, ROW_BLOCK, WINDOW)))
    attn_rows = attended.reshape(BATCH, HEADS * HEAD_DIM).astype(jnp.bfloat16)
    x_out = (x_in.astype(jnp.float32) + jnp.dot(attn_rows, w_o, preferred_element_type=jnp.float32) + b_o.astype(jnp.float32)).astype(jnp.bfloat16)
    return (x_out, k_out, v_out, slot_pos_out)
```

```python
import functools

import jax
import jax.numpy as jnp
import numpy as np
from jax import lax
from jax.experimental import pallas as pl
from jax.experimental.pallas import tpu as pltpu
from jax.sharding import PartitionSpec as P

HEADS = 4
HEAD_DIM = 256
ROPE_DIM = 128
ROPE_HALF = ROPE_DIM // 2
ROPE_BASE = 10000.0
EPS = 1e-6
SCORE_SCALE = HEAD_DIM ** -0.5
NEG_LARGE = float(np.finfo(np.float32).min)
FAR = 1e9
F32 = jnp.float32
BF16 = jnp.bfloat16

BATCH = 512
D_MODEL = 1152
SLOTS = 64
QW = HEADS * HEAD_DIM
PW = QW + 128
GROUP = 8
STEP = 32
LOADS = BATCH // STEP
CHUNK = 64
NCHUNK = BATCH // CHUNK
ROWS = 256


def sin_cos(theta):
    k = jnp.floor(theta * np.float32(2.0 / np.pi) + 0.5)
    r = theta - k * np.float32(1.5703125)
    r = r - k * np.float32(4.83751296997070312e-4)
    r = r - k * np.float32(7.54978995489188e-8)
    r2 = r * r
    s = r + r * r2 * (-1.6666654611e-1 + r2 * (8.3321608736e-3 + r2 * -1.9515295891e-4))
    c = 1.0 - 0.5 * r2 + r2 * r2 * (4.166664568298827e-2 + r2 * (-1.388731625493765e-3 + r2 * 2.443315711809948e-5))
    q = k - 4.0 * jnp.floor(k * 0.25)
    swap = (q == 1.0) | (q == 3.0)
    sin_v = jnp.where(swap, c, s)
    cos_v = jnp.where(swap, s, c)
    sin_v = jnp.where(q >= 2.0, -sin_v, sin_v)
    cos_v = jnp.where((q == 1.0) | (q == 2.0), -cos_v, cos_v)
    return sin_v, cos_v


def inv_freq_row():
    i = np.arange(ROPE_DIM) % ROPE_HALF
    return (ROPE_BASE ** (-i / ROPE_HALF)).astype(np.float32).reshape(1, ROPE_DIM)


def attn_kernel(pos_row, freq_ref, sp_ref, ns_ref, x_hbm, wq_hbm, wk_hbm, wv_hbm, k_hbm, v_hbm,
                part_ref, sp_out, k_out, v_out,
                kbuf, vbuf, x_v, wq_v, wk_v, wv_v, n_v, q_v, kn_v, vn_v, p_col, js_col, cos_v, sin_v,
                w_sem, k_sem, v_sem, ko_sem, vo_sem):
    off = lax.axis_index('kv') * SLOTS
    weights = ((x_hbm, x_v), (wk_hbm, wk_v), (wv_hbm, wv_v), (wq_hbm, wq_v))
    for n, (src, dst) in enumerate(weights):
        pltpu.make_async_copy(src, dst, w_sem.at[n]).start()

    def rows_of(c):
        return pl.ds(pl.multiple_of(c * STEP, STEP), STEP)

    def k_in(c):
        return pltpu.make_async_copy(k_hbm.at[rows_of(c)], kbuf.at[rows_of(c)], k_sem.at[c])

    def v_in(c):
        return pltpu.make_async_copy(v_hbm.at[rows_of(c)], vbuf.at[rows_of(c)], v_sem.at[c])

    def k_back(c):
        return pltpu.make_async_copy(kbuf.at[rows_of(c)], k_out.at[rows_of(c)], ko_sem.at[c])

    def v_back(c):
        return pltpu.make_async_copy(vbuf.at[rows_of(c)], v_out.at[rows_of(c)], vo_sem.at[c])

    @pl.loop(0, LOADS)
    def _(c):
        k_in(c).start()
        v_in(c).start()

    offf = off.astype(F32)
    for t in range(BATCH // 128):
        row = jnp.broadcast_to(pos_row[:, t * 128:(t + 1) * 128].astype(F32), (128, 128))
        col = row.T
        p_col[pl.ds(t * 128, 128), :] = col
        js = col - 512.0 * jnp.floor(col * (1.0 / 512.0)) - offf
        js_col[pl.ds(t * 128, 128), :] = jnp.where((js >= 0.0) & (js < float(SLOTS)), js, -1.0)
        s, c = sin_cos(col * freq_ref[...])
        lane = lax.broadcasted_iota(jnp.int32, (128, 128), 1)
        sin_v[pl.ds(t * 128, 128), :] = jnp.where(lane < ROPE_HALF, -s, s)
        cos_v[pl.ds(t * 128, 128), :] = c

    p_all = pos_row[...]
    slot_ids = off + lax.broadcasted_iota(jnp.int32, (SLOTS, BATCH), 0)
    sp_out[...] = jnp.where(slot_ids == (p_all & 511), p_all, sp_ref[...])

    def rotate(t, rows):
        r = t[:, :ROPE_DIM]
        r = r * cos_v[rows, :] + pltpu.roll(r, ROPE_HALF, 1) * sin_v[rows, :]
        return jnp.concatenate([r, t[:, ROPE_DIM:]], axis=1)

    for n in range(3):
        src, dst = weights[n]
        pltpu.make_async_copy(src, dst, w_sem.at[n]).wait()

    @pl.loop(0, BATCH // ROWS)
    def _(i):
        rows = pl.ds(pl.multiple_of(i * ROWS, ROWS), ROWS)
        xf = x_v[rows, :].astype(F32)
        mean_sq = jnp.sum(xf * xf, axis=1, keepdims=True) * (1.0 / D_MODEL)
        n_v[rows, :] = (xf * lax.rsqrt(mean_sq + EPS) * (1.0 + ns_ref[...].astype(F32))).astype(BF16)
        kn = jnp.dot(n_v[rows, :], wk_v[...], preferred_element_type=F32)
        kn_v[rows, :] = rotate(kn, rows)
        vn_v[rows, :] = jnp.dot(n_v[rows, :], wv_v[...], preferred_element_type=F32)

    pltpu.make_async_copy(wq_hbm, wq_v, w_sem.at[3]).wait()

    @pl.loop(0, BATCH // ROWS)
    def _(i):
        rows = pl.ds(pl.multiple_of(i * ROWS, ROWS), ROWS)

        @pl.loop(0, HEADS)
        def _(h):
            cols = pl.ds(pl.multiple_of(h * HEAD_DIM, HEAD_DIM), HEAD_DIM)
            qh = jnp.dot(n_v[rows, :], wq_v[:, cols], preferred_element_type=F32)
            q_v[rows, cols] = rotate(qh, rows) * SCORE_SCALE

    sub = lax.broadcasted_iota(jnp.int32, (GROUP, 128), 0)
    lane = lax.broadcasted_iota(jnp.int32, (GROUP, 128), 1)
    slot_c = jnp.where((lane // SLOTS) == (sub % 2), (lane % SLOTS).astype(F32) + offf, FAR)
    pick = [(sub // 2) == cc for cc in range(4)]
    iotas = [(lax.broadcasted_iota(jnp.int32, (16, HEAD_DIM), 0) + 16 * t).astype(F32).astype(BF16) for t in range(SLOTS // 16)]

    def refresh(buf, new_ref, b, hits):
        fresh = jnp.broadcast_to(new_ref[pl.ds(b, 1), :], (16, HEAD_DIM)).astype(BF16)
        out = []
        for t in range(SLOTS // 16):
            piece = jnp.where(hits[t], fresh, buf[b, pl.ds(16 * t, 16), :])
            buf[b, pl.ds(16 * t, 16), :] = piece
            out.append(piece)
        return out

    def group(r0):
        ks, vs = [], []
        for i in range(GROUP):
            b = r0 + i
            js = jnp.broadcast_to(js_col[pl.ds(b, 1), :], (16, 128)).astype(BF16)
            js = jnp.concatenate([js, js], axis=1)
            hits = [io == js for io in iotas]
            ks += refresh(kbuf, kn_v, b, hits)
            vs += refresh(vbuf, vn_v, b, hits)
        rows = pl.ds(r0, GROUP)
        q = jnp.concatenate([q_v[rows, h * HEAD_DIM:(h + 1) * HEAD_DIM] for h in range(HEADS)], axis=0).astype(BF16)
        kmat = jnp.concatenate(ks, axis=0)
        vmat = jnp.concatenate(vs, axis=0)
        s = lax.dot_general(q, kmat, (((1,), (1,)), ((), ())), preferred_element_type=F32)
        valid = slot_c <= p_col[rows, :]
        stats = jnp.zeros((GROUP, 128), F32)
        ps = []
        for h in range(HEADS):
            sh = s[h * GROUP:(h + 1) * GROUP, :]
            c = sh[:, 384:512]
            for cc in range(3):
                c = jnp.where(pick[cc], sh[:, cc * 128:(cc + 1) * 128], c)
            c = jnp.where(valid, c, NEG_LARGE)
            m = jnp.max(c, axis=1, keepdims=True)
            e = jnp.where(valid, jnp.exp(c - m), 0.0)
            l = jnp.sum(e, axis=1, keepdims=True)
            stats = jnp.where(lane == h, m, stats)
            stats = jnp.where(lane == HEADS + h, l, stats)
            ps.append(jnp.concatenate([jnp.where(pick[cc], e, 0.0) for cc in range(4)], axis=1))
        pm = jnp.concatenate(ps, axis=0).astype(BF16)
        o = jnp.dot(pm, vmat, preferred_element_type=F32)
        for h in range(HEADS):
            part_ref[rows, h * HEAD_DIM:(h + 1) * HEAD_DIM] = o[h * GROUP:(h + 1) * GROUP, :]
        part_ref[rows, QW:PW] = stats

    @pl.loop(0, LOADS)
    def _(c):
        k_in(c).wait()
        v_in(c).wait()
        for g in range(STEP // GROUP):
            group(pl.multiple_of(c * STEP + g * GROUP, GROUP))
        k_back(c).start()
        v_back(c).start()

    @pl.loop(0, LOADS)
    def _(c):
        k_back(c).wait()
        v_back(c).wait()


def merge_rows(a_rows, b_rows):
    sa, sb = a_rows[1], b_rows[1]
    lane = lax.broadcasted_iota(jnp.int32, sa.shape, 1)
    ma, mb = sa, sb
    mm = jnp.maximum(ma, mb)
    fa, fb = jnp.exp(ma - mm), jnp.exp(mb - mm)
    fa_l = pltpu.roll(fa, HEADS, 1)
    fb_l = pltpu.roll(fb, HEADS, 1)
    stats = jnp.where(lane < HEADS, mm, sa * fa_l + sb * fb_l)
    vals = []
    for h in range(HEADS):
        va = a_rows[0][:, h * HEAD_DIM:(h + 1) * HEAD_DIM]
        vb = b_rows[0][:, h * HEAD_DIM:(h + 1) * HEAD_DIM]
        vals.append(va * fa[:, h:h + 1] + vb * fb[:, h:h + 1])
    return jnp.concatenate(vals, axis=1), stats


class Places:
    def __init__(self):
        me = lax.axis_index('kv')
        self.core = me % 2
        self.x = (me // 2) % 2
        self.y = me // 4
        self.mate = me + 1 - 2 * self.core
        self.x_peer = me + 2 - 4 * self.x
        self.y_peer = me + 4 - 8 * self.y

    def first(self, c):
        odd = c % 2
        return self.x_peer + odd * (self.y_peer - self.x_peer), self.x + odd * (self.y - self.x)

    def second(self, c):
        odd = c % 2
        return self.y_peer + odd * (self.x_peer - self.y_peer), self.y + odd * (self.x - self.y)


def enter(pl_):
    barrier = pltpu.get_barrier_semaphore()
    for peer in (pl_.mate, pl_.x_peer, pl_.y_peer):
        pl.semaphore_signal(barrier, inc=1, device_id={'kv': peer}, device_id_type=pl.DeviceIdType.MESH)
    pl.semaphore_wait(barrier, 3)


def send(src, dst, ss, rs, peer):
    return pltpu.make_async_remote_copy(src_ref=src, dst_ref=dst, send_sem=ss, recv_sem=rs,
                                        device_id={'kv': peer}, device_id_type=pl.DeviceIdType.MESH)


def al(v, m=8):
    return pl.multiple_of(v, m)


class Reduce:
    def __init__(self, places, part, r0, r1, r2, own, sems):
        self.p = places
        self.part, self.r0, self.r1, self.r2, self.own = part, r0, r1, r2, own
        self.s0s, self.s0r, self.s1s, self.s1r, self.s2s, self.s2r = sems

    def copy0(self, c):
        src = al(c * CHUNK + 32 * (1 - self.p.core))
        return send(self.part.at[pl.ds(src, 32)], self.r0.at[pl.ds(al(c * 32), 32)], self.s0s.at[c], self.s0r.at[c], self.p.mate)

    def copy1(self, c):
        peer, k = self.p.first(c)
        src = al(c * CHUNK + 32 * self.p.core + 16 * (1 - k))
        return send(self.part.at[pl.ds(src, 16)], self.r1.at[pl.ds(al(c * 16), 16)], self.s1s.at[c], self.s1r.at[c], peer)

    def copy2(self, c):
        peer, k2 = self.p.second(c)
        k1 = self.p.first(c)[1]
        src = al(c * CHUNK + 32 * self.p.core + 16 * k1 + 8 * (1 - k2))
        return send(self.part.at[pl.ds(src, 8)], self.r2.at[pl.ds(al(c * 8), 8)], self.s2s.at[c], self.s2r.at[c], peer)

    def merge(self, mine, other_ref, theirs):
        a = self.part[pl.ds(mine, 8), :]
        b = other_ref[pl.ds(theirs, 8), :]
        return merge_rows((a[:, :QW], a[:, QW:]), (b[:, :QW], b[:, QW:]))

    def step0(self, c):
        self.copy0(c).wait_recv()
        base = c * CHUNK + 32 * self.p.core
        for t in range(4):
            v, s = self.merge(al(base + 8 * t), self.r0, al(c * 32 + 8 * t))
            self.part[pl.ds(al(base + 8 * t), 8), :] = jnp.concatenate([v, s], axis=1)

    def step1(self, c):
        self.copy1(c).wait_recv()
        base = c * CHUNK + 32 * self.p.core + 16 * self.p.first(c)[1]
        for t in range(2):
            v, s = self.merge(al(base + 8 * t), self.r1, al(c * 16 + 8 * t))
            self.part[pl.ds(al(base + 8 * t), 8), :] = jnp.concatenate([v, s], axis=1)

    def step2(self, c):
        self.copy2(c).wait_recv()
        base = c * CHUNK + 32 * self.p.core + 16 * self.p.first(c)[1] + 8 * self.p.second(c)[1]
        v, s = self.merge(al(base), self.r2, al(c * 8))
        outs = [v[:, h * HEAD_DIM:(h + 1) * HEAD_DIM] / s[:, HEADS + h:HEADS + h + 1] for h in range(HEADS)]
        self.own[pl.ds(al(base), 8), :] = jnp.concatenate(outs, axis=1)

    def drain(self, c):
        self.copy0(c).wait_send()
        self.copy1(c).wait_send()
        self.copy2(c).wait_send()


class Gather:
    def __init__(self, places, g, sems):
        self.p, self.g = places, g
        self.s0s, self.s0r, self.s1s, self.s1r, self.s2s, self.s2r = sems

    def copy0(self, c):
        peer, k2 = self.p.second(c)
        k1 = self.p.first(c)[1]
        rows = pl.ds(al(c * CHUNK + 32 * self.p.core + 16 * k1 + 8 * k2), 8)
        return send(self.g.at[rows], self.g.at[rows], self.s0s.at[c], self.s0r.at[c], peer)

    def copy1(self, c):
        peer, k1 = self.p.first(c)
        rows = pl.ds(al(c * CHUNK + 32 * self.p.core + 16 * k1), 16)
        return send(self.g.at[rows], self.g.at[rows], self.s1s.at[c], self.s1r.at[c], peer)

    def copy2(self, c):
        rows = pl.ds(al(c * CHUNK + 32 * self.p.core), 32)
        return send(self.g.at[rows], self.g.at[rows], self.s2s.at[c], self.s2r.at[c], self.p.mate)

    def drain(self, c):
        self.copy0(c).wait_send()
        self.copy1(c).wait_send()
        self.copy2(c).wait_send()


def comm_kernel(part_in, x_ref, wo_ref, b_ref, out_ref, part, r0, r1, r2, g, lsem, rsems, gsems):
    p = Places()
    cp = pltpu.make_async_copy(part_in, part, lsem)
    cp.start()
    cp.wait()
    enter(p)
    red = Reduce(p, part, r0, r1, r2, g, [rsems.at[i] for i in range(6)])
    gat = Gather(p, g, [gsems.at[i] for i in range(6)])

    @pl.loop(0, NCHUNK)
    def _(c):
        red.copy0(c).start()

    @pl.loop(0, NCHUNK)
    def _(c):
        red.step0(c)
        red.copy1(c).start()

    @pl.loop(0, NCHUNK)
    def _(c):
        red.step1(c)
        red.copy2(c).start()

    @pl.loop(0, NCHUNK)
    def _(c):
        red.step2(c)
        gat.copy0(c).start()

    @pl.loop(0, NCHUNK)
    def _(c):
        gat.copy0(c).wait_recv()
        gat.copy1(c).start()

    @pl.loop(0, NCHUNK)
    def _(c):
        gat.copy1(c).wait_recv()
        gat.copy2(c).start()

    @pl.loop(0, NCHUNK // 2)
    def _(i):
        gat.copy2(2 * i).wait_recv()
        gat.copy2(2 * i + 1).wait_recv()
        rows = pl.ds(al(i * 2 * CHUNK, 2 * CHUNK), 2 * CHUNK)
        o = g[rows, :].astype(BF16)
        y = x_ref[rows, :].astype(F32) + jnp.dot(o, wo_ref[...], preferred_element_type=F32) + b_ref[...].astype(F32)
        out_ref[rows, :] = y.astype(BF16)

    @pl.loop(0, NCHUNK)
    def _(c):
        red.drain(c)
        gat.drain(c)


def solution(mesh):
    row_spec = P('dp', None)
    cache_spec = P('dp', 'kv', None)
    slot_spec = P('dp', 'kv')
    vec_spec = P(None)
    mat_spec = P(None, None)
    hbm = pl.BlockSpec(memory_space=pltpu.HBM)
    vmem = pl.BlockSpec(memory_space=pltpu.VMEM)

    def local_step(x_in, positions, k_cache, v_cache, slot_pos, norm_scale, w_q, w_k, w_v, w_o, b_o):
        part, sp_t, k_out, v_out = pl.pallas_call(
            attn_kernel,
            out_shape=(jax.ShapeDtypeStruct((BATCH, PW), F32),
                       jax.ShapeDtypeStruct((SLOTS, BATCH), jnp.int32),
                       jax.ShapeDtypeStruct(k_cache.shape, BF16),
                       jax.ShapeDtypeStruct(v_cache.shape, BF16)),
            in_specs=[vmem, vmem, vmem, vmem, hbm, hbm, hbm, hbm, hbm, hbm],
            out_specs=(vmem, vmem, hbm, hbm),
            scratch_shapes=[
                pltpu.VMEM((BATCH, SLOTS, HEAD_DIM), BF16),
                pltpu.VMEM((BATCH, SLOTS, HEAD_DIM), BF16),
                pltpu.VMEM((BATCH, D_MODEL), BF16),
                pltpu.VMEM((D_MODEL, QW), BF16),
                pltpu.VMEM((D_MODEL, HEAD_DIM), BF16),
                pltpu.VMEM((D_MODEL, HEAD_DIM), BF16),
                pltpu.VMEM((BATCH, D_MODEL), BF16),
                pltpu.VMEM((BATCH, QW), F32),
                pltpu.VMEM((BATCH, HEAD_DIM), F32),
                pltpu.VMEM((BATCH, HEAD_DIM), F32),
                pltpu.VMEM((BATCH, 128), F32),
                pltpu.VMEM((BATCH, 128), F32),
                pltpu.VMEM((BATCH, 128), F32),
                pltpu.VMEM((BATCH, 128), F32),
                pltpu.SemaphoreType.DMA((4,)),
                pltpu.SemaphoreType.DMA((LOADS,)),
                pltpu.SemaphoreType.DMA((LOADS,)),
                pltpu.SemaphoreType.DMA((LOADS,)),
                pltpu.SemaphoreType.DMA((LOADS,)),
            ],
            cost_estimate=pl.CostEstimate(flops=4_000_000_000, bytes_accessed=72_000_000, transcendentals=200_000),
            compiler_params=pltpu.CompilerParams(vmem_limit_bytes=60 * 1024 * 1024),
        )(positions.reshape(1, BATCH), jnp.asarray(inv_freq_row()), slot_pos.T, norm_scale.reshape(1, D_MODEL),
          x_in, w_q, w_k, w_v, k_cache, v_cache)
        x_out = pl.pallas_call(
            comm_kernel,
            out_shape=jax.ShapeDtypeStruct((BATCH, D_MODEL), BF16),
            in_specs=[pl.BlockSpec(memory_space=pl.ANY), vmem, vmem, vmem],
            out_specs=vmem,
            scratch_shapes=[
                pltpu.VMEM((BATCH, PW), F32),
                pltpu.VMEM((NCHUNK * 32, PW), F32),
                pltpu.VMEM((NCHUNK * 16, PW), F32),
                pltpu.VMEM((NCHUNK * 8, PW), F32),
                pltpu.VMEM((BATCH, QW), F32),
                pltpu.SemaphoreType.DMA,
                pltpu.SemaphoreType.DMA((6, NCHUNK)),
                pltpu.SemaphoreType.DMA((6, NCHUNK)),
            ],
            cost_estimate=pl.CostEstimate(flops=1_200_000_000, bytes_accessed=6_000_000, transcendentals=0),
            compiler_params=pltpu.CompilerParams(collective_id=0, has_side_effects=True, vmem_limit_bytes=32 * 1024 * 1024),
        )(part, x_in, w_o, b_o.reshape(1, D_MODEL))
        return x_out, k_out, v_out, sp_t.T

    return jax.shard_map(
        local_step,
        mesh=mesh,
        in_specs=(row_spec, P('dp'), cache_spec, cache_spec, slot_spec, vec_spec, mat_spec, mat_spec, mat_spec, mat_spec, vec_spec),
        out_specs=(row_spec, cache_spec, cache_spec, slot_spec),
        check_vma=False)
```

```python
import functools

import jax
import jax.numpy as jnp
import numpy as np
from jax import lax
from jax.experimental import pallas as pl
from jax.experimental.pallas import tpu as pltpu
from jax.sharding import PartitionSpec as P

HEADS = 4
HEAD_DIM = 256
ROPE_DIM = 128
ROPE_HALF = ROPE_DIM // 2
ROPE_BASE = 10000.0
EPS = 1e-6
SCORE_SCALE = HEAD_DIM ** -0.5
NEG_LARGE = float(np.finfo(np.float32).min)
FAR = 1e9
F32 = jnp.float32
BF16 = jnp.bfloat16

BATCH = 512
D_MODEL = 1152
SLOTS = 64
QW = HEADS * HEAD_DIM
PW = QW + 128
GROUP = 8
STEP = 32
CHUNK = 64
AHEAD = 4
NCHUNK = BATCH // CHUNK
ROWS = 256


def sin_cos(theta):
    k = jnp.floor(theta * np.float32(2.0 / np.pi) + 0.5)
    r = theta - k * np.float32(1.5703125)
    r = r - k * np.float32(4.83751296997070312e-4)
    r = r - k * np.float32(7.54978995489188e-8)
    r2 = r * r
    s = r + r * r2 * (-1.6666654611e-1 + r2 * (8.3321608736e-3 + r2 * -1.9515295891e-4))
    c = 1.0 - 0.5 * r2 + r2 * r2 * (4.166664568298827e-2 + r2 * (-1.388731625493765e-3 + r2 * 2.443315711809948e-5))
    q = k - 4.0 * jnp.floor(k * 0.25)
    swap = (q == 1.0) | (q == 3.0)
    sin_v = jnp.where(swap, c, s)
    cos_v = jnp.where(swap, s, c)
    sin_v = jnp.where(q >= 2.0, -sin_v, sin_v)
    cos_v = jnp.where((q == 1.0) | (q == 2.0), -cos_v, cos_v)
    return sin_v, cos_v


def inv_freq_row():
    i = np.arange(ROPE_DIM) % ROPE_HALF
    return (ROPE_BASE ** (-i / ROPE_HALF)).astype(np.float32).reshape(1, ROPE_DIM)


def merge_rows(a_rows, b_rows):
    sa, sb = a_rows[1], b_rows[1]
    lane = lax.broadcasted_iota(jnp.int32, sa.shape, 1)
    ma, mb = sa, sb
    mm = jnp.maximum(ma, mb)
    fa, fb = jnp.exp(ma - mm), jnp.exp(mb - mm)
    fa_l = pltpu.roll(fa, HEADS, 1)
    fb_l = pltpu.roll(fb, HEADS, 1)
    stats = jnp.where(lane < HEADS, mm, sa * fa_l + sb * fb_l)
    vals = []
    for h in range(HEADS):
        va = a_rows[0][:, h * HEAD_DIM:(h + 1) * HEAD_DIM]
        vb = b_rows[0][:, h * HEAD_DIM:(h + 1) * HEAD_DIM]
        vals.append(va * fa[:, h:h + 1] + vb * fb[:, h:h + 1])
    return jnp.concatenate(vals, axis=1), stats


class Places:
    def __init__(self):
        me = lax.axis_index('kv')
        self.core = me % 2
        self.x = (me // 2) % 2
        self.y = me // 4
        self.mate = me + 1 - 2 * self.core
        self.x_peer = me + 2 - 4 * self.x
        self.y_peer = me + 4 - 8 * self.y

    def first(self, c):
        odd = c % 2
        return self.x_peer + odd * (self.y_peer - self.x_peer), self.x + odd * (self.y - self.x)

    def second(self, c):
        odd = c % 2
        return self.y_peer + odd * (self.x_peer - self.y_peer), self.y + odd * (self.x - self.y)


def send(src, dst, ss, rs, peer):
    return pltpu.make_async_remote_copy(src_ref=src, dst_ref=dst, send_sem=ss, recv_sem=rs,
                                        device_id={'kv': peer}, device_id_type=pl.DeviceIdType.MESH)


def al(v, m=8):
    return pl.multiple_of(v, m)


class Reduce:
    def __init__(self, places, part, r0, r1, r2, own, sems):
        self.p = places
        self.part, self.r0, self.r1, self.r2, self.own = part, r0, r1, r2, own
        self.s0s, self.s0r, self.s1s, self.s1r, self.s2s, self.s2r = sems

    def copy0(self, c):
        src = al(c * CHUNK + 32 * (1 - self.p.core))
        return send(self.part.at[pl.ds(src, 32)], self.r0.at[pl.ds(al(c * 32), 32)], self.s0s.at[c], self.s0r.at[c], self.p.mate)

    def copy1(self, c):
        peer, k = self.p.first(c)
        src = al(c * CHUNK + 32 * self.p.core + 16 * (1 - k))
        return send(self.part.at[pl.ds(src, 16)], self.r1.at[pl.ds(al(c * 16), 16)], self.s1s.at[c], self.s1r.at[c], peer)

    def copy2(self, c):
        peer, k2 = self.p.second(c)
        k1 = self.p.first(c)[1]
        src = al(c * CHUNK + 32 * self.p.core + 16 * k1 + 8 * (1 - k2))
        return send(self.part.at[pl.ds(src, 8)], self.r2.at[pl.ds(al(c * 8), 8)], self.s2s.at[c], self.s2r.at[c], peer)

    def merge(self, mine, other_ref, theirs):
        a = self.part[pl.ds(mine, 8), :]
        b = other_ref[pl.ds(theirs, 8), :]
        return merge_rows((a[:, :QW], a[:, QW:]), (b[:, :QW], b[:, QW:]))

    def step0(self, c):
        self.copy0(c).wait_recv()
        base = c * CHUNK + 32 * self.p.core
        for t in range(4):
            v, s = self.merge(al(base + 8 * t), self.r0, al(c * 32 + 8 * t))
            self.part[pl.ds(al(base + 8 * t), 8), :] = jnp.concatenate([v, s], axis=1)

    def step1(self, c):
        self.copy1(c).wait_recv()
        base = c * CHUNK + 32 * self.p.core + 16 * self.p.first(c)[1]
        for t in range(2):
            v, s = self.merge(al(base + 8 * t), self.r1, al(c * 16 + 8 * t))
            self.part[pl.ds(al(base + 8 * t), 8), :] = jnp.concatenate([v, s], axis=1)

    def step2(self, c):
        self.copy2(c).wait_recv()
        base = c * CHUNK + 32 * self.p.core + 16 * self.p.first(c)[1] + 8 * self.p.second(c)[1]
        v, s = self.merge(al(base), self.r2, al(c * 8))
        outs = [v[:, h * HEAD_DIM:(h + 1) * HEAD_DIM] / s[:, HEADS + h:HEADS + h + 1] for h in range(HEADS)]
        self.own[pl.ds(al(base), 8), :] = jnp.concatenate(outs, axis=1)

    def drain(self, c):
        self.copy0(c).wait_send()
        self.copy1(c).wait_send()
        self.copy2(c).wait_send()


class Gather:
    def __init__(self, places, g, sems):
        self.p, self.g = places, g
        self.s0s, self.s0r, self.s1s, self.s1r, self.s2s, self.s2r = sems

    def copy0(self, c):
        peer, k2 = self.p.second(c)
        k1 = self.p.first(c)[1]
        rows = pl.ds(al(c * CHUNK + 32 * self.p.core + 16 * k1 + 8 * k2), 8)
        return send(self.g.at[rows], self.g.at[rows], self.s0s.at[c], self.s0r.at[c], peer)

    def copy1(self, c):
        peer, k1 = self.p.first(c)
        rows = pl.ds(al(c * CHUNK + 32 * self.p.core + 16 * k1), 16)
        return send(self.g.at[rows], self.g.at[rows], self.s1s.at[c], self.s1r.at[c], peer)

    def copy2(self, c):
        rows = pl.ds(al(c * CHUNK + 32 * self.p.core), 32)
        return send(self.g.at[rows], self.g.at[rows], self.s2s.at[c], self.s2r.at[c], self.p.mate)

    def drain(self, c):
        self.copy0(c).wait_send()
        self.copy1(c).wait_send()
        self.copy2(c).wait_send()


def step_kernel(pos_row, freq_ref, ns_ref, b_ref, x_hbm, wq_hbm, wk_hbm, wv_hbm, wo_hbm, k_hbm, v_hbm,
                kbuf, vbuf, out_ref,
                x_v, wq_v, wk_v, wv_v, wo_v, n_v, q_v, kn_v, vn_v, p_col, js_col, cos_v, sin_v,
                part, r0, r1, r2, g, w_sem, k_sem, v_sem, rsems, gsems):
    p = Places()
    barrier = pltpu.get_barrier_semaphore()
    for peer in (p.mate, p.x_peer, p.y_peer):
        pl.semaphore_signal(barrier, inc=1, device_id={'kv': peer}, device_id_type=pl.DeviceIdType.MESH)
    off = lax.axis_index('kv') * SLOTS
    weights = ((x_hbm, x_v), (wk_hbm, wk_v), (wv_hbm, wv_v), (wq_hbm, wq_v), (wo_hbm, wo_v))

    def w_in(n):
        return pltpu.make_async_copy(weights[n][0], weights[n][1], w_sem.at[n])

    def rows_of(c):
        return pl.ds(pl.multiple_of(c * CHUNK, CHUNK), CHUNK)

    def k_in(c):
        return pltpu.make_async_copy(k_hbm.at[rows_of(c)], kbuf.at[rows_of(c)], k_sem.at[c])

    def v_in(c):
        return pltpu.make_async_copy(v_hbm.at[rows_of(c)], vbuf.at[rows_of(c)], v_sem.at[c])

    for n in range(4):
        w_in(n).start()
    for c in range(AHEAD):
        k_in(c).start()
        v_in(c).start()

    offf = off.astype(F32)

    @pl.loop(0, BATCH // 128)
    def _(t):
        rows = pl.ds(pl.multiple_of(t * 128, 128), 128)
        col = jnp.broadcast_to(pos_row[:, rows].astype(F32), (128, 128)).T
        p_col[rows, :] = col
        js = col - 512.0 * jnp.floor(col * (1.0 / 512.0)) - offf
        js_col[rows, :] = jnp.where((js >= 0.0) & (js < float(SLOTS)), js, -1.0)

    @pl.loop(0, BATCH // 64)
    def _(t):
        rows = pl.ds(pl.multiple_of(t * 64, 64), 64)
        s, c = sin_cos(p_col[rows, :] * freq_ref[...])
        lane = lax.broadcasted_iota(jnp.int32, (64, 128), 1)
        sin_v[rows, :] = jnp.where(lane < ROPE_HALF, -s, s)
        cos_v[rows, :] = c

    def rotate(t, rows):
        r = t[:, :ROPE_DIM]
        r = r * cos_v[rows, :] + pltpu.roll(r, ROPE_HALF, 1) * sin_v[rows, :]
        return jnp.concatenate([r, t[:, ROPE_DIM:]], axis=1)

    w_in(0).wait()
    gain = 1.0 + ns_ref[...].astype(F32).reshape(1, D_MODEL)

    @pl.loop(0, BATCH // 64)
    def _(i):
        rows = pl.ds(pl.multiple_of(i * 64, 64), 64)
        xf = x_v[rows, :].astype(F32)
        mean_sq = jnp.sum(xf * xf, axis=1, keepdims=True) * (1.0 / D_MODEL)
        n_v[rows, :] = (xf * lax.rsqrt(mean_sq + EPS) * gain).astype(BF16)

    w_in(1).wait()
    w_in(2).wait()
    w_in(3).wait()

    def project(i):
        rows = pl.ds(pl.multiple_of(i * ROWS, ROWS), ROWS)
        kn_v[rows, :] = rotate(jnp.dot(n_v[rows, :], wk_v[...], preferred_element_type=F32), rows)
        vn_v[rows, :] = jnp.dot(n_v[rows, :], wv_v[...], preferred_element_type=F32)

        @pl.loop(0, HEADS)
        def _(h):
            cols = pl.ds(pl.multiple_of(h * HEAD_DIM, HEAD_DIM), HEAD_DIM)
            qh = jnp.dot(n_v[rows, :], wq_v[:, cols], preferred_element_type=F32)
            q_v[rows, cols] = rotate(qh, rows) * SCORE_SCALE

    sub = lax.broadcasted_iota(jnp.int32, (GROUP, 128), 0)
    lane = lax.broadcasted_iota(jnp.int32, (GROUP, 128), 1)
    slot_c = jnp.where((lane // SLOTS) == (sub % 2), (lane % SLOTS).astype(F32) + offf, FAR)
    pick = [(sub // 2) == cc for cc in range(4)]
    iotas = [(lax.broadcasted_iota(jnp.int32, (16, HEAD_DIM), 0) + 16 * t).astype(F32).astype(BF16) for t in range(SLOTS // 16)]
    def refresh(buf, new_ref, b, hits):
        fresh = jnp.broadcast_to(new_ref[pl.ds(b, 1), :], (16, HEAD_DIM)).astype(BF16)
        out = []
        for t in range(SLOTS // 16):
            piece = jnp.where(hits[t], fresh, buf[b, pl.ds(16 * t, 16), :])
            buf[b, pl.ds(16 * t, 16), :] = piece
            out.append(piece)
        return out

    def group(r0):
        ks, vs = [], []
        for i in range(GROUP):
            b = r0 + i
            js = jnp.broadcast_to(js_col[pl.ds(b, 1), :], (16, 128)).astype(BF16)
            js = jnp.concatenate([js, js], axis=1)
            hits = [io == js for io in iotas]
            ks += refresh(kbuf, kn_v, b, hits)
            vs += refresh(vbuf, vn_v, b, hits)
        rows = pl.ds(r0, GROUP)
        q = jnp.concatenate([q_v[rows, h * HEAD_DIM:(h + 1) * HEAD_DIM] for h in range(HEADS)], axis=0).astype(BF16)
        kmat = jnp.concatenate(ks, axis=0)
        vmat = jnp.concatenate(vs, axis=0)
        s = lax.dot_general(q, kmat, (((1,), (1,)), ((), ())), preferred_element_type=F32)
        valid = slot_c <= p_col[rows, :]
        stats = jnp.zeros((GROUP, 128), F32)
        ps = []
        for h in range(HEADS):
            sh = s[h * GROUP:(h + 1) * GROUP, :]
            c = sh[:, 384:512]
            for cc in range(3):
                c = jnp.where(pick[cc], sh[:, cc * 128:(cc + 1) * 128], c)
            c = jnp.where(valid, c, NEG_LARGE)
            m = jnp.max(c, axis=1, keepdims=True)
            e = jnp.where(valid, jnp.exp(c - m), 0.0)
            l = jnp.sum(e, axis=1, keepdims=True)
            stats = jnp.where(lane == h, m, stats)
            stats = jnp.where(lane == HEADS + h, l, stats)
            ps.append(jnp.concatenate([jnp.where(pick[cc], e, 0.0) for cc in range(4)], axis=1))
        pm = jnp.concatenate(ps, axis=0).astype(BF16)
        o = jnp.dot(pm, vmat, preferred_element_type=F32)
        for h in range(HEADS):
            part[rows, h * HEAD_DIM:(h + 1) * HEAD_DIM] = o[h * GROUP:(h + 1) * GROUP, :]
        part[rows, QW:PW] = stats

    red = Reduce(p, part, r0, r1, r2, g, [rsems.at[i] for i in range(6)])
    gat = Gather(p, g, [gsems.at[i] for i in range(6)])

    def when_chunk(c, body):
        @pl.when((c >= 0) & (c < NCHUNK))
        def _():
            body(c)

    def attend(i):
        @pl.when(i + AHEAD < NCHUNK)
        def _():
            k_in(i + AHEAD).start()
            v_in(i + AHEAD).start()

        @pl.when(i == AHEAD)
        def _():
            w_in(4).start()

        @pl.when(i % (ROWS // CHUNK) == 0)
        def _():
            project(i // (ROWS // CHUNK))

        k_in(i).wait()
        v_in(i).wait()

        @pl.loop(0, CHUNK // STEP)
        def _(t):
            for gg in range(STEP // GROUP):
                group(pl.multiple_of(i * CHUNK + t * STEP + gg * GROUP, GROUP))

        @pl.when(i == 0)
        def _():
            pl.semaphore_wait(barrier, 3)

        red.copy0(i).start()

    def pair_step(c):
        red.step0(c)
        red.copy1(c).start()

    def first_step(c):
        red.step1(c)
        red.copy2(c).start()

    def second_step(c):
        red.step2(c)
        gat.copy0(c).start()

    def back_first(c):
        gat.copy0(c).wait_recv()
        gat.copy1(c).start()

    def back_second(c):
        gat.copy1(c).wait_recv()
        gat.copy2(c).start()

    bias = b_ref[...].astype(F32).reshape(1, D_MODEL)

    def project_out(c):
        gat.copy2(c).wait_recv()

        @pl.when(c == 1)
        def _():
            w_in(4).wait()

        @pl.when(c % 2 == 1)
        def _():
            rows = pl.ds(al((c - 1) * CHUNK, CHUNK), 2 * CHUNK)
            o = g[rows, :].astype(BF16)
            y = x_v[rows, :].astype(F32) + jnp.dot(o, wo_v[...], preferred_element_type=F32) + bias
            out_ref[rows, :] = y.astype(BF16)

    lags = ((0, attend), (1, pair_step), (4, first_step), (6, second_step), (8, back_first), (10, back_second), (11, project_out))

    @pl.loop(0, NCHUNK + lags[-1][0])
    def _(i):
        for lag, body in lags:
            when_chunk(i - lag, body)

    @pl.loop(0, NCHUNK)
    def _(c):
        red.drain(c)
        gat.drain(c)


def slot_kernel(pos_row, sp_ref, sp_out):
    off = lax.axis_index('kv') * SLOTS
    p_all = pos_row[...]
    slot_ids = off + lax.broadcasted_iota(jnp.int32, (SLOTS, BATCH), 0)
    sp_out[...] = jnp.where(slot_ids == (p_all & 511), p_all, sp_ref[...])


def solution(mesh):
    row_spec = P('dp', None)
    cache_spec = P('dp', 'kv', None)
    slot_spec = P('dp', 'kv')
    vec_spec = P(None)
    mat_spec = P(None, None)
    hbm = pl.BlockSpec(memory_space=pltpu.HBM)
    vmem = pl.BlockSpec(memory_space=pltpu.VMEM)

    def local_step(x_in, positions, k_cache, v_cache, slot_pos, norm_scale, w_q, w_k, w_v, w_o, b_o):
        pos_row = positions.reshape(1, BATCH)
        kbuf, vbuf, x_new = pl.pallas_call(
            step_kernel,
            out_shape=(pltpu.VMEM((BATCH, SLOTS, HEAD_DIM), BF16),
                       pltpu.VMEM((BATCH, SLOTS, HEAD_DIM), BF16),
                       pltpu.VMEM((BATCH, D_MODEL), BF16)),
            in_specs=[vmem, vmem, vmem, vmem, hbm, hbm, hbm, hbm, hbm, hbm, hbm],
            out_specs=(vmem, vmem, vmem),
            scratch_shapes=[
                pltpu.VMEM((BATCH, D_MODEL), BF16),
                pltpu.VMEM((D_MODEL, QW), BF16),
                pltpu.VMEM((D_MODEL, HEAD_DIM), BF16),
                pltpu.VMEM((D_MODEL, HEAD_DIM), BF16),
                pltpu.VMEM((QW, D_MODEL), BF16),
                pltpu.VMEM((BATCH, D_MODEL), BF16),
                pltpu.VMEM((BATCH, QW), F32),
                pltpu.VMEM((BATCH, HEAD_DIM), F32),
                pltpu.VMEM((BATCH, HEAD_DIM), F32),
                pltpu.VMEM((BATCH, 128), F32),
                pltpu.VMEM((BATCH, 128), F32),
                pltpu.VMEM((BATCH, 128), F32),
                pltpu.VMEM((BATCH, 128), F32),
                pltpu.VMEM((BATCH, PW), F32),
                pltpu.VMEM((NCHUNK * 32, PW), F32),
                pltpu.VMEM((NCHUNK * 16, PW), F32),
                pltpu.VMEM((NCHUNK * 8, PW), F32),
                pltpu.VMEM((BATCH, QW), F32),
                pltpu.SemaphoreType.DMA((5,)),
                pltpu.SemaphoreType.DMA((NCHUNK,)),
                pltpu.SemaphoreType.DMA((NCHUNK,)),
                pltpu.SemaphoreType.DMA((6, NCHUNK)),
                pltpu.SemaphoreType.DMA((6, NCHUNK)),
            ],
            cost_estimate=pl.CostEstimate(flops=5_000_000_000, bytes_accessed=40_000_000, transcendentals=200_000),
            compiler_params=pltpu.CompilerParams(collective_id=0, has_side_effects=True, vmem_limit_bytes=22 * 1024 * 1024),
        )(pos_row, jnp.asarray(inv_freq_row()), norm_scale, b_o, x_in, w_q, w_k, w_v, w_o, k_cache, v_cache)
        sp_t = pl.pallas_call(
            slot_kernel,
            out_shape=jax.ShapeDtypeStruct((SLOTS, BATCH), jnp.int32),
            in_specs=[vmem, vmem],
            out_specs=vmem,
        )(pos_row, slot_pos.T)
        return x_new, kbuf, vbuf, sp_t.T


    return jax.shard_map(
        local_step,
        mesh=mesh,
        in_specs=(row_spec, P('dp'), cache_spec, cache_spec, slot_spec, vec_spec, mat_spec, mat_spec, mat_spec, mat_spec, vec_spec),
        out_specs=(row_spec, cache_spec, cache_spec, slot_spec),
        check_vma=False)
```

```python
import functools

import jax
import jax.numpy as jnp
import numpy as np
from jax import lax
from jax.experimental import pallas as pl
from jax.experimental.pallas import tpu as pltpu
from jax.sharding import PartitionSpec as P

HEADS = 4
HEAD_DIM = 256
ROPE_DIM = 128
ROPE_HALF = ROPE_DIM // 2
ROPE_BASE = 10000.0
EPS = 1e-6
SCORE_SCALE = HEAD_DIM ** -0.5
NEG_LARGE = float(np.finfo(np.float32).min)
FAR = 1e9
F32 = jnp.float32
BF16 = jnp.bfloat16

BATCH = 512
D_MODEL = 1152
SLOTS = 64
QW = HEADS * HEAD_DIM
PW = QW + 128
GROUP = 8
STEP = 64
CHUNK = 64
AHEAD = 4
NCHUNK = BATCH // CHUNK
ROWS = 256


def sin_cos(theta):
    k = jnp.floor(theta * np.float32(2.0 / np.pi) + 0.5)
    r = theta - k * np.float32(1.5703125)
    r = r - k * np.float32(4.83751296997070312e-4)
    r = r - k * np.float32(7.54978995489188e-8)
    r2 = r * r
    s = r + r * r2 * (-1.6666654611e-1 + r2 * (8.3321608736e-3 + r2 * -1.9515295891e-4))
    c = 1.0 - 0.5 * r2 + r2 * r2 * (4.166664568298827e-2 + r2 * (-1.388731625493765e-3 + r2 * 2.443315711809948e-5))
    q = k - 4.0 * jnp.floor(k * 0.25)
    swap = (q == 1.0) | (q == 3.0)
    sin_v = jnp.where(swap, c, s)
    cos_v = jnp.where(swap, s, c)
    sin_v = jnp.where(q >= 2.0, -sin_v, sin_v)
    cos_v = jnp.where((q == 1.0) | (q == 2.0), -cos_v, cos_v)
    return sin_v, cos_v


def inv_freq_row():
    i = np.arange(ROPE_DIM) % ROPE_HALF
    return (ROPE_BASE ** (-i / ROPE_HALF)).astype(np.float32).reshape(1, ROPE_DIM)


def merge_rows(a_rows, b_rows):
    sa, sb = a_rows[1], b_rows[1]
    lane = lax.broadcasted_iota(jnp.int32, sa.shape, 1)
    ma, mb = sa, sb
    mm = jnp.maximum(ma, mb)
    fa, fb = jnp.exp(ma - mm), jnp.exp(mb - mm)
    fa_l = pltpu.roll(fa, HEADS, 1)
    fb_l = pltpu.roll(fb, HEADS, 1)
    stats = jnp.where(lane < HEADS, mm, sa * fa_l + sb * fb_l)
    vals = []
    for h in range(HEADS):
        va = a_rows[0][:, h * HEAD_DIM:(h + 1) * HEAD_DIM]
        vb = b_rows[0][:, h * HEAD_DIM:(h + 1) * HEAD_DIM]
        vals.append(va * fa[:, h:h + 1] + vb * fb[:, h:h + 1])
    return jnp.concatenate(vals, axis=1), stats


class Places:
    def __init__(self):
        me = lax.axis_index('kv')
        self.core = me % 2
        self.x = (me // 2) % 2
        self.y = me // 4
        self.mate = me + 1 - 2 * self.core
        self.x_peer = me + 2 - 4 * self.x
        self.y_peer = me + 4 - 8 * self.y

    def first(self, c):
        odd = c % 2
        return self.x_peer + odd * (self.y_peer - self.x_peer), self.x + odd * (self.y - self.x)

    def second(self, c):
        odd = c % 2
        return self.y_peer + odd * (self.x_peer - self.y_peer), self.y + odd * (self.x - self.y)


def send(src, dst, ss, rs, peer):
    return pltpu.make_async_remote_copy(src_ref=src, dst_ref=dst, send_sem=ss, recv_sem=rs,
                                        device_id={'kv': peer}, device_id_type=pl.DeviceIdType.MESH)


def al(v, m=8):
    return pl.multiple_of(v, m)


class Reduce:
    def __init__(self, places, part, r0, r1, r2, own, sems):
        self.p = places
        self.part, self.r0, self.r1, self.r2, self.own = part, r0, r1, r2, own
        self.s0s, self.s0r, self.s1s, self.s1r, self.s2s, self.s2r = sems

    def copy0(self, c):
        src = al(c * CHUNK + 32 * (1 - self.p.core))
        return send(self.part.at[pl.ds(src, 32)], self.r0.at[pl.ds(al(c * 32), 32)], self.s0s.at[c], self.s0r.at[c], self.p.mate)

    def copy1(self, c):
        peer, k = self.p.first(c)
        src = al(c * CHUNK + 32 * self.p.core + 16 * (1 - k))
        return send(self.part.at[pl.ds(src, 16)], self.r1.at[pl.ds(al(c * 16), 16)], self.s1s.at[c], self.s1r.at[c], peer)

    def copy2(self, c):
        peer, k2 = self.p.second(c)
        k1 = self.p.first(c)[1]
        src = al(c * CHUNK + 32 * self.p.core + 16 * k1 + 8 * (1 - k2))
        return send(self.part.at[pl.ds(src, 8)], self.r2.at[pl.ds(al(c * 8), 8)], self.s2s.at[c], self.s2r.at[c], peer)

    def merge(self, mine, other_ref, theirs, n):
        a = self.part[pl.ds(mine, n), :]
        b = other_ref[pl.ds(theirs, n), :]
        return merge_rows((a[:, :QW], a[:, QW:]), (b[:, :QW], b[:, QW:]))

    def step0(self, c):
        self.copy0(c).wait_recv()
        base = al(c * CHUNK + 32 * self.p.core)
        v, s = self.merge(base, self.r0, al(c * 32), 32)
        self.part[pl.ds(base, 32), :] = jnp.concatenate([v, s], axis=1)

    def step1(self, c):
        self.copy1(c).wait_recv()
        base = al(c * CHUNK + 32 * self.p.core + 16 * self.p.first(c)[1])
        v, s = self.merge(base, self.r1, al(c * 16), 16)
        self.part[pl.ds(base, 16), :] = jnp.concatenate([v, s], axis=1)

    def step2(self, c):
        self.copy2(c).wait_recv()
        base = al(c * CHUNK + 32 * self.p.core + 16 * self.p.first(c)[1] + 8 * self.p.second(c)[1])
        v, s = self.merge(base, self.r2, al(c * 8), 8)
        outs = [v[:, h * HEAD_DIM:(h + 1) * HEAD_DIM] / s[:, HEADS + h:HEADS + h + 1] for h in range(HEADS)]
        self.own[pl.ds(base, 8), :] = jnp.concatenate(outs, axis=1)

    def drain(self, c):
        self.copy0(c).wait_send()
        self.copy1(c).wait_send()
        self.copy2(c).wait_send()


class Gather:
    def __init__(self, places, g, sems):
        self.p, self.g = places, g
        self.s0s, self.s0r, self.s1s, self.s1r, self.s2s, self.s2r = sems

    def copy0(self, c):
        peer, k2 = self.p.second(c)
        k1 = self.p.first(c)[1]
        rows = pl.ds(al(c * CHUNK + 32 * self.p.core + 16 * k1 + 8 * k2), 8)
        return send(self.g.at[rows], self.g.at[rows], self.s0s.at[c], self.s0r.at[c], peer)

    def copy1(self, c):
        peer, k1 = self.p.first(c)
        rows = pl.ds(al(c * CHUNK + 32 * self.p.core + 16 * k1), 16)
        return send(self.g.at[rows], self.g.at[rows], self.s1s.at[c], self.s1r.at[c], peer)

    def copy2(self, c):
        rows = pl.ds(al(c * CHUNK + 32 * self.p.core), 32)
        return send(self.g.at[rows], self.g.at[rows], self.s2s.at[c], self.s2r.at[c], self.p.mate)

    def drain(self, c):
        self.copy0(c).wait_send()
        self.copy1(c).wait_send()
        self.copy2(c).wait_send()


def step_kernel(pos_row, freq_ref, ns_ref, b_ref, x_hbm, wq_hbm, wk_hbm, wv_hbm, wo_hbm, k_hbm, v_hbm,
                kbuf, vbuf, out_ref,
                x_v, wq_v, wk_v, wv_v, wo_v, n_v, q_v, kn_v, vn_v, p_col, js_col, cos_v, sin_v,
                part, r0, r1, r2, g, w_sem, k_sem, v_sem, rsems, gsems):
    p = Places()
    barrier = pltpu.get_barrier_semaphore()
    for peer in (p.mate, p.x_peer, p.y_peer):
        pl.semaphore_signal(barrier, inc=1, device_id={'kv': peer}, device_id_type=pl.DeviceIdType.MESH)
    off = lax.axis_index('kv') * SLOTS
    weights = ((x_hbm, x_v), (wk_hbm, wk_v), (wv_hbm, wv_v), (wq_hbm, wq_v), (wo_hbm, wo_v))

    def w_in(n):
        return pltpu.make_async_copy(weights[n][0], weights[n][1], w_sem.at[n])

    def rows_of(c):
        return pl.ds(pl.multiple_of(c * CHUNK, CHUNK), CHUNK)

    def k_in(c):
        return pltpu.make_async_copy(k_hbm.at[rows_of(c)], kbuf.at[rows_of(c)], k_sem.at[c])

    def v_in(c):
        return pltpu.make_async_copy(v_hbm.at[rows_of(c)], vbuf.at[rows_of(c)], v_sem.at[c])

    for n in range(4):
        w_in(n).start()
    for c in range(AHEAD):
        k_in(c).start()
        v_in(c).start()

    offf = off.astype(F32)

    @pl.loop(0, BATCH // 128)
    def _(t):
        rows = pl.ds(pl.multiple_of(t * 128, 128), 128)
        col = jnp.broadcast_to(pos_row[:, rows].astype(F32), (128, 128)).T
        p_col[rows, :] = col
        js = col - 512.0 * jnp.floor(col * (1.0 / 512.0)) - offf
        js_col[rows, :] = jnp.where((js >= 0.0) & (js < float(SLOTS)), js, -1.0)

    @pl.loop(0, BATCH // 64)
    def _(t):
        rows = pl.ds(pl.multiple_of(t * 64, 64), 64)
        s, c = sin_cos(p_col[rows, :] * freq_ref[...])
        lane = lax.broadcasted_iota(jnp.int32, (64, 128), 1)
        sin_v[rows, :] = jnp.where(lane < ROPE_HALF, -s, s)
        cos_v[rows, :] = c

    def rotate(t, rows):
        r = t[:, :ROPE_DIM]
        r = r * cos_v[rows, :] + pltpu.roll(r, ROPE_HALF, 1) * sin_v[rows, :]
        return jnp.concatenate([r, t[:, ROPE_DIM:]], axis=1)

    w_in(0).wait()
    gain = 1.0 + ns_ref[...].astype(F32).reshape(1, D_MODEL)

    @pl.loop(0, BATCH // 64)
    def _(i):
        rows = pl.ds(pl.multiple_of(i * 64, 64), 64)
        xf = x_v[rows, :].astype(F32)
        mean_sq = jnp.sum(xf * xf, axis=1, keepdims=True) * (1.0 / D_MODEL)
        n_v[rows, :] = (xf * lax.rsqrt(mean_sq + EPS) * gain).astype(BF16)

    w_in(1).wait()
    w_in(2).wait()
    w_in(3).wait()

    def project(i):
        rows = pl.ds(pl.multiple_of(i * ROWS, ROWS), ROWS)
        kn_v[rows, :] = rotate(jnp.dot(n_v[rows, :], wk_v[...], preferred_element_type=F32), rows)
        vn_v[rows, :] = jnp.dot(n_v[rows, :], wv_v[...], preferred_element_type=F32)

        for h in range(HEADS):
            cols = pl.ds(h * HEAD_DIM, HEAD_DIM)
            qh = jnp.dot(n_v[rows, :], wq_v[:, cols], preferred_element_type=F32)
            q_v[rows, cols] = rotate(qh, rows) * SCORE_SCALE

    sub = lax.broadcasted_iota(jnp.int32, (GROUP, 128), 0)
    lane = lax.broadcasted_iota(jnp.int32, (GROUP, 128), 1)
    slot_c = jnp.where((lane // SLOTS) == (sub % 2), (lane % SLOTS).astype(F32) + offf, FAR)
    pick = [(sub // 2) == cc for cc in range(4)]
    iotas = [(lax.broadcasted_iota(jnp.int32, (16, HEAD_DIM), 0) + 16 * t).astype(F32).astype(BF16) for t in range(SLOTS // 16)]
    def hits_of(b):
        js = jnp.broadcast_to(js_col[pl.ds(b, 1), :], (16, 128)).astype(BF16)
        js = jnp.concatenate([js, js], axis=1)
        return [io == js for io in iotas]

    def refresh(buf, new_ref, r0):
        out = []
        for i in range(GROUP):
            b = r0 + i
            hits = hits_of(b)
            fresh = jnp.broadcast_to(new_ref[pl.ds(b, 1), :], (16, HEAD_DIM)).astype(BF16)
            for t in range(SLOTS // 16):
                piece = jnp.where(hits[t], fresh, buf[b, pl.ds(16 * t, 16), :])
                buf[b, pl.ds(16 * t, 16), :] = piece
                out.append(piece)
        return jnp.concatenate(out, axis=0)

    def scores(r0):
        rows = pl.ds(r0, GROUP)
        q = jnp.concatenate([q_v[rows, h * HEAD_DIM:(h + 1) * HEAD_DIM] for h in range(HEADS)], axis=0).astype(BF16)
        s = lax.dot_general(q, refresh(kbuf, kn_v, r0), (((1,), (1,)), ((), ())), preferred_element_type=F32)
        out = []
        for h in range(HEADS):
            sh = s[h * GROUP:(h + 1) * GROUP, :]
            c = sh[:, 384:512]
            for cc in range(3):
                c = jnp.where(pick[cc], sh[:, cc * 128:(cc + 1) * 128], c)
            out.append(c)
        return out

    def soften(r0, cs):
        rows = pl.ds(r0, GROUP)
        valid = slot_c <= p_col[rows, :]
        stats = jnp.zeros((GROUP, 128), F32)
        ps = []
        for h in range(HEADS):
            c = jnp.where(valid, cs[h], NEG_LARGE)
            m = jnp.max(c, axis=1, keepdims=True)
            e = jnp.where(valid, jnp.exp(c - m), 0.0)
            l = jnp.sum(e, axis=1, keepdims=True)
            stats = jnp.where(lane == h, m, stats)
            stats = jnp.where(lane == HEADS + h, l, stats)
            ps.append(e)
        part[rows, QW:PW] = stats
        return ps

    def values(r0, ps):
        rows = pl.ds(r0, GROUP)
        pm = jnp.concatenate([jnp.concatenate([jnp.where(pick[cc], e, 0.0) for cc in range(4)], axis=1) for e in ps], axis=0).astype(BF16)
        o = jnp.dot(pm, refresh(vbuf, vn_v, r0), preferred_element_type=F32)
        for h in range(HEADS):
            part[rows, h * HEAD_DIM:(h + 1) * HEAD_DIM] = o[h * GROUP:(h + 1) * GROUP, :]

    def attend_rows(base):
        starts = [al(base + g * GROUP, GROUP) for g in range(STEP // GROUP)]
        cs = [scores(r0) for r0 in starts]
        ps = [soften(r0, c) for r0, c in zip(starts, cs)]
        for r0, e in zip(starts, ps):
            values(r0, e)

    red = Reduce(p, part, r0, r1, r2, g, [rsems.at[i] for i in range(6)])
    gat = Gather(p, g, [gsems.at[i] for i in range(6)])

    def when_chunk(c, body):
        @pl.when((c >= 0) & (c < NCHUNK))
        def _():
            body(c)

    def attend(i):
        @pl.when(i + AHEAD < NCHUNK)
        def _():
            k_in(i + AHEAD).start()
            v_in(i + AHEAD).start()

        @pl.when(i == AHEAD)
        def _():
            w_in(4).start()

        @pl.when(i % (ROWS // CHUNK) == 0)
        def _():
            project(i // (ROWS // CHUNK))

        k_in(i).wait()
        v_in(i).wait()

        for t in range(CHUNK // STEP):
            attend_rows(i * CHUNK + t * STEP)

        @pl.when(i == 0)
        def _():
            pl.semaphore_wait(barrier, 3)

        red.copy0(i).start()

    def pair_step(c):
        red.step0(c)
        red.copy1(c).start()

    def first_step(c):
        red.step1(c)
        red.copy2(c).start()

    def second_step(c):
        red.step2(c)
        gat.copy0(c).start()

    def back_first(c):
        gat.copy0(c).wait_recv()
        gat.copy1(c).start()

    def back_second(c):
        gat.copy1(c).wait_recv()
        gat.copy2(c).start()

    bias = b_ref[...].astype(F32).reshape(1, D_MODEL)

    def project_out(c):
        gat.copy2(c).wait_recv()

        @pl.when(c == 1)
        def _():
            w_in(4).wait()

        @pl.when(c % 2 == 1)
        def _():
            rows = pl.ds(al((c - 1) * CHUNK, CHUNK), 2 * CHUNK)
            o = g[rows, :].astype(BF16)
            y = x_v[rows, :].astype(F32) + jnp.dot(o, wo_v[...], preferred_element_type=F32) + bias
            out_ref[rows, :] = y.astype(BF16)

    lags = ((0, attend), (1, pair_step), (4, first_step), (6, second_step), (8, back_first), (10, back_second), (11, project_out))

    @pl.loop(0, NCHUNK + lags[-1][0])
    def _(i):
        for lag, body in lags:
            when_chunk(i - lag, body)

    @pl.loop(0, NCHUNK)
    def _(c):
        red.drain(c)
        gat.drain(c)


def slot_kernel(pos_row, sp_ref, sp_out):
    off = lax.axis_index('kv') * SLOTS
    p_all = pos_row[...]
    slot_ids = off + lax.broadcasted_iota(jnp.int32, (SLOTS, BATCH), 0)
    sp_out[...] = jnp.where(slot_ids == (p_all & 511), p_all, sp_ref[...])


def solution(mesh):
    row_spec = P('dp', None)
    cache_spec = P('dp', 'kv', None)
    slot_spec = P('dp', 'kv')
    vec_spec = P(None)
    mat_spec = P(None, None)
    hbm = pl.BlockSpec(memory_space=pltpu.HBM)
    vmem = pl.BlockSpec(memory_space=pltpu.VMEM)

    def local_step(x_in, positions, k_cache, v_cache, slot_pos, norm_scale, w_q, w_k, w_v, w_o, b_o):
        pos_row = positions.reshape(1, BATCH)
        kbuf, vbuf, x_new = pl.pallas_call(
            step_kernel,
            out_shape=(pltpu.VMEM((BATCH, SLOTS, HEAD_DIM), BF16),
                       pltpu.VMEM((BATCH, SLOTS, HEAD_DIM), BF16),
                       pltpu.VMEM((BATCH, D_MODEL), BF16)),
            in_specs=[vmem, vmem, vmem, vmem, hbm, hbm, hbm, hbm, hbm, hbm, hbm],
            out_specs=(vmem, vmem, vmem),
            scratch_shapes=[
                pltpu.VMEM((BATCH, D_MODEL), BF16),
                pltpu.VMEM((D_MODEL, QW), BF16),
                pltpu.VMEM((D_MODEL, HEAD_DIM), BF16),
                pltpu.VMEM((D_MODEL, HEAD_DIM), BF16),
                pltpu.VMEM((QW, D_MODEL), BF16),
                pltpu.VMEM((BATCH, D_MODEL), BF16),
                pltpu.VMEM((BATCH, QW), F32),
                pltpu.VMEM((BATCH, HEAD_DIM), F32),
                pltpu.VMEM((BATCH, HEAD_DIM), F32),
                pltpu.VMEM((BATCH, 128), F32),
                pltpu.VMEM((BATCH, 128), F32),
                pltpu.VMEM((BATCH, 128), F32),
                pltpu.VMEM((BATCH, 128), F32),
                pltpu.VMEM((BATCH, PW), F32),
                pltpu.VMEM((NCHUNK * 32, PW), F32),
                pltpu.VMEM((NCHUNK * 16, PW), F32),
                pltpu.VMEM((NCHUNK * 8, PW), F32),
                pltpu.VMEM((BATCH, QW), F32),
                pltpu.SemaphoreType.DMA((5,)),
                pltpu.SemaphoreType.DMA((NCHUNK,)),
                pltpu.SemaphoreType.DMA((NCHUNK,)),
                pltpu.SemaphoreType.DMA((6, NCHUNK)),
                pltpu.SemaphoreType.DMA((6, NCHUNK)),
            ],
            cost_estimate=pl.CostEstimate(flops=5_000_000_000, bytes_accessed=40_000_000, transcendentals=200_000),
            compiler_params=pltpu.CompilerParams(collective_id=0, has_side_effects=True, vmem_limit_bytes=22 * 1024 * 1024),
        )(pos_row, jnp.asarray(inv_freq_row()), norm_scale, b_o, x_in, w_q, w_k, w_v, w_o, k_cache, v_cache)
        sp_t = pl.pallas_call(
            slot_kernel,
            out_shape=jax.ShapeDtypeStruct((SLOTS, BATCH), jnp.int32),
            in_specs=[vmem, vmem],
            out_specs=vmem,
        )(pos_row, slot_pos.T)
        return x_new, kbuf, vbuf, sp_t.T


    return jax.shard_map(
        local_step,
        mesh=mesh,
        in_specs=(row_spec, P('dp'), cache_spec, cache_spec, slot_spec, vec_spec, mat_spec, mat_spec, mat_spec, mat_spec, vec_spec),
        out_specs=(row_spec, cache_spec, cache_spec, slot_spec),
        check_vma=False)
```

```python
import functools

import jax
import jax.numpy as jnp
import numpy as np
from jax import lax
from jax.experimental import pallas as pl
from jax.experimental.pallas import tpu as pltpu
from jax.sharding import PartitionSpec as P

HEADS = 4
HEAD_DIM = 256
ROPE_DIM = 128
ROPE_HALF = ROPE_DIM // 2
ROPE_BASE = 10000.0
EPS = 1e-6
SCORE_SCALE = HEAD_DIM ** -0.5
NEG_LARGE = float(np.finfo(np.float32).min)
FAR = 1e9
F32 = jnp.float32
BF16 = jnp.bfloat16

BATCH = 512
D_MODEL = 1152
SLOTS = 64
QW = HEADS * HEAD_DIM
PW = QW + 128
GROUP = 8
STEP = 64
CHUNK = 64
AHEAD = 4
NCHUNK = BATCH // CHUNK
N_RS = 6
N_RD = NCHUNK - N_RS
ROWS = 256


def sin_cos(theta):
    k = jnp.floor(theta * np.float32(2.0 / np.pi) + 0.5)
    r = theta - k * np.float32(1.5703125)
    r = r - k * np.float32(4.83751296997070312e-4)
    r = r - k * np.float32(7.54978995489188e-8)
    r2 = r * r
    s = r + r * r2 * (-1.6666654611e-1 + r2 * (8.3321608736e-3 + r2 * -1.9515295891e-4))
    c = 1.0 - 0.5 * r2 + r2 * r2 * (4.166664568298827e-2 + r2 * (-1.388731625493765e-3 + r2 * 2.443315711809948e-5))
    q = k - 4.0 * jnp.floor(k * 0.25)
    swap = (q == 1.0) | (q == 3.0)
    sin_v = jnp.where(swap, c, s)
    cos_v = jnp.where(swap, s, c)
    sin_v = jnp.where(q >= 2.0, -sin_v, sin_v)
    cos_v = jnp.where((q == 1.0) | (q == 2.0), -cos_v, cos_v)
    return sin_v, cos_v


def inv_freq_row():
    i = np.arange(ROPE_DIM) % ROPE_HALF
    return (ROPE_BASE ** (-i / ROPE_HALF)).astype(np.float32).reshape(1, ROPE_DIM)


def merge_rows(a_rows, b_rows):
    sa, sb = a_rows[1], b_rows[1]
    lane = lax.broadcasted_iota(jnp.int32, sa.shape, 1)
    ma, mb = sa, sb
    mm = jnp.maximum(ma, mb)
    fa, fb = jnp.exp(ma - mm), jnp.exp(mb - mm)
    fa_l = pltpu.roll(fa, HEADS, 1)
    fb_l = pltpu.roll(fb, HEADS, 1)
    stats = jnp.where(lane < HEADS, mm, sa * fa_l + sb * fb_l)
    vals = []
    for h in range(HEADS):
        va = a_rows[0][:, h * HEAD_DIM:(h + 1) * HEAD_DIM]
        vb = b_rows[0][:, h * HEAD_DIM:(h + 1) * HEAD_DIM]
        vals.append(va * fa[:, h:h + 1] + vb * fb[:, h:h + 1])
    return jnp.concatenate(vals, axis=1), stats


def normalise(v, s):
    inv = 1.0 / s
    return jnp.concatenate([v[:, h * HEAD_DIM:(h + 1) * HEAD_DIM] * inv[:, HEADS + h:HEADS + h + 1] for h in range(HEADS)], axis=1)


class Places:
    def __init__(self):
        me = lax.axis_index('kv')
        self.core = me % 2
        self.x = (me // 2) % 2
        self.y = me // 4
        self.mate = me + 1 - 2 * self.core
        self.x_peer = me + 2 - 4 * self.x
        self.y_peer = me + 4 - 8 * self.y

    def first(self, c):
        odd = c % 2
        return self.x_peer + odd * (self.y_peer - self.x_peer), self.x + odd * (self.y - self.x)

    def second(self, c):
        odd = c % 2
        return self.y_peer + odd * (self.x_peer - self.y_peer), self.y + odd * (self.x - self.y)


def send(src, dst, ss, rs, peer):
    return pltpu.make_async_remote_copy(src_ref=src, dst_ref=dst, send_sem=ss, recv_sem=rs,
                                        device_id={'kv': peer}, device_id_type=pl.DeviceIdType.MESH)


def al(v, m=8):
    return pl.multiple_of(v, m)


class Reduce:
    def __init__(self, places, part, r0, r1, r2, own, sems):
        self.p = places
        self.part, self.r0, self.r1, self.r2, self.own = part, r0, r1, r2, own
        self.s0s, self.s0r, self.s1s, self.s1r, self.s2s, self.s2r = sems

    def copy0(self, c):
        src = al(c * CHUNK + 32 * (1 - self.p.core))
        return send(self.part.at[pl.ds(src, 32)], self.r0.at[pl.ds(al(c * 32), 32)], self.s0s.at[c], self.s0r.at[c], self.p.mate)

    def copy1(self, c):
        peer, k = self.p.first(c)
        src = al(c * CHUNK + 32 * self.p.core + 16 * (1 - k))
        return send(self.part.at[pl.ds(src, 16)], self.r1.at[pl.ds(al(c * 16), 16)], self.s1s.at[c], self.s1r.at[c], peer)

    def copy2(self, c):
        peer, k2 = self.p.second(c)
        k1 = self.p.first(c)[1]
        src = al(c * CHUNK + 32 * self.p.core + 16 * k1 + 8 * (1 - k2))
        return send(self.part.at[pl.ds(src, 8)], self.r2.at[pl.ds(al(c * 8), 8)], self.s2s.at[c], self.s2r.at[c], peer)

    def merge(self, mine, other_ref, theirs, n):
        a = self.part[pl.ds(mine, n), :]
        b = other_ref[pl.ds(theirs, n), :]
        return merge_rows((a[:, :QW], a[:, QW:]), (b[:, :QW], b[:, QW:]))

    def step0(self, c):
        self.copy0(c).wait_recv()
        base = al(c * CHUNK + 32 * self.p.core)
        v, s = self.merge(base, self.r0, al(c * 32), 32)
        self.part[pl.ds(base, 32), :] = jnp.concatenate([v, s], axis=1)

    def step1(self, c):
        self.copy1(c).wait_recv()
        base = al(c * CHUNK + 32 * self.p.core + 16 * self.p.first(c)[1])
        v, s = self.merge(base, self.r1, al(c * 16), 16)
        self.part[pl.ds(base, 16), :] = jnp.concatenate([v, s], axis=1)

    def step2(self, c):
        self.copy2(c).wait_recv()
        base = al(c * CHUNK + 32 * self.p.core + 16 * self.p.first(c)[1] + 8 * self.p.second(c)[1])
        v, s = self.merge(base, self.r2, al(c * 8), 8)
        self.own[pl.ds(base, 8), :] = normalise(v, s)

    def drain(self, c):
        self.copy1(c).wait_send()
        self.copy2(c).wait_send()


class Double:
    def __init__(self, places, red, mid, d1, d2, sems):
        self.p, self.red, self.mid, self.d1, self.d2 = places, red, mid, d1, d2
        self.s1s, self.s1r, self.s2s, self.s2r = sems

    def copies1(self, c):
        d = c - N_RS
        base = c * CHUNK + 32 * self.p.core
        return [send(self.red.part.at[pl.ds(al(base + 16 * t), 16)], self.d1.at[pl.ds(al(d * 32 + 16 * t), 16)],
                     self.s1s.at[2 * d + t], self.s1r.at[2 * d + t], (self.p.x_peer, self.p.y_peer)[t]) for t in range(2)]

    def copies2(self, c):
        d = c - N_RS
        return [send(self.mid.at[pl.ds(al(d * 32 + 16 * t), 16)], self.d2.at[pl.ds(al(d * 32 + 16 * t), 16)],
                     self.s2s.at[2 * d + t], self.s2r.at[2 * d + t], (self.p.y_peer, self.p.x_peer)[t]) for t in range(2)]

    def step1(self, c):
        for cp in self.copies1(c):
            cp.wait_recv()
        d = c - N_RS
        v, s = self.red.merge(al(c * CHUNK + 32 * self.p.core), self.d1, al(d * 32), 32)
        self.mid[pl.ds(al(d * 32), 32), :] = jnp.concatenate([v, s], axis=1)

    def step2(self, c):
        for cp in self.copies2(c):
            cp.wait_recv()
        rows = pl.ds(al((c - N_RS) * 32), 32)
        a, b = self.mid[rows, :], self.d2[rows, :]
        v, s = merge_rows((a[:, :QW], a[:, QW:]), (b[:, :QW], b[:, QW:]))
        self.red.own[pl.ds(al(c * CHUNK + 32 * self.p.core), 32), :] = normalise(v, s)

    def drain(self, c):
        for cp in self.copies1(c) + self.copies2(c):
            cp.wait_send()


class Gather:
    def __init__(self, places, g, sems):
        self.p, self.g = places, g
        self.s0s, self.s0r, self.s1s, self.s1r, self.s2s, self.s2r = sems

    def copy0(self, c):
        peer, k2 = self.p.second(c)
        k1 = self.p.first(c)[1]
        rows = pl.ds(al(c * CHUNK + 32 * self.p.core + 16 * k1 + 8 * k2), 8)
        return send(self.g.at[rows], self.g.at[rows], self.s0s.at[c], self.s0r.at[c], peer)

    def copy1(self, c):
        peer, k1 = self.p.first(c)
        rows = pl.ds(al(c * CHUNK + 32 * self.p.core + 16 * k1), 16)
        return send(self.g.at[rows], self.g.at[rows], self.s1s.at[c], self.s1r.at[c], peer)

    def copy2(self, c):
        rows = pl.ds(al(c * CHUNK + 32 * self.p.core), 32)
        return send(self.g.at[rows], self.g.at[rows], self.s2s.at[c], self.s2r.at[c], self.p.mate)

    def drain(self, c):
        self.copy0(c).wait_send()
        self.copy1(c).wait_send()


def step_kernel(pos_row, freq_ref, sp_ref, ns_ref, b_ref, x_hbm, wq_hbm, wk_hbm, wv_hbm, wo_hbm, k_hbm, v_hbm,
                kbuf, vbuf, out_ref, sp_out,
                x_v, wq_v, wk_v, wv_v, wo_v, n_v, q_v, kn_v, vn_v, p_col, js_col, cos_v, sin_v,
                part, r0, r1, r2, g, mid, d1, d2, w_sem, k_sem, v_sem, rsems, gsems, dsems):
    p = Places()
    barrier = pltpu.get_barrier_semaphore()
    for peer in (p.mate, p.x_peer, p.y_peer):
        pl.semaphore_signal(barrier, inc=1, device_id={'kv': peer}, device_id_type=pl.DeviceIdType.MESH)
    off = lax.axis_index('kv') * SLOTS
    weights = ((x_hbm, x_v), (wk_hbm, wk_v), (wv_hbm, wv_v), (wq_hbm, wq_v), (wo_hbm, wo_v))

    def w_in(n):
        return pltpu.make_async_copy(weights[n][0], weights[n][1], w_sem.at[n])

    def rows_of(c):
        return pl.ds(pl.multiple_of(c * CHUNK, CHUNK), CHUNK)

    def k_in(c):
        return pltpu.make_async_copy(k_hbm.at[rows_of(c)], kbuf.at[rows_of(c)], k_sem.at[c])

    def v_in(c):
        return pltpu.make_async_copy(v_hbm.at[rows_of(c)], vbuf.at[rows_of(c)], v_sem.at[c])

    for n in range(4):
        w_in(n).start()
    for c in range(AHEAD):
        k_in(c).start()
        v_in(c).start()

    offf = off.astype(F32)

    @pl.loop(0, BATCH // 128)
    def _(t):
        rows = pl.ds(pl.multiple_of(t * 128, 128), 128)
        col = jnp.broadcast_to(pos_row[:, rows].astype(F32), (128, 128)).T
        p_col[rows, :] = col
        js = col - 512.0 * jnp.floor(col * (1.0 / 512.0)) - offf
        js_col[rows, :] = jnp.where((js >= 0.0) & (js < float(SLOTS)), js, -1.0)

    @pl.loop(0, BATCH // 64)
    def _(t):
        rows = pl.ds(pl.multiple_of(t * 64, 64), 64)
        s, c = sin_cos(p_col[rows, :] * freq_ref[...])
        lane = lax.broadcasted_iota(jnp.int32, (64, 128), 1)
        sin_v[rows, :] = jnp.where(lane < ROPE_HALF, -s, s)
        cos_v[rows, :] = c

    def rotate(t, rows):
        r = t[:, :ROPE_DIM]
        r = r * cos_v[rows, :] + pltpu.roll(r, ROPE_HALF, 1) * sin_v[rows, :]
        return jnp.concatenate([r, t[:, ROPE_DIM:]], axis=1)

    w_in(0).wait()
    gain = 1.0 + ns_ref[...].astype(F32).reshape(1, D_MODEL)

    @pl.loop(0, BATCH // 64)
    def _(i):
        rows = pl.ds(pl.multiple_of(i * 64, 64), 64)
        xf = x_v[rows, :].astype(F32)
        mean_sq = jnp.sum(xf * xf, axis=1, keepdims=True) * (1.0 / D_MODEL)
        n_v[rows, :] = (xf * lax.rsqrt(mean_sq + EPS) * gain).astype(BF16)

    w_in(1).wait()
    w_in(2).wait()
    w_in(3).wait()

    def project(i):
        rows = pl.ds(pl.multiple_of(i * ROWS, ROWS), ROWS)
        kn_v[rows, :] = rotate(jnp.dot(n_v[rows, :], wk_v[...], preferred_element_type=F32), rows)
        vn_v[rows, :] = jnp.dot(n_v[rows, :], wv_v[...], preferred_element_type=F32)

        for h in range(HEADS):
            cols = pl.ds(h * HEAD_DIM, HEAD_DIM)
            qh = jnp.dot(n_v[rows, :], wq_v[:, cols], preferred_element_type=F32)
            q_v[rows, cols] = rotate(qh, rows) * SCORE_SCALE

    sub = lax.broadcasted_iota(jnp.int32, (GROUP, 128), 0)
    lane = lax.broadcasted_iota(jnp.int32, (GROUP, 128), 1)
    slot_c = jnp.where((lane // SLOTS) == (sub % 2), (lane % SLOTS).astype(F32) + offf, FAR)
    pick = [(sub // 2) == cc for cc in range(4)]
    iotas = [(lax.broadcasted_iota(jnp.int32, (16, HEAD_DIM), 0) + 16 * t).astype(F32).astype(BF16) for t in range(SLOTS // 16)]
    def hits_of(b):
        js = jnp.broadcast_to(js_col[pl.ds(b, 1), :], (16, 128)).astype(BF16)
        js = jnp.concatenate([js, js], axis=1)
        return [io == js for io in iotas]

    def refresh(buf, new_ref, r0):
        out = []
        for i in range(GROUP):
            b = r0 + i
            hits = hits_of(b)
            fresh = jnp.broadcast_to(new_ref[pl.ds(b, 1), :], (16, HEAD_DIM)).astype(BF16)
            for t in range(SLOTS // 16):
                piece = jnp.where(hits[t], fresh, buf[b, pl.ds(16 * t, 16), :])
                buf[b, pl.ds(16 * t, 16), :] = piece
                out.append(piece)
        return jnp.concatenate(out, axis=0)

    def scores(r0):
        rows = pl.ds(r0, GROUP)
        q = jnp.concatenate([q_v[rows, h * HEAD_DIM:(h + 1) * HEAD_DIM] for h in range(HEADS)], axis=0).astype(BF16)
        s = lax.dot_general(q, refresh(kbuf, kn_v, r0), (((1,), (1,)), ((), ())), preferred_element_type=F32)
        out = []
        for h in range(HEADS):
            sh = s[h * GROUP:(h + 1) * GROUP, :]
            c = sh[:, 384:512]
            for cc in range(3):
                c = jnp.where(pick[cc], sh[:, cc * 128:(cc + 1) * 128], c)
            out.append(c)
        return out

    def soften(r0, cs):
        rows = pl.ds(r0, GROUP)
        valid = slot_c <= p_col[rows, :]
        stats = jnp.zeros((GROUP, 128), F32)
        ps = []
        for h in range(HEADS):
            c = jnp.where(valid, cs[h], NEG_LARGE)
            m = jnp.max(c, axis=1, keepdims=True)
            e = jnp.where(valid, jnp.exp(c - m), 0.0)
            l = jnp.sum(e, axis=1, keepdims=True)
            stats = jnp.where(lane == h, m, stats)
            stats = jnp.where(lane == HEADS + h, l, stats)
            ps.append(e)
        part[rows, QW:PW] = stats
        return ps

    def values(r0, ps):
        rows = pl.ds(r0, GROUP)
        pm = jnp.concatenate([jnp.concatenate([jnp.where(pick[cc], e, 0.0) for cc in range(4)], axis=1) for e in ps], axis=0).astype(BF16)
        o = jnp.dot(pm, refresh(vbuf, vn_v, r0), preferred_element_type=F32)
        for h in range(HEADS):
            part[rows, h * HEAD_DIM:(h + 1) * HEAD_DIM] = o[h * GROUP:(h + 1) * GROUP, :]

    def attend_rows(base):
        starts = [al(base + g * GROUP, GROUP) for g in range(STEP // GROUP)]
        cs = [scores(r0) for r0 in starts]
        ps = [soften(r0, c) for r0, c in zip(starts, cs)]
        for r0, e in zip(starts, ps):
            values(r0, e)

    red = Reduce(p, part, r0, r1, r2, g, [rsems.at[i] for i in range(6)])
    gat = Gather(p, g, [gsems.at[i] for i in range(6)])
    dbl = Double(p, red, mid, d1, d2, [dsems.at[i] for i in range(4)])

    def when_chunk(c, body, lo=0, hi=NCHUNK):
        @pl.when((c >= lo) & (c < hi))
        def _():
            body(c)

    def attend(i):
        @pl.when(i + AHEAD < NCHUNK)
        def _():
            k_in(i + AHEAD).start()
            v_in(i + AHEAD).start()

        @pl.when(i == AHEAD)
        def _():
            w_in(4).start()

        @pl.when(i % (ROWS // CHUNK) == 0)
        def _():
            project(i // (ROWS // CHUNK))

        k_in(i).wait()
        v_in(i).wait()

        for t in range(CHUNK // STEP):
            attend_rows(i * CHUNK + t * STEP)

        @pl.when(i == 0)
        def _():
            pl.semaphore_wait(barrier, 3)

        red.copy0(i).start()

    def pair_step(c):
        red.step0(c)
        red.copy1(c).start()

    def first_step(c):
        red.step1(c)
        red.copy2(c).start()

    def second_step(c):
        red.step2(c)
        gat.copy0(c).start()

    def back_first(c):
        gat.copy0(c).wait_recv()
        gat.copy1(c).start()

    def back_second(c):
        gat.copy1(c).wait_recv()
        gat.copy2(c).start()

    bias = b_ref[...].astype(F32).reshape(1, D_MODEL)

    def project_out(c):
        gat.copy2(c).wait_recv()

        @pl.when(c % 2 == 1)
        def _():
            rows = pl.ds(al((c - 1) * CHUNK, CHUNK), 2 * CHUNK)
            o = g[rows, :].astype(BF16)
            y = x_v[rows, :].astype(F32) + jnp.dot(o, wo_v[...], preferred_element_type=F32) + bias
            out_ref[rows, :] = y.astype(BF16)

    def pair_double(c):
        red.step0(c)
        for cp in dbl.copies1(c):
            cp.start()

    def double_first(c):
        dbl.step1(c)
        for cp in dbl.copies2(c):
            cp.start()

    def double_second(c):
        dbl.step2(c)
        gat.copy2(c).start()

    p_all = pos_row[...]
    slot_ids = off + lax.broadcasted_iota(jnp.int32, (SLOTS, BATCH), 0)
    sp_out[...] = jnp.where(slot_ids == (p_all & 511), p_all, sp_ref[...])

    lags = ((0, attend, 0, NCHUNK),
            (1, pair_step, 0, N_RS), (1, pair_double, N_RS, NCHUNK),
            (4, first_step, 0, N_RS), (4, double_first, N_RS, NCHUNK),
            (7, second_step, 0, N_RS), (7, double_second, N_RS, NCHUNK),
            (10, back_first, 0, N_RS), (13, back_second, 0, N_RS),
            (15, project_out, 0, N_RS), (9, project_out, N_RS, NCHUNK))

    @pl.loop(0, max(lag + hi for lag, _, _, hi in lags))
    def _(i):
        @pl.when(i == NCHUNK + 2)
        def _():
            w_in(4).wait()

        for lag, body, lo, hi in lags:
            when_chunk(i - lag, body, lo, hi)

    @pl.loop(0, NCHUNK)
    def _(c):
        red.copy0(c).wait_send()
        gat.copy2(c).wait_send()

    @pl.loop(0, N_RS)
    def _(c):
        red.drain(c)
        gat.drain(c)

    @pl.loop(N_RS, NCHUNK)
    def _(c):
        dbl.drain(c)


def solution(mesh):
    row_spec = P('dp', None)
    cache_spec = P('dp', 'kv', None)
    slot_spec = P('dp', 'kv')
    vec_spec = P(None)
    mat_spec = P(None, None)
    hbm = pl.BlockSpec(memory_space=pltpu.HBM)
    vmem = pl.BlockSpec(memory_space=pltpu.VMEM)

    def local_step(x_in, positions, k_cache, v_cache, slot_pos, norm_scale, w_q, w_k, w_v, w_o, b_o):
        pos_row = positions.reshape(1, BATCH)
        kbuf, vbuf, x_new, sp_t = pl.pallas_call(
            step_kernel,
            out_shape=(pltpu.VMEM((BATCH, SLOTS, HEAD_DIM), BF16),
                       pltpu.VMEM((BATCH, SLOTS, HEAD_DIM), BF16),
                       pltpu.VMEM((BATCH, D_MODEL), BF16),
                       pltpu.VMEM((SLOTS, BATCH), jnp.int32)),
            in_specs=[vmem, vmem, vmem, vmem, vmem, hbm, hbm, hbm, hbm, hbm, hbm, hbm],
            out_specs=(vmem, vmem, vmem, vmem),
            scratch_shapes=[
                pltpu.VMEM((BATCH, D_MODEL), BF16),
                pltpu.VMEM((D_MODEL, QW), BF16),
                pltpu.VMEM((D_MODEL, HEAD_DIM), BF16),
                pltpu.VMEM((D_MODEL, HEAD_DIM), BF16),
                pltpu.VMEM((QW, D_MODEL), BF16),
                pltpu.VMEM((BATCH, D_MODEL), BF16),
                pltpu.VMEM((BATCH, QW), F32),
                pltpu.VMEM((BATCH, HEAD_DIM), F32),
                pltpu.VMEM((BATCH, HEAD_DIM), F32),
                pltpu.VMEM((BATCH, 128), F32),
                pltpu.VMEM((BATCH, 128), F32),
                pltpu.VMEM((BATCH, 128), F32),
                pltpu.VMEM((BATCH, 128), F32),
                pltpu.VMEM((BATCH, PW), F32),
                pltpu.VMEM((NCHUNK * 32, PW), F32),
                pltpu.VMEM((N_RS * 16, PW), F32),
                pltpu.VMEM((N_RS * 8, PW), F32),
                pltpu.VMEM((BATCH, QW), F32),
                pltpu.VMEM((N_RD * 32, PW), F32),
                pltpu.VMEM((N_RD * 32, PW), F32),
                pltpu.VMEM((N_RD * 32, PW), F32),
                pltpu.SemaphoreType.DMA((5,)),
                pltpu.SemaphoreType.DMA((NCHUNK,)),
                pltpu.SemaphoreType.DMA((NCHUNK,)),
                pltpu.SemaphoreType.DMA((6, NCHUNK)),
                pltpu.SemaphoreType.DMA((6, NCHUNK)),
                pltpu.SemaphoreType.DMA((4, 2 * N_RD)),
            ],
            cost_estimate=pl.CostEstimate(flops=5_000_000_000, bytes_accessed=40_000_000, transcendentals=200_000),
            compiler_params=pltpu.CompilerParams(collective_id=0, has_side_effects=True, vmem_limit_bytes=22 * 1024 * 1024),
        )(pos_row, jnp.asarray(inv_freq_row()), slot_pos.T, norm_scale, b_o, x_in, w_q, w_k, w_v, w_o, k_cache, v_cache)
        return x_new, kbuf, vbuf, sp_t.T


    return jax.shard_map(
        local_step,
        mesh=mesh,
        in_specs=(row_spec, P('dp'), cache_spec, cache_spec, slot_spec, vec_spec, mat_spec, mat_spec, mat_spec, mat_spec, vec_spec),
        out_specs=(row_spec, cache_spec, cache_spec, slot_spec),
        check_vma=False)
```

```python
import functools

import jax
import jax.numpy as jnp
import numpy as np
from jax import lax
from jax.experimental import pallas as pl
from jax.experimental.pallas import tpu as pltpu
from jax.sharding import PartitionSpec as P

HEADS = 4
HEAD_DIM = 256
ROPE_DIM = 128
ROPE_HALF = ROPE_DIM // 2
ROPE_BASE = 10000.0
EPS = 1e-6
SCORE_SCALE = HEAD_DIM ** -0.5
NEG_LARGE = float(np.finfo(np.float32).min)
FAR = 1e9
F32 = jnp.float32
BF16 = jnp.bfloat16

BATCH = 512
D_MODEL = 1152
SLOTS = 64
QW = HEADS * HEAD_DIM
PW = QW + 128
GROUP = 8
STEP = 64
CHUNK = 64
AHEAD = 4
NCHUNK = BATCH // CHUNK
N_RS = 6
N_RD = NCHUNK - N_RS
ROWS = 256


def sin_cos(theta):
    k = jnp.floor(theta * np.float32(2.0 / np.pi) + 0.5)
    r = theta - k * np.float32(1.5703125)
    r = r - k * np.float32(4.83751296997070312e-4)
    r = r - k * np.float32(7.54978995489188e-8)
    r2 = r * r
    s = r + r * r2 * (-1.6666654611e-1 + r2 * (8.3321608736e-3 + r2 * -1.9515295891e-4))
    c = 1.0 - 0.5 * r2 + r2 * r2 * (4.166664568298827e-2 + r2 * (-1.388731625493765e-3 + r2 * 2.443315711809948e-5))
    q = k - 4.0 * jnp.floor(k * 0.25)
    swap = (q == 1.0) | (q == 3.0)
    sin_v = jnp.where(swap, c, s)
    cos_v = jnp.where(swap, s, c)
    sin_v = jnp.where(q >= 2.0, -sin_v, sin_v)
    cos_v = jnp.where((q == 1.0) | (q == 2.0), -cos_v, cos_v)
    return sin_v, cos_v


def inv_freq_row():
    i = np.arange(ROPE_DIM) % ROPE_HALF
    return (ROPE_BASE ** (-i / ROPE_HALF)).astype(np.float32).reshape(1, ROPE_DIM)


def merge_rows(a_rows, b_rows):
    sa, sb = a_rows[1], b_rows[1]
    lane = lax.broadcasted_iota(jnp.int32, sa.shape, 1)
    ma, mb = sa, sb
    mm = jnp.maximum(ma, mb)
    fa, fb = jnp.exp(ma - mm), jnp.exp(mb - mm)
    fa_l = pltpu.roll(fa, HEADS, 1)
    fb_l = pltpu.roll(fb, HEADS, 1)
    stats = jnp.where(lane < HEADS, mm, sa * fa_l + sb * fb_l)
    vals = []
    for h in range(HEADS):
        va = a_rows[0][:, h * HEAD_DIM:(h + 1) * HEAD_DIM]
        vb = b_rows[0][:, h * HEAD_DIM:(h + 1) * HEAD_DIM]
        vals.append(va * fa[:, h:h + 1] + vb * fb[:, h:h + 1])
    return jnp.concatenate(vals, axis=1), stats


def normalise(v, s):
    inv = 1.0 / s
    return jnp.concatenate([v[:, h * HEAD_DIM:(h + 1) * HEAD_DIM] * inv[:, HEADS + h:HEADS + h + 1] for h in range(HEADS)], axis=1)


class Places:
    def __init__(self):
        me = lax.axis_index('kv')
        self.core = me % 2
        self.x = (me // 2) % 2
        self.y = me // 4
        self.mate = me + 1 - 2 * self.core
        self.x_peer = me + 2 - 4 * self.x
        self.y_peer = me + 4 - 8 * self.y

    def first(self, c):
        odd = c % 2
        return self.x_peer + odd * (self.y_peer - self.x_peer), self.x + odd * (self.y - self.x)

    def second(self, c):
        odd = c % 2
        return self.y_peer + odd * (self.x_peer - self.y_peer), self.y + odd * (self.x - self.y)


def send(src, dst, ss, rs, peer):
    return pltpu.make_async_remote_copy(src_ref=src, dst_ref=dst, send_sem=ss, recv_sem=rs,
                                        device_id={'kv': peer}, device_id_type=pl.DeviceIdType.MESH)


def al(v, m=8):
    return pl.multiple_of(v, m)


class Reduce:
    def __init__(self, places, part, r0, r1, r2, own, sems):
        self.p = places
        self.part, self.r0, self.r1, self.r2, self.own = part, r0, r1, r2, own
        self.s0s, self.s0r, self.s1s, self.s1r, self.s2s, self.s2r = sems

    def copy0(self, c):
        src = al(c * CHUNK + 32 * (1 - self.p.core))
        return send(self.part.at[pl.ds(src, 32)], self.r0.at[pl.ds(al(c * 32), 32)], self.s0s.at[c], self.s0r.at[c], self.p.mate)

    def copy1(self, c):
        peer, k = self.p.first(c)
        src = al(c * CHUNK + 32 * self.p.core + 16 * (1 - k))
        return send(self.part.at[pl.ds(src, 16)], self.r1.at[pl.ds(al(c * 16), 16)], self.s1s.at[c], self.s1r.at[c], peer)

    def copy2(self, c):
        peer, k2 = self.p.second(c)
        k1 = self.p.first(c)[1]
        src = al(c * CHUNK + 32 * self.p.core + 16 * k1 + 8 * (1 - k2))
        return send(self.part.at[pl.ds(src, 8)], self.r2.at[pl.ds(al(c * 8), 8)], self.s2s.at[c], self.s2r.at[c], peer)

    def merge(self, mine, other_ref, theirs, n):
        a = self.part[pl.ds(mine, n), :]
        b = other_ref[pl.ds(theirs, n), :]
        return merge_rows((a[:, :QW], a[:, QW:]), (b[:, :QW], b[:, QW:]))

    def step0(self, c):
        self.copy0(c).wait_recv()
        base = al(c * CHUNK + 32 * self.p.core)
        v, s = self.merge(base, self.r0, al(c * 32), 32)
        self.part[pl.ds(base, 32), :] = jnp.concatenate([v, s], axis=1)

    def step1(self, c):
        self.copy1(c).wait_recv()
        base = al(c * CHUNK + 32 * self.p.core + 16 * self.p.first(c)[1])
        v, s = self.merge(base, self.r1, al(c * 16), 16)
        self.part[pl.ds(base, 16), :] = jnp.concatenate([v, s], axis=1)

    def step2(self, c):
        self.copy2(c).wait_recv()
        base = al(c * CHUNK + 32 * self.p.core + 16 * self.p.first(c)[1] + 8 * self.p.second(c)[1])
        v, s = self.merge(base, self.r2, al(c * 8), 8)
        self.own[pl.ds(base, 8), :] = normalise(v, s)

    def drain(self, c):
        self.copy1(c).wait_send()
        self.copy2(c).wait_send()


class Double:
    def __init__(self, places, red, mid, d1, d2, sems):
        self.p, self.red, self.mid, self.d1, self.d2 = places, red, mid, d1, d2
        self.s1s, self.s1r, self.s2s, self.s2r = sems

    def copies1(self, c):
        d = c - N_RS
        base = c * CHUNK + 32 * self.p.core
        return [send(self.red.part.at[pl.ds(al(base + 16 * t), 16)], self.d1.at[pl.ds(al(d * 32 + 16 * t), 16)],
                     self.s1s.at[2 * d + t], self.s1r.at[2 * d + t], (self.p.x_peer, self.p.y_peer)[t]) for t in range(2)]

    def copies2(self, c):
        d = c - N_RS
        return [send(self.mid.at[pl.ds(al(d * 32 + 16 * t), 16)], self.d2.at[pl.ds(al(d * 32 + 16 * t), 16)],
                     self.s2s.at[2 * d + t], self.s2r.at[2 * d + t], (self.p.y_peer, self.p.x_peer)[t]) for t in range(2)]

    def step1(self, c):
        for cp in self.copies1(c):
            cp.wait_recv()
        d = c - N_RS
        v, s = self.red.merge(al(c * CHUNK + 32 * self.p.core), self.d1, al(d * 32), 32)
        self.mid[pl.ds(al(d * 32), 32), :] = jnp.concatenate([v, s], axis=1)

    def step2(self, c):
        for cp in self.copies2(c):
            cp.wait_recv()
        rows = pl.ds(al((c - N_RS) * 32), 32)
        a, b = self.mid[rows, :], self.d2[rows, :]
        v, s = merge_rows((a[:, :QW], a[:, QW:]), (b[:, :QW], b[:, QW:]))
        self.red.own[pl.ds(al(c * CHUNK + 32 * self.p.core), 32), :] = normalise(v, s)

    def drain(self, c):
        for cp in self.copies1(c) + self.copies2(c):
            cp.wait_send()


class Gather:
    def __init__(self, places, g, sems):
        self.p, self.g = places, g
        self.s0s, self.s0r, self.s1s, self.s1r, self.s2s, self.s2r = sems

    def copy0(self, c):
        peer, k2 = self.p.second(c)
        k1 = self.p.first(c)[1]
        rows = pl.ds(al(c * CHUNK + 32 * self.p.core + 16 * k1 + 8 * k2), 8)
        return send(self.g.at[rows], self.g.at[rows], self.s0s.at[c], self.s0r.at[c], peer)

    def copy1(self, c):
        peer, k1 = self.p.first(c)
        rows = pl.ds(al(c * CHUNK + 32 * self.p.core + 16 * k1), 16)
        return send(self.g.at[rows], self.g.at[rows], self.s1s.at[c], self.s1r.at[c], peer)

    def copy2(self, c):
        rows = pl.ds(al(c * CHUNK + 32 * self.p.core), 32)
        return send(self.g.at[rows], self.g.at[rows], self.s2s.at[c], self.s2r.at[c], self.p.mate)

    def drain(self, c):
        self.copy0(c).wait_send()
        self.copy1(c).wait_send()


def step_kernel(pos_row, freq_ref, sp_ref, ns_ref, b_ref, x_hbm, wq_hbm, wk_hbm, wv_hbm, wo_hbm, k_hbm, v_hbm,
                kbuf, vbuf, out_ref, sp_out,
                x_v, wq_v, wk_v, wv_v, wo_v, n_v, q_v, kn_v, vn_v, p_col, js_col, cos_v, sin_v,
                part, r0, r1, r2, g, mid, d1, d2, w_sem, k_sem, v_sem, rsems, gsems, dsems):
    p = Places()
    barrier = pltpu.get_barrier_semaphore()
    for peer in (p.mate, p.x_peer, p.y_peer):
        pl.semaphore_signal(barrier, inc=1, device_id={'kv': peer}, device_id_type=pl.DeviceIdType.MESH)
    off = lax.axis_index('kv') * SLOTS
    weights = ((x_hbm, x_v), (wk_hbm, wk_v), (wv_hbm, wv_v), (wq_hbm, wq_v), (wo_hbm, wo_v), (sp_ref, sp_out))

    def w_in(n):
        return pltpu.make_async_copy(weights[n][0], weights[n][1], w_sem.at[n])

    def rows_of(c):
        return pl.ds(pl.multiple_of(c * CHUNK, CHUNK), CHUNK)

    def k_in(c):
        return pltpu.make_async_copy(k_hbm.at[rows_of(c)], kbuf.at[rows_of(c)], k_sem.at[c])

    def v_in(c):
        return pltpu.make_async_copy(v_hbm.at[rows_of(c)], vbuf.at[rows_of(c)], v_sem.at[c])

    for n in range(4):
        w_in(n).start()
    offf = off.astype(F32)

    @pl.loop(0, BATCH // 128)
    def _(t):
        rows = pl.ds(pl.multiple_of(t * 128, 128), 128)
        col = jnp.broadcast_to(pos_row[:, rows].astype(F32), (128, 128)).T
        p_col[rows, :] = col
        js = col - 512.0 * jnp.floor(col * (1.0 / 512.0)) - offf
        js_col[rows, :] = jnp.where((js >= 0.0) & (js < float(SLOTS)), js, -1.0)

    @pl.loop(0, BATCH // 64)
    def _(t):
        rows = pl.ds(pl.multiple_of(t * 64, 64), 64)
        s, c = sin_cos(p_col[rows, :] * freq_ref[...])
        lane = lax.broadcasted_iota(jnp.int32, (64, 128), 1)
        sin_v[rows, :] = jnp.where(lane < ROPE_HALF, -s, s)
        cos_v[rows, :] = c

    def rotate(t, rows):
        r = t[:, :ROPE_DIM]
        r = r * cos_v[rows, :] + pltpu.roll(r, ROPE_HALF, 1) * sin_v[rows, :]
        return jnp.concatenate([r, t[:, ROPE_DIM:]], axis=1)

    w_in(0).wait()
    k_in(0).start()
    v_in(0).start()
    gain = 1.0 + ns_ref[...].astype(F32).reshape(1, D_MODEL)

    @pl.loop(0, BATCH // 64)
    def _(i):
        rows = pl.ds(pl.multiple_of(i * 64, 64), 64)
        xf = x_v[rows, :].astype(F32)
        mean_sq = jnp.sum(xf * xf, axis=1, keepdims=True) * (1.0 / D_MODEL)
        n_v[rows, :] = (xf * lax.rsqrt(mean_sq + EPS) * gain).astype(BF16)

    w_in(1).wait()
    w_in(2).wait()
    w_in(3).wait()
    for c in range(1, AHEAD):
        k_in(c).start()
        v_in(c).start()

    def project(i):
        rows = pl.ds(pl.multiple_of(i * ROWS, ROWS), ROWS)
        kn_v[rows, :] = rotate(jnp.dot(n_v[rows, :], wk_v[...], preferred_element_type=F32), rows)
        vn_v[rows, :] = jnp.dot(n_v[rows, :], wv_v[...], preferred_element_type=F32)

        for h in range(HEADS):
            cols = pl.ds(h * HEAD_DIM, HEAD_DIM)
            qh = jnp.dot(n_v[rows, :], wq_v[:, cols], preferred_element_type=F32)
            q_v[rows, cols] = rotate(qh, rows) * SCORE_SCALE

    sub = lax.broadcasted_iota(jnp.int32, (GROUP, 128), 0)
    lane = lax.broadcasted_iota(jnp.int32, (GROUP, 128), 1)
    slot_c = jnp.where((lane // SLOTS) == (sub % 2), (lane % SLOTS).astype(F32) + offf, FAR)
    pick = [(sub // 2) == cc for cc in range(4)]
    iotas = [(lax.broadcasted_iota(jnp.int32, (16, HEAD_DIM), 0) + 16 * t).astype(F32).astype(BF16) for t in range(SLOTS // 16)]
    def hits_of(b):
        js = jnp.broadcast_to(js_col[pl.ds(b, 1), :], (16, 128)).astype(BF16)
        js = jnp.concatenate([js, js], axis=1)
        return [io == js for io in iotas]

    def refresh(buf, new_ref, r0):
        out = []
        for i in range(GROUP):
            b = r0 + i
            hits = hits_of(b)
            fresh = jnp.broadcast_to(new_ref[pl.ds(b, 1), :], (16, HEAD_DIM)).astype(BF16)
            for t in range(SLOTS // 16):
                piece = jnp.where(hits[t], fresh, buf[b, pl.ds(16 * t, 16), :])
                buf[b, pl.ds(16 * t, 16), :] = piece
                out.append(piece)
        return jnp.concatenate(out, axis=0)

    def scores(r0):
        rows = pl.ds(r0, GROUP)
        q = jnp.concatenate([q_v[rows, h * HEAD_DIM:(h + 1) * HEAD_DIM] for h in range(HEADS)], axis=0).astype(BF16)
        s = lax.dot_general(q, refresh(kbuf, kn_v, r0), (((1,), (1,)), ((), ())), preferred_element_type=F32)
        out = []
        for h in range(HEADS):
            sh = s[h * GROUP:(h + 1) * GROUP, :]
            c = sh[:, 384:512]
            for cc in range(3):
                c = jnp.where(pick[cc], sh[:, cc * 128:(cc + 1) * 128], c)
            out.append(c)
        return out

    def soften(r0, cs):
        rows = pl.ds(r0, GROUP)
        valid = slot_c <= p_col[rows, :]
        stats = jnp.zeros((GROUP, 128), F32)
        ps = []
        for h in range(HEADS):
            c = jnp.where(valid, cs[h], NEG_LARGE)
            m = jnp.max(c, axis=1, keepdims=True)
            e = jnp.where(valid, jnp.exp(c - m), 0.0)
            l = jnp.sum(e, axis=1, keepdims=True)
            stats = jnp.where(lane == h, m, stats)
            stats = jnp.where(lane == HEADS + h, l, stats)
            ps.append(e)
        part[rows, QW:PW] = stats
        return ps

    def values(r0, ps):
        rows = pl.ds(r0, GROUP)
        pm = jnp.concatenate([jnp.concatenate([jnp.where(pick[cc], e, 0.0) for cc in range(4)], axis=1) for e in ps], axis=0).astype(BF16)
        o = jnp.dot(pm, refresh(vbuf, vn_v, r0), preferred_element_type=F32)
        for h in range(HEADS):
            part[rows, h * HEAD_DIM:(h + 1) * HEAD_DIM] = o[h * GROUP:(h + 1) * GROUP, :]

    def attend_rows(base):
        starts = [al(base + g * GROUP, GROUP) for g in range(STEP // GROUP)]
        cs = [scores(r0) for r0 in starts]
        ps = [soften(r0, c) for r0, c in zip(starts, cs)]
        for r0, e in zip(starts, ps):
            values(r0, e)

    red = Reduce(p, part, r0, r1, r2, g, [rsems.at[i] for i in range(6)])
    gat = Gather(p, g, [gsems.at[i] for i in range(6)])
    dbl = Double(p, red, mid, d1, d2, [dsems.at[i] for i in range(4)])

    def when_chunk(c, body, lo=0, hi=NCHUNK):
        @pl.when((c >= lo) & (c < hi))
        def _():
            body(c)

    def attend(i):
        @pl.when(i + AHEAD < NCHUNK)
        def _():
            k_in(i + AHEAD).start()
            v_in(i + AHEAD).start()

        @pl.when(i == AHEAD)
        def _():
            w_in(4).start()
            w_in(5).start()

        @pl.when(i % (ROWS // CHUNK) == 0)
        def _():
            project(i // (ROWS // CHUNK))

        k_in(i).wait()
        v_in(i).wait()

        for t in range(CHUNK // STEP):
            attend_rows(i * CHUNK + t * STEP)

        @pl.when(i == 0)
        def _():
            pl.semaphore_wait(barrier, 3)

        red.copy0(i).start()

    def pair_step(c):
        red.step0(c)
        red.copy1(c).start()

    def first_step(c):
        red.step1(c)
        red.copy2(c).start()

    def second_step(c):
        red.step2(c)
        gat.copy0(c).start()

    def back_first(c):
        gat.copy0(c).wait_recv()
        gat.copy1(c).start()

    def back_second(c):
        gat.copy1(c).wait_recv()
        gat.copy2(c).start()

    bias = b_ref[...].astype(F32).reshape(1, D_MODEL)

    def project_out(c):
        gat.copy2(c).wait_recv()

        @pl.when(c % 2 == 1)
        def _():
            rows = pl.ds(al((c - 1) * CHUNK, CHUNK), 2 * CHUNK)
            o = g[rows, :].astype(BF16)
            y = x_v[rows, :].astype(F32) + jnp.dot(o, wo_v[...], preferred_element_type=F32) + bias
            out_ref[rows, :] = y.astype(BF16)

    def pair_double(c):
        red.step0(c)
        for cp in dbl.copies1(c):
            cp.start()

    def double_first(c):
        dbl.step1(c)
        for cp in dbl.copies2(c):
            cp.start()

    def double_second(c):
        dbl.step2(c)
        gat.copy2(c).start()

    lags = ((0, attend, 0, NCHUNK),
            (1, pair_step, 0, N_RS), (1, pair_double, N_RS, NCHUNK),
            (4, first_step, 0, N_RS), (4, double_first, N_RS, NCHUNK),
            (7, second_step, 0, N_RS), (7, double_second, N_RS, NCHUNK),
            (10, back_first, 0, N_RS), (13, back_second, 0, N_RS),
            (15, project_out, 0, N_RS), (9, project_out, N_RS, NCHUNK))

    @pl.loop(0, max(lag + hi for lag, _, _, hi in lags))
    def _(i):
        @pl.when(i == NCHUNK + 2)
        def _():
            w_in(4).wait()
            w_in(5).wait()
            p_all = pos_row[...]
            slot_ids = off + lax.broadcasted_iota(jnp.int32, (SLOTS, BATCH), 0)
            sp_out[...] = jnp.where(slot_ids == (p_all & 511), p_all, sp_out[...])

        for lag, body, lo, hi in lags:
            when_chunk(i - lag, body, lo, hi)

    @pl.loop(0, NCHUNK)
    def _(c):
        red.copy0(c).wait_send()
        gat.copy2(c).wait_send()

    @pl.loop(0, N_RS)
    def _(c):
        red.drain(c)
        gat.drain(c)

    @pl.loop(N_RS, NCHUNK)
    def _(c):
        dbl.drain(c)


def solution(mesh):
    row_spec = P('dp', None)
    cache_spec = P('dp', 'kv', None)
    slot_spec = P('dp', 'kv')
    vec_spec = P(None)
    mat_spec = P(None, None)
    hbm = pl.BlockSpec(memory_space=pltpu.HBM)
    vmem = pl.BlockSpec(memory_space=pltpu.VMEM)

    def local_step(x_in, positions, k_cache, v_cache, slot_pos, norm_scale, w_q, w_k, w_v, w_o, b_o):
        pos_row = positions.reshape(1, BATCH)
        kbuf, vbuf, x_new, sp_t = pl.pallas_call(
            step_kernel,
            out_shape=(pltpu.VMEM((BATCH, SLOTS, HEAD_DIM), BF16),
                       pltpu.VMEM((BATCH, SLOTS, HEAD_DIM), BF16),
                       pltpu.VMEM((BATCH, D_MODEL), BF16),
                       pltpu.VMEM((SLOTS, BATCH), jnp.int32)),
            in_specs=[vmem, vmem, hbm, vmem, vmem, hbm, hbm, hbm, hbm, hbm, hbm, hbm],
            out_specs=(vmem, vmem, vmem, vmem),
            scratch_shapes=[
                pltpu.VMEM((BATCH, D_MODEL), BF16),
                pltpu.VMEM((D_MODEL, QW), BF16),
                pltpu.VMEM((D_MODEL, HEAD_DIM), BF16),
                pltpu.VMEM((D_MODEL, HEAD_DIM), BF16),
                pltpu.VMEM((QW, D_MODEL), BF16),
                pltpu.VMEM((BATCH, D_MODEL), BF16),
                pltpu.VMEM((BATCH, QW), F32),
                pltpu.VMEM((BATCH, HEAD_DIM), F32),
                pltpu.VMEM((BATCH, HEAD_DIM), F32),
                pltpu.VMEM((BATCH, 128), F32),
                pltpu.VMEM((BATCH, 128), F32),
                pltpu.VMEM((BATCH, 128), F32),
                pltpu.VMEM((BATCH, 128), F32),
                pltpu.VMEM((BATCH, PW), F32),
                pltpu.VMEM((NCHUNK * 32, PW), F32),
                pltpu.VMEM((N_RS * 16, PW), F32),
                pltpu.VMEM((N_RS * 8, PW), F32),
                pltpu.VMEM((BATCH, QW), F32),
                pltpu.VMEM((N_RD * 32, PW), F32),
                pltpu.VMEM((N_RD * 32, PW), F32),
                pltpu.VMEM((N_RD * 32, PW), F32),
                pltpu.SemaphoreType.DMA((6,)),
                pltpu.SemaphoreType.DMA((NCHUNK,)),
                pltpu.SemaphoreType.DMA((NCHUNK,)),
                pltpu.SemaphoreType.DMA((6, NCHUNK)),
                pltpu.SemaphoreType.DMA((6, NCHUNK)),
                pltpu.SemaphoreType.DMA((4, 2 * N_RD)),
            ],
            cost_estimate=pl.CostEstimate(flops=5_000_000_000, bytes_accessed=40_000_000, transcendentals=200_000),
            compiler_params=pltpu.CompilerParams(collective_id=0, has_side_effects=True, vmem_limit_bytes=22 * 1024 * 1024),
        )(pos_row, jnp.asarray(inv_freq_row()), slot_pos.T, norm_scale, b_o, x_in, w_q, w_k, w_v, w_o, k_cache, v_cache)
        return x_new, kbuf, vbuf, sp_t.T


    return jax.shard_map(
        local_step,
        mesh=mesh,
        in_specs=(row_spec, P('dp'), cache_spec, cache_spec, slot_spec, vec_spec, mat_spec, mat_spec, mat_spec, mat_spec, vec_spec),
        out_specs=(row_spec, cache_spec, cache_spec, slot_spec),
        check_vma=False)
```

```python
import functools

import jax
import jax.numpy as jnp
import numpy as np
from jax import lax
from jax.experimental import pallas as pl
from jax.experimental.pallas import tpu as pltpu
from jax.sharding import PartitionSpec as P

HEADS = 4
HEAD_DIM = 256
ROPE_DIM = 128
ROPE_HALF = ROPE_DIM // 2
ROPE_BASE = 10000.0
EPS = 1e-6
SCORE_SCALE = HEAD_DIM ** -0.5
NEG_LARGE = float(np.finfo(np.float32).min)
FAR = 1e9
F32 = jnp.float32
BF16 = jnp.bfloat16

BATCH = 512
D_MODEL = 1152
SLOTS = 64
QW = HEADS * HEAD_DIM
PW = QW + 128
GROUP = 8
STEP = 64
CHUNK = 64
AHEAD = 4
NCHUNK = BATCH // CHUNK
EARLY = 4
SPLIT = EARLY * CHUNK
LATE = BATCH - SPLIT
ROWS = 256


def sin_cos(theta):
    k = jnp.floor(theta * np.float32(2.0 / np.pi) + 0.5)
    r = theta - k * np.float32(1.5703125)
    r = r - k * np.float32(4.83751296997070312e-4)
    r = r - k * np.float32(7.54978995489188e-8)
    r2 = r * r
    s = r + r * r2 * (-1.6666654611e-1 + r2 * (8.3321608736e-3 + r2 * -1.9515295891e-4))
    c = 1.0 - 0.5 * r2 + r2 * r2 * (4.166664568298827e-2 + r2 * (-1.388731625493765e-3 + r2 * 2.443315711809948e-5))
    q = k - 4.0 * jnp.floor(k * 0.25)
    swap = (q == 1.0) | (q == 3.0)
    sin_v = jnp.where(swap, c, s)
    cos_v = jnp.where(swap, s, c)
    sin_v = jnp.where(q >= 2.0, -sin_v, sin_v)
    cos_v = jnp.where((q == 1.0) | (q == 2.0), -cos_v, cos_v)
    return sin_v, cos_v


def inv_freq_row():
    i = np.arange(ROPE_DIM) % ROPE_HALF
    return (ROPE_BASE ** (-i / ROPE_HALF)).astype(np.float32).reshape(1, ROPE_DIM)


def merge_rows(a_rows, b_rows):
    sa, sb = a_rows[1], b_rows[1]
    lane = lax.broadcasted_iota(jnp.int32, sa.shape, 1)
    ma, mb = sa, sb
    mm = jnp.maximum(ma, mb)
    fa, fb = jnp.exp(ma - mm), jnp.exp(mb - mm)
    fa_l = pltpu.roll(fa, HEADS, 1)
    fb_l = pltpu.roll(fb, HEADS, 1)
    stats = jnp.where(lane < HEADS, mm, sa * fa_l + sb * fb_l)
    vals = []
    for h in range(HEADS):
        va = a_rows[0][:, h * HEAD_DIM:(h + 1) * HEAD_DIM]
        vb = b_rows[0][:, h * HEAD_DIM:(h + 1) * HEAD_DIM]
        vals.append(va * fa[:, h:h + 1] + vb * fb[:, h:h + 1])
    return jnp.concatenate(vals, axis=1), stats


def normalise(v, s):
    inv = 1.0 / s
    return jnp.concatenate([v[:, h * HEAD_DIM:(h + 1) * HEAD_DIM] * inv[:, HEADS + h:HEADS + h + 1] for h in range(HEADS)], axis=1)


class Places:
    def __init__(self):
        me = lax.axis_index('kv')
        self.core = me % 2
        self.x = (me // 2) % 2
        self.y = me // 4
        self.mate = me + 1 - 2 * self.core
        self.x_peer = me + 2 - 4 * self.x
        self.y_peer = me + 4 - 8 * self.y

    def first(self, c):
        odd = c % 2
        return self.x_peer + odd * (self.y_peer - self.x_peer), self.x + odd * (self.y - self.x)

    def second(self, c):
        odd = c % 2
        return self.y_peer + odd * (self.x_peer - self.y_peer), self.y + odd * (self.x - self.y)


def send(src, dst, ss, rs, peer):
    return pltpu.make_async_remote_copy(src_ref=src, dst_ref=dst, send_sem=ss, recv_sem=rs,
                                        device_id={'kv': peer}, device_id_type=pl.DeviceIdType.MESH)


def al(v, m=8):
    return pl.multiple_of(v, m)


class Reduce:
    def __init__(self, places, part, r0, r1, r2, own, sems):
        self.p = places
        self.part, self.r0, self.r1, self.r2, self.own = part, r0, r1, r2, own
        self.s0s, self.s0r, self.s1s, self.s1r, self.s2s, self.s2r = sems

    def copy0(self, c):
        src = al(c * CHUNK + 32 * (1 - self.p.core))
        return send(self.part.at[pl.ds(src, 32)], self.r0.at[pl.ds(al(c * 32), 32)], self.s0s.at[c], self.s0r.at[c], self.p.mate)

    def copy1(self, c):
        peer, k = self.p.first(c)
        src = al(c * CHUNK + 32 * self.p.core + 16 * (1 - k))
        return send(self.part.at[pl.ds(src, 16)], self.r1.at[pl.ds(al(c * 16), 16)], self.s1s.at[c], self.s1r.at[c], peer)

    def copy2(self, c):
        peer, k2 = self.p.second(c)
        k1 = self.p.first(c)[1]
        src = al(c * CHUNK + 32 * self.p.core + 16 * k1 + 8 * (1 - k2))
        return send(self.part.at[pl.ds(src, 8)], self.r2.at[pl.ds(al(c * 8), 8)], self.s2s.at[c], self.s2r.at[c], peer)

    def merge(self, mine, other_ref, theirs, n):
        a = self.part[pl.ds(mine, n), :]
        b = other_ref[pl.ds(theirs, n), :]
        return merge_rows((a[:, :QW], a[:, QW:]), (b[:, :QW], b[:, QW:]))

    def step0(self, c):
        self.copy0(c).wait_recv()
        base = al(c * CHUNK + 32 * self.p.core)
        v, s = self.merge(base, self.r0, al(c * 32), 32)
        self.part[pl.ds(base, 32), :] = jnp.concatenate([v, s], axis=1)

    def step1(self, c):
        self.copy1(c).wait_recv()
        base = al(c * CHUNK + 32 * self.p.core + 16 * self.p.first(c)[1])
        v, s = self.merge(base, self.r1, al(c * 16), 16)
        self.part[pl.ds(base, 16), :] = jnp.concatenate([v, s], axis=1)

    def step2(self, c):
        self.copy2(c).wait_recv()
        base = al(c * CHUNK + 32 * self.p.core + 16 * self.p.first(c)[1] + 8 * self.p.second(c)[1])
        v, s = self.merge(base, self.r2, al(c * 8), 8)
        self.own[pl.ds(base, 8), :] = normalise(v, s)

    def drain(self, c):
        self.copy1(c).wait_send()
        self.copy2(c).wait_send()


class Gather:
    def __init__(self, places, g, sems):
        self.p, self.g = places, g
        self.s0s, self.s0r, self.s1s, self.s1r, self.s2s, self.s2r = sems

    def copy0(self, c):
        peer, k2 = self.p.second(c)
        k1 = self.p.first(c)[1]
        rows = pl.ds(al(c * CHUNK + 32 * self.p.core + 16 * k1 + 8 * k2), 8)
        return send(self.g.at[rows], self.g.at[rows], self.s0s.at[c], self.s0r.at[c], peer)

    def copy1(self, c):
        peer, k1 = self.p.first(c)
        rows = pl.ds(al(c * CHUNK + 32 * self.p.core + 16 * k1), 16)
        return send(self.g.at[rows], self.g.at[rows], self.s1s.at[c], self.s1r.at[c], peer)

    def copy2(self, c):
        rows = pl.ds(al(c * CHUNK + 32 * self.p.core), 32)
        return send(self.g.at[rows], self.g.at[rows], self.s2s.at[c], self.s2r.at[c], self.p.mate)

    def drain(self, c):
        self.copy0(c).wait_send()
        self.copy1(c).wait_send()


SLOTS_TOTAL = 37
PLAN = (
    (0, ((4, 0), (5, 4), (6, 5), (7, 6))),
    (1, ((0, 0), (1, 1), (2, 2), (3, 3), (4, 4), (5, 6), (6, 7), (7, 9))),
    (2, ()),
    (3, ((0, 7), (1, 8), (2, 9), (3, 10), (4, 11), (5, 12), (6, 13), (7, 16))),
    (4, ()),
    (5, ((0, 13), (1, 14), (2, 15), (3, 16), (4, 17), (5, 18), (6, 19), (7, 22))),
    (6, ()),
    (7, ((0, 19), (1, 20), (2, 21), (3, 22), (4, 23), (5, 24), (6, 25), (7, 27))),
    (8, ((0, 25), (1, 26), (2, 28), (3, 29), (4, 30), (5, 31), (6, 33), (7, 34))),
    (9, ((0, 27), (1, 28), (2, 30), (3, 31), (4, 32), (5, 34), (6, 35), (7, 36))),
)


class Attention:
    def __init__(self, off, kbuf, vbuf, q_v, kn_v, vn_v, p_col, js_col, part, shift):
        self.refs = kbuf, vbuf, q_v, kn_v, vn_v, p_col, js_col, part
        self.shift = shift
        self.sub = lax.broadcasted_iota(jnp.int32, (GROUP, 128), 0)
        self.lane = lax.broadcasted_iota(jnp.int32, (GROUP, 128), 1)
        self.slot_c = jnp.where((self.lane // SLOTS) == (self.sub % 2), (self.lane % SLOTS).astype(F32) + off.astype(F32), FAR)
        self.pick = [(self.sub // 2) == cc for cc in range(4)]
        self.iotas = [(lax.broadcasted_iota(jnp.int32, (16, HEAD_DIM), 0) + 16 * t).astype(F32).astype(BF16) for t in range(SLOTS // 16)]

    def rows(self, base):
        kbuf, vbuf, q_v, kn_v, vn_v, p_col, js_col, part = self.refs
        pick, iotas, lane, slot_c = self.pick, self.iotas, self.lane, self.slot_c

        def hits_of(b):
            js = jnp.broadcast_to(js_col[pl.ds(b, 1), :], (16, 128)).astype(BF16)
            js = jnp.concatenate([js, js], axis=1)
            return [io == js for io in iotas]

        def refresh(buf, new_ref, r0):
            out = []
            for i in range(GROUP):
                b = r0 + i
                hits = hits_of(b)
                fresh = jnp.broadcast_to(new_ref[pl.ds(b, 1), :], (16, HEAD_DIM)).astype(BF16)
                for t in range(SLOTS // 16):
                    piece = jnp.where(hits[t], fresh, buf[b, pl.ds(16 * t, 16), :])
                    buf[b, pl.ds(16 * t, 16), :] = piece
                    out.append(piece)
            return jnp.concatenate(out, axis=0)

        def scores(r0):
            rows = pl.ds(r0, GROUP)
            q = jnp.concatenate([q_v[rows, h * HEAD_DIM:(h + 1) * HEAD_DIM] for h in range(HEADS)], axis=0).astype(BF16)
            s = lax.dot_general(q, refresh(kbuf, kn_v, r0), (((1,), (1,)), ((), ())), preferred_element_type=F32)
            out = []
            for h in range(HEADS):
                sh = s[h * GROUP:(h + 1) * GROUP, :]
                c = sh[:, 384:512]
                for cc in range(3):
                    c = jnp.where(pick[cc], sh[:, cc * 128:(cc + 1) * 128], c)
                out.append(c)
            return out

        def soften(r0, cs):
            valid = slot_c <= p_col[pl.ds(r0, GROUP), :]
            stats = jnp.zeros((GROUP, 128), F32)
            ps = []
            for h in range(HEADS):
                c = jnp.where(valid, cs[h], NEG_LARGE)
                m = jnp.max(c, axis=1, keepdims=True)
                e = jnp.where(valid, jnp.exp(c - m), 0.0)
                l = jnp.sum(e, axis=1, keepdims=True)
                stats = jnp.where(lane == h, m, stats)
                stats = jnp.where(lane == HEADS + h, l, stats)
                ps.append(e)
            part[pl.ds(r0 + self.shift, GROUP), QW:PW] = stats
            return ps

        def values(r0, ps):
            pm = jnp.concatenate([jnp.concatenate([jnp.where(pick[cc], e, 0.0) for cc in range(4)], axis=1) for e in ps], axis=0).astype(BF16)
            o = jnp.dot(pm, refresh(vbuf, vn_v, r0), preferred_element_type=F32)
            rows = pl.ds(r0 + self.shift, GROUP)
            for h in range(HEADS):
                part[rows, h * HEAD_DIM:(h + 1) * HEAD_DIM] = o[h * GROUP:(h + 1) * GROUP, :]

        starts = [al(base + g * GROUP, GROUP) for g in range(CHUNK // GROUP)]
        cs = [scores(r0) for r0 in starts]
        ps = [soften(r0, c) for r0, c in zip(starts, cs)]
        for r0, e in zip(starts, ps):
            values(r0, e)


def chunk_rows(c):
    return pl.ds(pl.multiple_of(c * CHUNK, CHUNK), CHUNK)


def early_kernel(pos_row, freq_ref, ns_ref, sp_hbm, x_hbm, wq_hbm, wk_hbm, wv_hbm, k_hbm, v_hbm,
                 part, q_late, kn_late, vn_late, p_late, js_late, sp_out, k_out, v_out,
                 kbuf, vbuf, x_v, wq_v, wk_v, wv_v, n_v, q_v, kn_v, vn_v, p_col, js_col, cos_v, sin_v,
                 w_sem, k_sem, v_sem, ko_sem, vo_sem):
    off = lax.axis_index('kv') * SLOTS
    weights = ((x_hbm, x_v), (wk_hbm, wk_v), (wv_hbm, wv_v), (wq_hbm, wq_v), (sp_hbm, sp_out))

    def w_in(n):
        return pltpu.make_async_copy(weights[n][0], weights[n][1], w_sem.at[n])

    def kv_in(c):
        return (pltpu.make_async_copy(k_hbm.at[chunk_rows(c)], kbuf.at[chunk_rows(c)], k_sem.at[c]),
                pltpu.make_async_copy(v_hbm.at[chunk_rows(c)], vbuf.at[chunk_rows(c)], v_sem.at[c]))

    def kv_back(c):
        return (pltpu.make_async_copy(kbuf.at[chunk_rows(c)], k_out.at[chunk_rows(c)], ko_sem.at[c]),
                pltpu.make_async_copy(vbuf.at[chunk_rows(c)], v_out.at[chunk_rows(c)], vo_sem.at[c]))

    for n in range(4):
        w_in(n).start()

    offf = off.astype(F32)

    @pl.loop(0, BATCH // 128)
    def _(t):
        rows = pl.ds(pl.multiple_of(t * 128, 128), 128)
        col = jnp.broadcast_to(pos_row[:, rows].astype(F32), (128, 128)).T
        p_col[rows, :] = col
        js = col - 512.0 * jnp.floor(col * (1.0 / 512.0)) - offf
        js_col[rows, :] = jnp.where((js >= 0.0) & (js < float(SLOTS)), js, -1.0)

    @pl.loop(0, BATCH // 64)
    def _(t):
        rows = pl.ds(pl.multiple_of(t * 64, 64), 64)
        s, c = sin_cos(p_col[rows, :] * freq_ref[...])
        lane = lax.broadcasted_iota(jnp.int32, (64, 128), 1)
        sin_v[rows, :] = jnp.where(lane < ROPE_HALF, -s, s)
        cos_v[rows, :] = c

    p_late[...] = p_col[SPLIT:, :]
    js_late[...] = js_col[SPLIT:, :]

    def rotate(t, rows):
        r = t[:, :ROPE_DIM]
        r = r * cos_v[rows, :] + pltpu.roll(r, ROPE_HALF, 1) * sin_v[rows, :]
        return jnp.concatenate([r, t[:, ROPE_DIM:]], axis=1)

    w_in(0).wait()
    for cp in kv_in(0):
        cp.start()
    gain = 1.0 + ns_ref[...].astype(F32).reshape(1, D_MODEL)

    @pl.loop(0, BATCH // 64)
    def _(i):
        rows = pl.ds(pl.multiple_of(i * 64, 64), 64)
        xf = x_v[rows, :].astype(F32)
        mean_sq = jnp.sum(xf * xf, axis=1, keepdims=True) * (1.0 / D_MODEL)
        n_v[rows, :] = (xf * lax.rsqrt(mean_sq + EPS) * gain).astype(BF16)

    for n in range(1, 4):
        w_in(n).wait()
    for c in range(1, EARLY):
        for cp in kv_in(c):
            cp.start()
    w_in(4).start()

    def project(lo, n, q_to, k_to, v_to):
        rows = pl.ds(lo, n)
        k_to[...] = rotate(jnp.dot(n_v[rows, :], wk_v[...], preferred_element_type=F32), rows)
        v_to[...] = jnp.dot(n_v[rows, :], wv_v[...], preferred_element_type=F32)
        for h in range(HEADS):
            cols = pl.ds(h * HEAD_DIM, HEAD_DIM)
            qh = jnp.dot(n_v[rows, :], wq_v[:, cols], preferred_element_type=F32)
            q_to[:, cols] = rotate(qh, rows) * SCORE_SCALE

    project(0, SPLIT, q_v, kn_v, vn_v)
    att = Attention(off, kbuf, vbuf, q_v, kn_v, vn_v, p_col, js_col, part, 0)

    @pl.loop(0, EARLY)
    def _(c):
        for cp in kv_in(c):
            cp.wait()
        att.rows(c * CHUNK)
        for cp in kv_back(c):
            cp.start()

    project(SPLIT, LATE, q_late, kn_late, vn_late)
    w_in(4).wait()
    p_all = pos_row[...]
    slot_ids = off + lax.broadcasted_iota(jnp.int32, (SLOTS, BATCH), 0)
    sp_out[...] = jnp.where(slot_ids == (p_all & 511), p_all, sp_out[...])

    @pl.loop(0, EARLY)
    def _(c):
        for cp in kv_back(c):
            cp.wait()


def late_kernel(part_in, q_v, kn_v, vn_v, p_col, js_col, x_v, wo_v, b_ref, k_hbm, v_hbm,
                kbuf, vbuf, out_ref,
                part, r0, r1, r2, g, l_sem, k_sem, v_sem, rsems, gsems):
    p = Places()
    barrier = pltpu.get_barrier_semaphore()
    for peer in (p.mate, p.x_peer, p.y_peer):
        pl.semaphore_signal(barrier, inc=1, device_id={'kv': peer}, device_id_type=pl.DeviceIdType.MESH)
    off = lax.axis_index('kv') * SLOTS
    load = pltpu.make_async_copy(part_in, part.at[pl.ds(0, SPLIT)], l_sem)
    load.start()

    def kv_in(j):
        return (pltpu.make_async_copy(k_hbm.at[chunk_rows(j + EARLY)], kbuf.at[chunk_rows(j)], k_sem.at[j]),
                pltpu.make_async_copy(v_hbm.at[chunk_rows(j + EARLY)], vbuf.at[chunk_rows(j)], v_sem.at[j]))

    for cp in kv_in(0):
        cp.start()
    load.wait()
    red = Reduce(p, part, r0, r1, r2, g, [rsems.at[i] for i in range(6)])
    gat = Gather(p, g, [gsems.at[i] for i in range(6)])
    att = Attention(off, kbuf, vbuf, q_v, kn_v, vn_v, p_col, js_col, part, SPLIT)
    pl.semaphore_wait(barrier, 3)

    @pl.loop(0, EARLY)
    def _(c):
        red.copy0(c).start()

    for j in range(1, NCHUNK - EARLY):
        for cp in kv_in(j):
            cp.start()

    def when_chunk(c, body, lo=0, hi=NCHUNK):
        @pl.when((c >= lo) & (c < hi))
        def _():
            body(c)

    def attend(c):
        for cp in kv_in(c - EARLY):
            cp.wait()
        att.rows((c - EARLY) * CHUNK)
        red.copy0(c).start()

    def pair_step(c):
        red.step0(c)
        red.copy1(c).start()

    def first_step(c):
        red.step1(c)
        red.copy2(c).start()

    def second_step(c):
        red.step2(c)
        gat.copy0(c).start()

    def back_first(c):
        gat.copy0(c).wait_recv()
        gat.copy1(c).start()

    def back_second(c):
        gat.copy1(c).wait_recv()
        gat.copy2(c).start()

    bias = b_ref[...].astype(F32).reshape(1, D_MODEL)

    def project_out(c):
        gat.copy2(c).wait_recv()

        @pl.when(c % 2 == 1)
        def _():
            rows = pl.ds(al((c - 1) * CHUNK, CHUNK), 2 * CHUNK)
            o = g[rows, :].astype(BF16)
            y = x_v[rows, :].astype(F32) + jnp.dot(o, wo_v[...], preferred_element_type=F32) + bias
            out_ref[rows, :] = y.astype(BF16)

    stages = (attend, pair_step, None, first_step, None, second_step, None, back_first, back_second, project_out)
    plan = [(stages[n], at) for n, at in PLAN if at]

    @pl.loop(0, SLOTS_TOTAL)
    def _(i):
        for body, at in plan:
            lo, hi = at[0][0], at[-1][0] + 1
            c = lo
            live = i == at[0][1]
            for k, slot in at[1:]:
                c = c + jnp.where(i >= slot, 1, 0)
                live = live | (i == slot)

            @pl.when(live)
            def _(body=body, c=c):
                body(c)

    @pl.loop(0, NCHUNK)
    def _(c):
        red.copy0(c).wait_send()
        gat.copy2(c).wait_send()

    @pl.loop(0, NCHUNK)
    def _(c):
        red.drain(c)
        gat.drain(c)


def solution(mesh):
    row_spec = P('dp', None)
    cache_spec = P('dp', 'kv', None)
    slot_spec = P('dp', 'kv')
    vec_spec = P(None)
    mat_spec = P(None, None)
    hbm = pl.BlockSpec(memory_space=pltpu.HBM)
    vmem = pl.BlockSpec(memory_space=pltpu.VMEM)

    def local_step(x_in, positions, k_cache, v_cache, slot_pos, norm_scale, w_q, w_k, w_v, w_o, b_o):
        part, q_late, kn_late, vn_late, p_late, js_late, sp_t, k_mid, v_mid = pl.pallas_call(
            early_kernel,
            out_shape=(jax.ShapeDtypeStruct((SPLIT, PW), F32),
                       jax.ShapeDtypeStruct((LATE, QW), F32),
                       jax.ShapeDtypeStruct((LATE, HEAD_DIM), F32),
                       jax.ShapeDtypeStruct((LATE, HEAD_DIM), F32),
                       jax.ShapeDtypeStruct((LATE, 128), F32),
                       jax.ShapeDtypeStruct((LATE, 128), F32),
                       jax.ShapeDtypeStruct((SLOTS, BATCH), jnp.int32),
                       jax.ShapeDtypeStruct(k_cache.shape, BF16),
                       jax.ShapeDtypeStruct(v_cache.shape, BF16)),
            in_specs=[vmem, vmem, vmem, hbm, hbm, hbm, hbm, hbm, hbm, hbm],
            out_specs=(vmem, vmem, vmem, vmem, vmem, vmem, vmem, hbm, hbm),
            scratch_shapes=[
                pltpu.VMEM((SPLIT, SLOTS, HEAD_DIM), BF16),
                pltpu.VMEM((SPLIT, SLOTS, HEAD_DIM), BF16),
                pltpu.VMEM((BATCH, D_MODEL), BF16),
                pltpu.VMEM((D_MODEL, QW), BF16),
                pltpu.VMEM((D_MODEL, HEAD_DIM), BF16),
                pltpu.VMEM((D_MODEL, HEAD_DIM), BF16),
                pltpu.VMEM((BATCH, D_MODEL), BF16),
                pltpu.VMEM((SPLIT, QW), F32),
                pltpu.VMEM((SPLIT, HEAD_DIM), F32),
                pltpu.VMEM((SPLIT, HEAD_DIM), F32),
                pltpu.VMEM((BATCH, 128), F32),
                pltpu.VMEM((BATCH, 128), F32),
                pltpu.VMEM((BATCH, 128), F32),
                pltpu.VMEM((BATCH, 128), F32),
                pltpu.SemaphoreType.DMA((5,)),
                pltpu.SemaphoreType.DMA((EARLY,)),
                pltpu.SemaphoreType.DMA((EARLY,)),
                pltpu.SemaphoreType.DMA((EARLY,)),
                pltpu.SemaphoreType.DMA((EARLY,)),
            ],
            cost_estimate=pl.CostEstimate(flops=3_000_000_000, bytes_accessed=40_000_000, transcendentals=100_000),
            compiler_params=pltpu.CompilerParams(vmem_limit_bytes=40 * 1024 * 1024),
        )(positions.reshape(1, BATCH), jnp.asarray(inv_freq_row()), norm_scale, *[pltpu.with_memory_space_constraint(a, pltpu.HBM) for a in (slot_pos.T, x_in, w_q, w_k, w_v, k_cache, v_cache)])
        k_new, v_new, x_out = pl.pallas_call(
            late_kernel,
            out_shape=(pltpu.VMEM((LATE, SLOTS, HEAD_DIM), BF16),
                       pltpu.VMEM((LATE, SLOTS, HEAD_DIM), BF16),
                       pltpu.VMEM((BATCH, D_MODEL), BF16)),
            in_specs=[pl.BlockSpec(memory_space=pl.ANY)] + [vmem] * 8 + [hbm, hbm],
            out_specs=(vmem, vmem, vmem),
            scratch_shapes=[
                pltpu.VMEM((BATCH, PW), F32),
                pltpu.VMEM((NCHUNK * 32, PW), F32),
                pltpu.VMEM((NCHUNK * 16, PW), F32),
                pltpu.VMEM((NCHUNK * 8, PW), F32),
                pltpu.VMEM((BATCH, QW), F32),
                pltpu.SemaphoreType.DMA,
                pltpu.SemaphoreType.DMA((NCHUNK - EARLY,)),
                pltpu.SemaphoreType.DMA((NCHUNK - EARLY,)),
                pltpu.SemaphoreType.DMA((6, NCHUNK)),
                pltpu.SemaphoreType.DMA((6, NCHUNK)),
            ],
            cost_estimate=pl.CostEstimate(flops=3_000_000_000, bytes_accessed=20_000_000, transcendentals=100_000),
            compiler_params=pltpu.CompilerParams(collective_id=0, has_side_effects=True, vmem_limit_bytes=24 * 1024 * 1024),
        )(part, q_late, kn_late, vn_late, p_late, js_late, x_in, w_o, b_o, k_cache, v_cache)
        k_out = lax.dynamic_update_slice(k_mid, k_new, (SPLIT, 0, 0))
        v_out = lax.dynamic_update_slice(v_mid, v_new, (SPLIT, 0, 0))
        return x_out, k_out, v_out, sp_t.T

    return jax.shard_map(
        local_step,
        mesh=mesh,
        in_specs=(row_spec, P('dp'), cache_spec, cache_spec, slot_spec, vec_spec, mat_spec, mat_spec, mat_spec, mat_spec, vec_spec),
        out_specs=(row_spec, cache_spec, cache_spec, slot_spec),
        check_vma=False)
```

```python
import functools

import jax
import jax.numpy as jnp
import numpy as np
from jax import lax
from jax.experimental import pallas as pl
from jax.experimental.pallas import tpu as pltpu
from jax.sharding import PartitionSpec as P

HEADS = 4
HEAD_DIM = 256
ROPE_DIM = 128
ROPE_HALF = ROPE_DIM // 2
ROPE_BASE = 10000.0
EPS = 1e-6
SCORE_SCALE = HEAD_DIM ** -0.5
NEG_LARGE = float(np.finfo(np.float32).min)
FAR = 1e9
F32 = jnp.float32
BF16 = jnp.bfloat16

BATCH = 512
D_MODEL = 1152
SLOTS = 64
QW = HEADS * HEAD_DIM
PW = QW + 128
GROUP = 8
STEP = 64
CHUNK = 64
AHEAD = 4
NCHUNK = BATCH // CHUNK
ROWS = 256


def sin_cos(theta):
    k = jnp.floor(theta * np.float32(2.0 / np.pi) + 0.5)
    r = theta - k * np.float32(1.5703125)
    r = r - k * np.float32(4.83751296997070312e-4)
    r = r - k * np.float32(7.54978995489188e-8)
    r2 = r * r
    s = r + r * r2 * (-1.6666654611e-1 + r2 * (8.3321608736e-3 + r2 * -1.9515295891e-4))
    c = 1.0 - 0.5 * r2 + r2 * r2 * (4.166664568298827e-2 + r2 * (-1.388731625493765e-3 + r2 * 2.443315711809948e-5))
    q = k - 4.0 * jnp.floor(k * 0.25)
    swap = (q == 1.0) | (q == 3.0)
    sin_v = jnp.where(swap, c, s)
    cos_v = jnp.where(swap, s, c)
    sin_v = jnp.where(q >= 2.0, -sin_v, sin_v)
    cos_v = jnp.where((q == 1.0) | (q == 2.0), -cos_v, cos_v)
    return sin_v, cos_v


def inv_freq_row():
    i = np.arange(ROPE_DIM) % ROPE_HALF
    return (ROPE_BASE ** (-i / ROPE_HALF)).astype(np.float32).reshape(1, ROPE_DIM)


def merge_rows(a_rows, b_rows):
    sa, sb = a_rows[1], b_rows[1]
    lane = lax.broadcasted_iota(jnp.int32, sa.shape, 1)
    ma, mb = sa, sb
    mm = jnp.maximum(ma, mb)
    fa, fb = jnp.exp(ma - mm), jnp.exp(mb - mm)
    fa_l = pltpu.roll(fa, HEADS, 1)
    fb_l = pltpu.roll(fb, HEADS, 1)
    stats = jnp.where(lane < HEADS, mm, sa * fa_l + sb * fb_l)
    vals = []
    for h in range(HEADS):
        va = a_rows[0][:, h * HEAD_DIM:(h + 1) * HEAD_DIM]
        vb = b_rows[0][:, h * HEAD_DIM:(h + 1) * HEAD_DIM]
        vals.append(va * fa[:, h:h + 1] + vb * fb[:, h:h + 1])
    return jnp.concatenate(vals, axis=1), stats


def normalise(v, s):
    inv = 1.0 / s
    return jnp.concatenate([v[:, h * HEAD_DIM:(h + 1) * HEAD_DIM] * inv[:, HEADS + h:HEADS + h + 1] for h in range(HEADS)], axis=1)


class Places:
    def __init__(self):
        me = lax.axis_index('kv')
        self.core = me % 2
        self.x = (me // 2) % 2
        self.y = me // 4
        self.mate = me + 1 - 2 * self.core
        self.x_peer = me + 2 - 4 * self.x
        self.y_peer = me + 4 - 8 * self.y

    def first(self, c):
        odd = c % 2
        return self.x_peer + odd * (self.y_peer - self.x_peer), self.x + odd * (self.y - self.x)

    def second(self, c):
        odd = c % 2
        return self.y_peer + odd * (self.x_peer - self.y_peer), self.y + odd * (self.x - self.y)


def send(src, dst, ss, rs, peer):
    return pltpu.make_async_remote_copy(src_ref=src, dst_ref=dst, send_sem=ss, recv_sem=rs,
                                        device_id={'kv': peer}, device_id_type=pl.DeviceIdType.MESH)


def al(v, m=8):
    return pl.multiple_of(v, m)


class Reduce:
    def __init__(self, places, part, r0, r1, r2, own, sems):
        self.p = places
        self.part, self.r0, self.r1, self.r2, self.own = part, r0, r1, r2, own
        self.s0s, self.s0r, self.s1s, self.s1r, self.s2s, self.s2r = sems

    def copy0(self, c):
        src = al(c * CHUNK + 32 * (1 - self.p.core))
        return send(self.part.at[pl.ds(src, 32)], self.r0.at[pl.ds(al(c * 32), 32)], self.s0s.at[c], self.s0r.at[c], self.p.mate)

    def copy1(self, c):
        peer, k = self.p.first(c)
        src = al(c * CHUNK + 32 * self.p.core + 16 * (1 - k))
        return send(self.part.at[pl.ds(src, 16)], self.r1.at[pl.ds(al(c * 16), 16)], self.s1s.at[c], self.s1r.at[c], peer)

    def copy2(self, c):
        peer, k2 = self.p.second(c)
        k1 = self.p.first(c)[1]
        src = al(c * CHUNK + 32 * self.p.core + 16 * k1 + 8 * (1 - k2))
        return send(self.part.at[pl.ds(src, 8)], self.r2.at[pl.ds(al(c * 8), 8)], self.s2s.at[c], self.s2r.at[c], peer)

    def merge(self, mine, other_ref, theirs, n):
        a = self.part[pl.ds(mine, n), :]
        b = other_ref[pl.ds(theirs, n), :]
        return merge_rows((a[:, :QW], a[:, QW:]), (b[:, :QW], b[:, QW:]))

    def step0(self, c):
        self.copy0(c).wait_recv()
        base = al(c * CHUNK + 32 * self.p.core)
        v, s = self.merge(base, self.r0, al(c * 32), 32)
        self.part[pl.ds(base, 32), :] = jnp.concatenate([v, s], axis=1)

    def step1(self, c):
        self.copy1(c).wait_recv()
        base = al(c * CHUNK + 32 * self.p.core + 16 * self.p.first(c)[1])
        v, s = self.merge(base, self.r1, al(c * 16), 16)
        self.part[pl.ds(base, 16), :] = jnp.concatenate([v, s], axis=1)

    def step2(self, c):
        self.copy2(c).wait_recv()
        base = al(c * CHUNK + 32 * self.p.core + 16 * self.p.first(c)[1] + 8 * self.p.second(c)[1])
        v, s = self.merge(base, self.r2, al(c * 8), 8)
        self.own[pl.ds(al(c * 8), 8), :] = normalise(v, s)

    def drain(self, c):
        self.copy1(c).wait_send()
        self.copy2(c).wait_send()


class Attention:
    def __init__(self, off, kbuf, vbuf, q_v, kn_v, vn_v, p_col, js_col, part):
        self.refs = kbuf, vbuf, q_v, kn_v, vn_v, p_col, js_col, part
        self.sub = lax.broadcasted_iota(jnp.int32, (GROUP, 128), 0)
        self.lane = lax.broadcasted_iota(jnp.int32, (GROUP, 128), 1)
        self.slot_c = jnp.where((self.lane // SLOTS) == (self.sub % 2), (self.lane % SLOTS).astype(F32) + off.astype(F32), FAR)
        self.pick = [(self.sub // 2) == cc for cc in range(4)]
        self.iotas = [(lax.broadcasted_iota(jnp.int32, (16, HEAD_DIM), 0) + 16 * t).astype(F32).astype(BF16) for t in range(SLOTS // 16)]

    def rows(self, base):
        kbuf, vbuf, q_v, kn_v, vn_v, p_col, js_col, part = self.refs
        pick, iotas, lane, slot_c = self.pick, self.iotas, self.lane, self.slot_c

        def hits_of(b):
            js = jnp.broadcast_to(js_col[pl.ds(b, 1), :], (16, 128)).astype(BF16)
            js = jnp.concatenate([js, js], axis=1)
            return [io == js for io in iotas]

        def refresh(buf, new_ref, r0):
            out = []
            for i in range(GROUP):
                b = r0 + i
                hits = hits_of(b)
                fresh = jnp.broadcast_to(new_ref[pl.ds(b, 1), :], (16, HEAD_DIM)).astype(BF16)
                for t in range(SLOTS // 16):
                    piece = jnp.where(hits[t], fresh, buf[b, pl.ds(16 * t, 16), :])
                    buf[b, pl.ds(16 * t, 16), :] = piece
                    out.append(piece)
            return jnp.concatenate(out, axis=0)

        def scores(r0):
            rows = pl.ds(r0, GROUP)
            q = jnp.concatenate([q_v[rows, h * HEAD_DIM:(h + 1) * HEAD_DIM] for h in range(HEADS)], axis=0).astype(BF16)
            s = lax.dot_general(q, refresh(kbuf, kn_v, r0), (((1,), (1,)), ((), ())), preferred_element_type=F32)
            out = []
            for h in range(HEADS):
                sh = s[h * GROUP:(h + 1) * GROUP, :]
                c = sh[:, 384:512]
                for cc in range(3):
                    c = jnp.where(pick[cc], sh[:, cc * 128:(cc + 1) * 128], c)
                out.append(c)
            return out

        def soften(r0, cs):
            valid = slot_c <= p_col[pl.ds(r0, GROUP), :]
            stats = jnp.zeros((GROUP, 128), F32)
            ps = []
            for h in range(HEADS):
                c = jnp.where(valid, cs[h], NEG_LARGE)
                m = jnp.max(c, axis=1, keepdims=True)
                e = jnp.where(valid, jnp.exp(c - m), 0.0)
                l = jnp.sum(e, axis=1, keepdims=True)
                stats = jnp.where(lane == h, m, stats)
                stats = jnp.where(lane == HEADS + h, l, stats)
                ps.append(e)
            part[pl.ds(r0, GROUP), QW:PW] = stats
            return ps

        def values(r0, ps):
            pm = jnp.concatenate([jnp.concatenate([jnp.where(pick[cc], e, 0.0) for cc in range(4)], axis=1) for e in ps], axis=0).astype(BF16)
            o = jnp.dot(pm, refresh(vbuf, vn_v, r0), preferred_element_type=F32)
            rows = pl.ds(r0, GROUP)
            for h in range(HEADS):
                part[rows, h * HEAD_DIM:(h + 1) * HEAD_DIM] = o[h * GROUP:(h + 1) * GROUP, :]

        starts = [al(base + g * GROUP, GROUP) for g in range(CHUNK // GROUP)]
        cs = [scores(r0) for r0 in starts]
        ps = [soften(r0, c) for r0, c in zip(starts, cs)]
        for r0, e in zip(starts, ps):
            values(r0, e)


def chunk_rows(c):
    return pl.ds(pl.multiple_of(c * CHUNK, CHUNK), CHUNK)


def step_kernel(pos_row, freq_ref, ns_ref, sp_hbm, x_hbm, wq_hbm, wk_hbm, wv_hbm, k_hbm, v_hbm,
                own, kbuf, vbuf, sp_out,
                x_v, wq_v, wk_v, wv_v, n_v, q_v, kn_v, vn_v, p_col, js_col, cos_v, sin_v,
                part, r0, r1, r2, w_sem, k_sem, v_sem, rsems):
    p = Places()
    barrier = pltpu.get_barrier_semaphore()
    for peer in (p.mate, p.x_peer, p.y_peer):
        pl.semaphore_signal(barrier, inc=1, device_id={'kv': peer}, device_id_type=pl.DeviceIdType.MESH)
    off = lax.axis_index('kv') * SLOTS
    weights = ((x_hbm, x_v), (wk_hbm, wk_v), (wv_hbm, wv_v), (wq_hbm, wq_v), (sp_hbm, sp_out))

    def w_in(n):
        return pltpu.make_async_copy(weights[n][0], weights[n][1], w_sem.at[n])

    def kv_in(c):
        return (pltpu.make_async_copy(k_hbm.at[chunk_rows(c)], kbuf.at[chunk_rows(c)], k_sem.at[c]),
                pltpu.make_async_copy(v_hbm.at[chunk_rows(c)], vbuf.at[chunk_rows(c)], v_sem.at[c]))

    for n in range(4):
        w_in(n).start()

    offf = off.astype(F32)

    @pl.loop(0, BATCH // 128)
    def _(t):
        rows = pl.ds(pl.multiple_of(t * 128, 128), 128)
        col = jnp.broadcast_to(pos_row[:, rows].astype(F32), (128, 128)).T
        p_col[rows, :] = col
        js = col - 512.0 * jnp.floor(col * (1.0 / 512.0)) - offf
        js_col[rows, :] = jnp.where((js >= 0.0) & (js < float(SLOTS)), js, -1.0)

    @pl.loop(0, BATCH // 64)
    def _(t):
        rows = pl.ds(pl.multiple_of(t * 64, 64), 64)
        s, c = sin_cos(p_col[rows, :] * freq_ref[...])
        lane = lax.broadcasted_iota(jnp.int32, (64, 128), 1)
        sin_v[rows, :] = jnp.where(lane < ROPE_HALF, -s, s)
        cos_v[rows, :] = c

    def rotate(t, rows):
        r = t[:, :ROPE_DIM]
        r = r * cos_v[rows, :] + pltpu.roll(r, ROPE_HALF, 1) * sin_v[rows, :]
        return jnp.concatenate([r, t[:, ROPE_DIM:]], axis=1)

    w_in(0).wait()
    for cp in kv_in(0):
        cp.start()
    gain = 1.0 + ns_ref[...].astype(F32).reshape(1, D_MODEL)

    @pl.loop(0, BATCH // 64)
    def _(i):
        rows = pl.ds(pl.multiple_of(i * 64, 64), 64)
        xf = x_v[rows, :].astype(F32)
        mean_sq = jnp.sum(xf * xf, axis=1, keepdims=True) * (1.0 / D_MODEL)
        n_v[rows, :] = (xf * lax.rsqrt(mean_sq + EPS) * gain).astype(BF16)

    for n in range(1, 4):
        w_in(n).wait()
    for c in range(1, AHEAD):
        for cp in kv_in(c):
            cp.start()
    red = Reduce(p, part, r0, r1, r2, own, [rsems.at[i] for i in range(6)])
    att = Attention(off, kbuf, vbuf, q_v, kn_v, vn_v, p_col, js_col, part)

    def attend(c):
        @pl.when(c + AHEAD < NCHUNK)
        def _():
            for cp in kv_in(c + AHEAD):
                cp.start()

        @pl.when(c == AHEAD)
        def _():
            w_in(4).start()

        @pl.when(c % (ROWS // CHUNK) == 0)
        def _():
            rows = pl.ds(al(c * CHUNK, ROWS), ROWS)
            kn_v[rows, :] = rotate(jnp.dot(n_v[rows, :], wk_v[...], preferred_element_type=F32), rows)
            vn_v[rows, :] = jnp.dot(n_v[rows, :], wv_v[...], preferred_element_type=F32)
            for h in range(HEADS):
                cols = pl.ds(h * HEAD_DIM, HEAD_DIM)
                qh = jnp.dot(n_v[rows, :], wq_v[:, cols], preferred_element_type=F32)
                q_v[rows, cols] = rotate(qh, rows) * SCORE_SCALE

        for cp in kv_in(c):
            cp.wait()
        att.rows(c * CHUNK)

        @pl.when(c == 0)
        def _():
            pl.semaphore_wait(barrier, 3)

        red.copy0(c).start()

    def pair_step(c):
        red.step0(c)
        red.copy1(c).start()

    def first_step(c):
        red.step1(c)
        red.copy2(c).start()

    lags = ((0, attend), (1, pair_step), (3, first_step), (5, red.step2))

    @pl.loop(0, NCHUNK + lags[-1][0])
    def _(i):
        for lag, body in lags:
            @pl.when((i >= lag) & (i < NCHUNK + lag))
            def _(lag=lag, body=body):
                body(i - lag)

    w_in(4).wait()
    p_all = pos_row[...]
    slot_ids = off + lax.broadcasted_iota(jnp.int32, (SLOTS, BATCH), 0)
    sp_out[...] = jnp.where(slot_ids == (p_all & 511), p_all, sp_out[...])

    @pl.loop(0, NCHUNK)
    def _(c):
        red.copy0(c).wait_send()
        red.drain(c)


def out_kernel(own, from_x, from_y, from_d, x_v, wo_v, b_ref, out_ref, g, lsem, ssem, rsem):
    p = Places()
    barrier = pltpu.get_barrier_semaphore()
    pl.semaphore_signal(barrier, inc=1, device_id={'kv': p.mate}, device_id_type=pl.DeviceIdType.MESH)
    refs = (own, from_x, from_y, from_d)

    def copy(n):
        return send(refs[n], g.at[n], ssem.at[n], rsem.at[n], p.mate)

    pl.semaphore_wait(barrier, 1)
    for n in range(4):
        copy(n).start()
    bias = b_ref[...].astype(F32).reshape(1, D_MODEL)

    def rows_of(n, t, core):
        x = p.x + (n % 2) * (1 - 2 * p.x)
        y = p.y + (n // 2) * (1 - 2 * p.y)
        a, b = (x, y) if t % 2 == 0 else (y, x)
        return al(t * CHUNK + 32 * core + 16 * a + 8 * b)

    def emit(n, ref, core):
        rows = [rows_of(n, t, core) for t in range(NCHUNK)]
        xin = jnp.concatenate([x_v[pl.ds(r, 8), :].astype(F32) for r in rows], axis=0)
        y = xin + jnp.dot(ref[...].astype(BF16), wo_v[...], preferred_element_type=F32) + bias
        for t, r in enumerate(rows):
            out_ref[pl.ds(r, 8), :] = y[8 * t:8 * t + 8, :]

    for n in range(4):
        emit(n, refs[n], p.core)
    for n in range(4):
        copy(n).wait_recv()
        emit(n, g.at[n], 1 - p.core)
    for n in range(4):
        copy(n).wait_send()


def solution(mesh):
    row_spec = P('dp', None)
    cache_spec = P('dp', 'kv', None)
    slot_spec = P('dp', 'kv')
    vec_spec = P(None)
    mat_spec = P(None, None)
    hbm = pl.BlockSpec(memory_space=pltpu.HBM)
    vmem = pl.BlockSpec(memory_space=pltpu.VMEM)

    def in_hbm(a):
        return pltpu.with_memory_space_constraint(a, pltpu.HBM)

    def local_step(x_in, positions, k_cache, v_cache, slot_pos, norm_scale, w_q, w_k, w_v, w_o, b_o):
        own, k_out, v_out, sp_t = pl.pallas_call(
            step_kernel,
            out_shape=(jax.ShapeDtypeStruct((BATCH // 8, QW), F32),
                       pltpu.VMEM((BATCH, SLOTS, HEAD_DIM), BF16),
                       pltpu.VMEM((BATCH, SLOTS, HEAD_DIM), BF16),
                       pltpu.VMEM((SLOTS, BATCH), jnp.int32)),
            in_specs=[vmem, vmem, vmem] + [hbm] * 7,
            out_specs=(vmem,) * 4,
            scratch_shapes=[
                pltpu.VMEM((BATCH, D_MODEL), BF16),
                pltpu.VMEM((D_MODEL, QW), BF16),
                pltpu.VMEM((D_MODEL, HEAD_DIM), BF16),
                pltpu.VMEM((D_MODEL, HEAD_DIM), BF16),
                pltpu.VMEM((BATCH, D_MODEL), BF16),
                pltpu.VMEM((BATCH, QW), F32),
                pltpu.VMEM((BATCH, HEAD_DIM), F32),
                pltpu.VMEM((BATCH, HEAD_DIM), F32),
                pltpu.VMEM((BATCH, 128), F32),
                pltpu.VMEM((BATCH, 128), F32),
                pltpu.VMEM((BATCH, 128), F32),
                pltpu.VMEM((BATCH, 128), F32),
                pltpu.VMEM((BATCH, PW), F32),
                pltpu.VMEM((NCHUNK * 32, PW), F32),
                pltpu.VMEM((NCHUNK * 16, PW), F32),
                pltpu.VMEM((NCHUNK * 8, PW), F32),
                pltpu.SemaphoreType.DMA((5,)),
                pltpu.SemaphoreType.DMA((NCHUNK,)),
                pltpu.SemaphoreType.DMA((NCHUNK,)),
                pltpu.SemaphoreType.DMA((6, NCHUNK)),
            ],
            cost_estimate=pl.CostEstimate(flops=30_000_000_000, bytes_accessed=40_000_000, transcendentals=200_000),
            compiler_params=pltpu.CompilerParams(collective_id=0, has_side_effects=True, vmem_limit_bytes=20 * 1024 * 1024),
        )(positions.reshape(1, BATCH), jnp.asarray(inv_freq_row()), norm_scale,
          *[in_hbm(a) for a in (slot_pos.T, x_in, w_q, w_k, w_v, k_cache, v_cache)])
        far = [lax.ppermute(own, 'kv', [(i, i ^ m) for i in range(8)]) for m in (2, 4, 6)]
        x_out = pl.pallas_call(
            out_kernel,
            out_shape=jax.ShapeDtypeStruct((BATCH, D_MODEL), F32),
            in_specs=[vmem] * 7,
            out_specs=vmem,
            scratch_shapes=[
                pltpu.VMEM((4, BATCH // 8, QW), F32),
                pltpu.SemaphoreType.DMA,
                pltpu.SemaphoreType.DMA((4,)),
                pltpu.SemaphoreType.DMA((4,)),
            ],
            cost_estimate=pl.CostEstimate(flops=1_200_000_000, bytes_accessed=6_000_000, transcendentals=0),
            compiler_params=pltpu.CompilerParams(collective_id=1, has_side_effects=True, vmem_limit_bytes=20 * 1024 * 1024),
        )(own, *far, x_in, w_o, b_o)
        return x_out.astype(BF16), k_out, v_out, sp_t.T

    return jax.shard_map(
        local_step,
        mesh=mesh,
        in_specs=(row_spec, P('dp'), cache_spec, cache_spec, slot_spec, vec_spec, mat_spec, mat_spec, mat_spec, mat_spec, vec_spec),
        out_specs=(row_spec, cache_spec, cache_spec, slot_spec),
        check_vma=False)
```

```python
import functools

import jax
import jax.numpy as jnp
import numpy as np
from jax import lax
from jax.experimental import pallas as pl
from jax.experimental.pallas import tpu as pltpu
from jax.sharding import PartitionSpec as P

HEADS = 4
HEAD_DIM = 256
ROPE_DIM = 128
ROPE_HALF = ROPE_DIM // 2
ROPE_BASE = 10000.0
EPS = 1e-6
SCORE_SCALE = HEAD_DIM ** -0.5
NEG_LARGE = float(np.finfo(np.float32).min)
FAR = 1e9
F32 = jnp.float32
BF16 = jnp.bfloat16

BATCH = 512
D_MODEL = 1152
SLOTS = 64
QW = HEADS * HEAD_DIM
PW = QW + 128
GROUP = 8
STEP = 64
CHUNK = 64
AHEAD = 4
NCHUNK = BATCH // CHUNK
ROWS = 256


def sin_cos(theta):
    k = jnp.floor(theta * np.float32(2.0 / np.pi) + 0.5)
    r = theta - k * np.float32(1.5703125)
    r = r - k * np.float32(4.83751296997070312e-4)
    r = r - k * np.float32(7.54978995489188e-8)
    r2 = r * r
    s = r + r * r2 * (-1.6666654611e-1 + r2 * (8.3321608736e-3 + r2 * -1.9515295891e-4))
    c = 1.0 - 0.5 * r2 + r2 * r2 * (4.166664568298827e-2 + r2 * (-1.388731625493765e-3 + r2 * 2.443315711809948e-5))
    q = k - 4.0 * jnp.floor(k * 0.25)
    swap = (q == 1.0) | (q == 3.0)
    sin_v = jnp.where(swap, c, s)
    cos_v = jnp.where(swap, s, c)
    sin_v = jnp.where(q >= 2.0, -sin_v, sin_v)
    cos_v = jnp.where((q == 1.0) | (q == 2.0), -cos_v, cos_v)
    return sin_v, cos_v


def inv_freq_row():
    i = np.arange(ROPE_DIM) % ROPE_HALF
    return (ROPE_BASE ** (-i / ROPE_HALF)).astype(np.float32).reshape(1, ROPE_DIM)


def merge_rows(blocks):
    stats = [t[:, QW:] for t in blocks]
    lane = lax.broadcasted_iota(jnp.int32, stats[0].shape, 1)
    top = functools.reduce(jnp.maximum, stats)
    factors = [jnp.exp(t - top) for t in stats]
    sums = [t * pltpu.roll(f, HEADS, 1) for t, f in zip(stats, factors)]
    out = jnp.where(lane < HEADS, top, functools.reduce(jnp.add, sums))
    vals = []
    for h in range(HEADS):
        terms = [t[:, h * HEAD_DIM:(h + 1) * HEAD_DIM] * f[:, h:h + 1] for t, f in zip(blocks, factors)]
        vals.append(functools.reduce(jnp.add, terms))
    return jnp.concatenate(vals, axis=1), out


def normalise(v, s):
    inv = 1.0 / s
    return jnp.concatenate([v[:, h * HEAD_DIM:(h + 1) * HEAD_DIM] * inv[:, HEADS + h:HEADS + h + 1] for h in range(HEADS)], axis=1)


class Places:
    def __init__(self):
        me = lax.axis_index('kv')
        self.core = me % 2
        self.x = (me // 2) % 2
        self.y = me // 4
        self.mate = me + 1 - 2 * self.core

    def flip(self, m):
        x = self.x + (m % 2) * (1 - 2 * self.x)
        y = self.y + (m // 2) * (1 - 2 * self.y)
        return x, y

    def peer(self, m):
        x, y = self.flip(m)
        return y * 4 + x * 2 + self.core

    def eighth(self, m, core):
        x, y = self.flip(m)
        return 32 * core + 16 * x + 8 * y


def send(src, dst, ss, rs, peer):
    return pltpu.make_async_remote_copy(src_ref=src, dst_ref=dst, send_sem=ss, recv_sem=rs,
                                        device_id={'kv': peer}, device_id_type=pl.DeviceIdType.MESH)


def al(v, m=8):
    return pl.multiple_of(v, m)


class Reduce:
    def __init__(self, places, part, r0, r1, own, s0, s1):
        self.p = places
        self.part, self.r0, self.r1, self.own, self.s0, self.s1 = part, r0, r1, own, s0, s1

    def pair_copy(self, c):
        src = al(c * CHUNK + 32 * (1 - self.p.core))
        return send(self.part.at[pl.ds(src, 32)], self.r0.at[pl.ds(al(c * 32), 32)], self.s0.at[0, c], self.s0.at[1, c], self.p.mate)

    def chip_copies(self, c):
        return [send(self.part.at[pl.ds(al(c * CHUNK + self.p.eighth(m, self.p.core)), 8)],
                     self.r1.at[pl.ds(al(c * 24 + 8 * (m - 1)), 8)],
                     self.s1.at[0, 3 * c + m - 1], self.s1.at[1, 3 * c + m - 1], self.p.peer(m)) for m in (3, 1, 2)]

    def pair_step(self, c):
        self.pair_copy(c).wait_recv()
        rows = pl.ds(al(c * CHUNK + 32 * self.p.core), 32)
        v, s = merge_rows([self.part[rows, :], self.r0[pl.ds(al(c * 32), 32), :]])
        self.part[rows, :] = jnp.concatenate([v, s], axis=1)
        for cp in self.chip_copies(c):
            cp.start()

    def chip_step(self, c):
        for cp in self.chip_copies(c):
            cp.wait_recv()
        mine = self.part[pl.ds(al(c * CHUNK + self.p.eighth(0, self.p.core)), 8), :]
        v, s = merge_rows([mine] + [self.r1[pl.ds(al(c * 24 + 8 * n), 8), :] for n in range(3)])
        self.own[pl.ds(al(c * 8), 8), :] = normalise(v, s)

    def drain(self, c):
        self.pair_copy(c).wait_send()
        for cp in self.chip_copies(c):
            cp.wait_send()


class Attention:
    def __init__(self, off, kbuf, vbuf, q_v, kn_v, vn_v, p_col, js_col, part):
        self.refs = kbuf, vbuf, q_v, kn_v, vn_v, p_col, js_col, part
        self.sub = lax.broadcasted_iota(jnp.int32, (GROUP, 128), 0)
        self.lane = lax.broadcasted_iota(jnp.int32, (GROUP, 128), 1)
        self.slot_c = jnp.where((self.lane // SLOTS) == (self.sub % 2), (self.lane % SLOTS).astype(F32) + off.astype(F32), FAR)
        self.pick = [(self.sub // 2) == cc for cc in range(4)]
        self.iotas = [(lax.broadcasted_iota(jnp.int32, (16, HEAD_DIM), 0) + 16 * t).astype(F32).astype(BF16) for t in range(SLOTS // 16)]

    def rows(self, base):
        kbuf, vbuf, q_v, kn_v, vn_v, p_col, js_col, part = self.refs
        pick, iotas, lane, slot_c = self.pick, self.iotas, self.lane, self.slot_c

        def hits_of(b):
            js = jnp.broadcast_to(js_col[pl.ds(b, 1), :], (16, 128)).astype(BF16)
            js = jnp.concatenate([js, js], axis=1)
            return [io == js for io in iotas]

        def refresh(buf, new_ref, r0):
            out = []
            for i in range(GROUP):
                b = r0 + i
                hits = hits_of(b)
                fresh = jnp.broadcast_to(new_ref[pl.ds(b, 1), :], (16, HEAD_DIM)).astype(BF16)
                for t in range(SLOTS // 16):
                    piece = jnp.where(hits[t], fresh, buf[b, pl.ds(16 * t, 16), :])
                    buf[b, pl.ds(16 * t, 16), :] = piece
                    out.append(piece)
            return jnp.concatenate(out, axis=0)

        def scores(r0):
            rows = pl.ds(r0, GROUP)
            q = jnp.concatenate([q_v[rows, h * HEAD_DIM:(h + 1) * HEAD_DIM] for h in range(HEADS)], axis=0).astype(BF16)
            s = lax.dot_general(q, refresh(kbuf, kn_v, r0), (((1,), (1,)), ((), ())), preferred_element_type=F32)
            out = []
            for h in range(HEADS):
                sh = s[h * GROUP:(h + 1) * GROUP, :]
                c = sh[:, 384:512]
                for cc in range(3):
                    c = jnp.where(pick[cc], sh[:, cc * 128:(cc + 1) * 128], c)
                out.append(c)
            return out

        def soften(r0, cs):
            valid = slot_c <= p_col[pl.ds(r0, GROUP), :]
            stats = jnp.zeros((GROUP, 128), F32)
            ps = []
            for h in range(HEADS):
                c = jnp.where(valid, cs[h], NEG_LARGE)
                m = jnp.max(c, axis=1, keepdims=True)
                e = jnp.where(valid, jnp.exp(c - m), 0.0)
                l = jnp.sum(e, axis=1, keepdims=True)
                stats = jnp.where(lane == h, m, stats)
                stats = jnp.where(lane == HEADS + h, l, stats)
                ps.append(e)
            part[pl.ds(r0, GROUP), QW:PW] = stats
            return ps

        def values(r0, ps):
            pm = jnp.concatenate([jnp.concatenate([jnp.where(pick[cc], e, 0.0) for cc in range(4)], axis=1) for e in ps], axis=0).astype(BF16)
            o = jnp.dot(pm, refresh(vbuf, vn_v, r0), preferred_element_type=F32)
            rows = pl.ds(r0, GROUP)
            for h in range(HEADS):
                part[rows, h * HEAD_DIM:(h + 1) * HEAD_DIM] = o[h * GROUP:(h + 1) * GROUP, :]

        starts = [al(base + g * GROUP, GROUP) for g in range(CHUNK // GROUP)]
        cs = [scores(r0) for r0 in starts]
        ps = [soften(r0, c) for r0, c in zip(starts, cs)]
        for r0, e in zip(starts, ps):
            values(r0, e)


def chunk_rows(c):
    return pl.ds(pl.multiple_of(c * CHUNK, CHUNK), CHUNK)


def step_kernel(pos_hbm, freq_hbm, ns_hbm, sp_hbm, x_hbm, wq_hbm, wk_hbm, wv_hbm, k_hbm, v_hbm,
                own, kbuf, vbuf, sp_out,
                x_v, wq_v, wk_v, wv_v, n_v, q_v, kn_v, vn_v, p_col, js_col, cos_v, sin_v,
                part, r0, r1, pos_row, freq_ref, ns_ref, w_sem, k_sem, v_sem, s0, s1):
    p = Places()
    barrier = pltpu.get_barrier_semaphore()
    for peer in (p.mate, p.peer(1), p.peer(2), p.peer(3)):
        pl.semaphore_signal(barrier, inc=1, device_id={'kv': peer}, device_id_type=pl.DeviceIdType.MESH)
    off = lax.axis_index('kv') * SLOTS
    weights = ((x_hbm, x_v), (wk_hbm, wk_v), (wv_hbm, wv_v), (wq_hbm, wq_v), (sp_hbm, sp_out),
               (pos_hbm, pos_row), (freq_hbm, freq_ref), (ns_hbm, ns_ref))

    def w_in(n):
        return pltpu.make_async_copy(weights[n][0], weights[n][1], w_sem.at[n])

    def kv_in(c):
        return (pltpu.make_async_copy(k_hbm.at[chunk_rows(c)], kbuf.at[chunk_rows(c)], k_sem.at[c]),
                pltpu.make_async_copy(v_hbm.at[chunk_rows(c)], vbuf.at[chunk_rows(c)], v_sem.at[c]))

    for n in (5, 6, 7, 0, 1, 2, 3):
        w_in(n).start()
    for n in (5, 6, 7):
        w_in(n).wait()

    offf = off.astype(F32)

    @pl.loop(0, BATCH // 128)
    def _(t):
        rows = pl.ds(pl.multiple_of(t * 128, 128), 128)
        col = jnp.broadcast_to(pos_row[:, rows].astype(F32), (128, 128)).T
        p_col[rows, :] = col
        js = col - 512.0 * jnp.floor(col * (1.0 / 512.0)) - offf
        js_col[rows, :] = jnp.where((js >= 0.0) & (js < float(SLOTS)), js, -1.0)

    @pl.loop(0, BATCH // 64)
    def _(t):
        rows = pl.ds(pl.multiple_of(t * 64, 64), 64)
        s, c = sin_cos(p_col[rows, :] * freq_ref[...])
        lane = lax.broadcasted_iota(jnp.int32, (64, 128), 1)
        sin_v[rows, :] = jnp.where(lane < ROPE_HALF, -s, s)
        cos_v[rows, :] = c

    def rotate(t, rows):
        r = t[:, :ROPE_DIM]
        r = r * cos_v[rows, :] + pltpu.roll(r, ROPE_HALF, 1) * sin_v[rows, :]
        return jnp.concatenate([r, t[:, ROPE_DIM:]], axis=1)

    w_in(0).wait()
    for cp in kv_in(0):
        cp.start()
    gain = 1.0 + ns_ref[...].astype(F32).reshape(1, D_MODEL)

    @pl.loop(0, BATCH // 64)
    def _(i):
        rows = pl.ds(pl.multiple_of(i * 64, 64), 64)
        xf = x_v[rows, :].astype(F32)
        mean_sq = jnp.sum(xf * xf, axis=1, keepdims=True) * (1.0 / D_MODEL)
        n_v[rows, :] = (xf * lax.rsqrt(mean_sq + EPS) * gain).astype(BF16)

    for n in range(1, 4):
        w_in(n).wait()
    for c in range(1, AHEAD):
        for cp in kv_in(c):
            cp.start()
    red = Reduce(p, part, r0, r1, own, s0, s1)
    att = Attention(off, kbuf, vbuf, q_v, kn_v, vn_v, p_col, js_col, part)

    def attend(c):
        @pl.when(c + AHEAD < NCHUNK)
        def _():
            for cp in kv_in(c + AHEAD):
                cp.start()

        @pl.when(c == AHEAD)
        def _():
            w_in(4).start()

        @pl.when(c % (ROWS // CHUNK) == 0)
        def _():
            rows = pl.ds(al(c * CHUNK, ROWS), ROWS)
            kn_v[rows, :] = rotate(jnp.dot(n_v[rows, :], wk_v[...], preferred_element_type=F32), rows)
            vn_v[rows, :] = jnp.dot(n_v[rows, :], wv_v[...], preferred_element_type=F32)
            for h in range(HEADS):
                cols = pl.ds(h * HEAD_DIM, HEAD_DIM)
                qh = jnp.dot(n_v[rows, :], wq_v[:, cols], preferred_element_type=F32)
                q_v[rows, cols] = rotate(qh, rows) * SCORE_SCALE

        for cp in kv_in(c):
            cp.wait()
        att.rows(c * CHUNK)

        @pl.when(c == 0)
        def _():
            pl.semaphore_wait(barrier, 4)

        red.pair_copy(c).start()

    lags = ((0, attend), (1, red.pair_step), (4, red.chip_step))

    @pl.loop(0, NCHUNK + lags[-1][0])
    def _(i):
        for lag, body in lags:
            @pl.when((i >= lag) & (i < NCHUNK + lag))
            def _(lag=lag, body=body):
                body(i - lag)

    w_in(4).wait()
    p_all = pos_row[...]
    slot_ids = off + lax.broadcasted_iota(jnp.int32, (SLOTS, BATCH), 0)
    sp_out[...] = jnp.where(slot_ids == (p_all & 511), p_all, sp_out[...])

    @pl.loop(0, NCHUNK)
    def _(c):
        red.drain(c)


def out_kernel(own, from_x, from_y, from_d, x_v, wo_v, b_ref, out_ref, g, lsem, ssem, rsem):
    p = Places()
    barrier = pltpu.get_barrier_semaphore()
    pl.semaphore_signal(barrier, inc=1, device_id={'kv': p.mate}, device_id_type=pl.DeviceIdType.MESH)
    refs = (own, from_x, from_y, from_d)

    def copy(n):
        return send(refs[n], g.at[n], ssem.at[n], rsem.at[n], p.mate)

    pl.semaphore_wait(barrier, 1)
    for n in range(4):
        copy(n).start()
    bias = b_ref[...].astype(F32).reshape(1, D_MODEL)

    def emit(blocks, core):
        rows = [al(t * CHUNK + p.eighth(n, core)) for n in range(4) for t in range(NCHUNK)]
        o = jnp.concatenate([t[...].astype(BF16) for t in blocks], axis=0)
        xin = jnp.concatenate([x_v[pl.ds(r, 8), :].astype(F32) for r in rows], axis=0)
        y = xin + jnp.dot(o, wo_v[...], preferred_element_type=F32) + bias
        for t, r in enumerate(rows):
            out_ref[pl.ds(r, 8), :] = y[8 * t:8 * t + 8, :]

    emit(refs, p.core)
    for n in range(4):
        copy(n).wait_recv()
    emit([g.at[n] for n in range(4)], 1 - p.core)
    for n in range(4):
        copy(n).wait_send()


def solution(mesh):
    row_spec = P('dp', None)
    cache_spec = P('dp', 'kv', None)
    slot_spec = P('dp', 'kv')
    vec_spec = P(None)
    mat_spec = P(None, None)
    hbm = pl.BlockSpec(memory_space=pltpu.HBM)
    vmem = pl.BlockSpec(memory_space=pltpu.VMEM)

    def in_hbm(a):
        return pltpu.with_memory_space_constraint(a, pltpu.HBM)

    def local_step(x_in, positions, k_cache, v_cache, slot_pos, norm_scale, w_q, w_k, w_v, w_o, b_o):
        own, k_out, v_out, sp_t = pl.pallas_call(
            step_kernel,
            out_shape=(jax.ShapeDtypeStruct((BATCH // 8, QW), F32),
                       pltpu.VMEM((BATCH, SLOTS, HEAD_DIM), BF16),
                       pltpu.VMEM((BATCH, SLOTS, HEAD_DIM), BF16),
                       pltpu.VMEM((SLOTS, BATCH), jnp.int32)),
            in_specs=[hbm] * 10,
            out_specs=(vmem,) * 4,
            scratch_shapes=[
                pltpu.VMEM((BATCH, D_MODEL), BF16),
                pltpu.VMEM((D_MODEL, QW), BF16),
                pltpu.VMEM((D_MODEL, HEAD_DIM), BF16),
                pltpu.VMEM((D_MODEL, HEAD_DIM), BF16),
                pltpu.VMEM((BATCH, D_MODEL), BF16),
                pltpu.VMEM((BATCH, QW), F32),
                pltpu.VMEM((BATCH, HEAD_DIM), F32),
                pltpu.VMEM((BATCH, HEAD_DIM), F32),
                pltpu.VMEM((BATCH, 128), F32),
                pltpu.VMEM((BATCH, 128), F32),
                pltpu.VMEM((BATCH, 128), F32),
                pltpu.VMEM((BATCH, 128), F32),
                pltpu.VMEM((BATCH, PW), F32),
                pltpu.VMEM((NCHUNK * 32, PW), F32),
                pltpu.VMEM((NCHUNK * 24, PW), F32),
                pltpu.VMEM((1, BATCH), jnp.int32),
                pltpu.VMEM((1, ROPE_DIM), F32),
                pltpu.VMEM((D_MODEL,), BF16),
                pltpu.SemaphoreType.DMA((8,)),
                pltpu.SemaphoreType.DMA((NCHUNK,)),
                pltpu.SemaphoreType.DMA((NCHUNK,)),
                pltpu.SemaphoreType.DMA((2, NCHUNK)),
                pltpu.SemaphoreType.DMA((2, 3 * NCHUNK)),
            ],
            cost_estimate=pl.CostEstimate(flops=30_000_000_000, bytes_accessed=40_000_000, transcendentals=200_000),
            compiler_params=pltpu.CompilerParams(collective_id=0, has_side_effects=True, vmem_limit_bytes=20 * 1024 * 1024),
        )(*[in_hbm(a) for a in (positions.reshape(1, BATCH), jnp.asarray(inv_freq_row()), norm_scale, slot_pos.T, x_in, w_q, w_k, w_v, k_cache, v_cache)])
        far = [lax.ppermute(own, 'kv', [(i, i ^ m) for i in range(8)]) for m in (2, 4, 6)]
        x_out = pl.pallas_call(
            out_kernel,
            out_shape=jax.ShapeDtypeStruct((BATCH, D_MODEL), F32),
            in_specs=[vmem] * 7,
            out_specs=vmem,
            scratch_shapes=[
                pltpu.VMEM((4, BATCH // 8, QW), F32),
                pltpu.SemaphoreType.DMA,
                pltpu.SemaphoreType.DMA((4,)),
                pltpu.SemaphoreType.DMA((4,)),
            ],
            cost_estimate=pl.CostEstimate(flops=1_200_000_000, bytes_accessed=6_000_000, transcendentals=0),
            compiler_params=pltpu.CompilerParams(collective_id=1, has_side_effects=True, vmem_limit_bytes=20 * 1024 * 1024),
        )(own, *far, x_in, w_o, b_o)
        return x_out.astype(BF16), k_out, v_out, sp_t.T

    return jax.shard_map(
        local_step,
        mesh=mesh,
        in_specs=(row_spec, P('dp'), cache_spec, cache_spec, slot_spec, vec_spec, mat_spec, mat_spec, mat_spec, mat_spec, vec_spec),
        out_specs=(row_spec, cache_spec, cache_spec, slot_spec),
        check_vma=False)
```

```python
import functools

import jax
import jax.numpy as jnp
import numpy as np
from jax import lax
from jax.experimental import pallas as pl
from jax.experimental.pallas import tpu as pltpu
from jax.sharding import PartitionSpec as P

HEADS = 4
HEAD_DIM = 256
ROPE_DIM = 128
ROPE_HALF = ROPE_DIM // 2
ROPE_BASE = 10000.0
EPS = 1e-6
SCORE_SCALE = HEAD_DIM ** -0.5
NEG_LARGE = float(np.finfo(np.float32).min)
FAR = 1e9
F32 = jnp.float32
BF16 = jnp.bfloat16

BATCH = 512
D_MODEL = 1152
SLOTS = 64
QW = HEADS * HEAD_DIM
PW = QW + 128
GROUP = 8
STEP = 64
CHUNK = 64
AHEAD = 4
NCHUNK = BATCH // CHUNK
ROWS = 512


def sin_cos(theta):
    k = jnp.floor(theta * np.float32(2.0 / np.pi) + 0.5)
    r = theta - k * np.float32(1.5703125)
    r = r - k * np.float32(4.83751296997070312e-4)
    r = r - k * np.float32(7.54978995489188e-8)
    r2 = r * r
    s = r + r * r2 * (-1.6666654611e-1 + r2 * (8.3321608736e-3 + r2 * -1.9515295891e-4))
    c = 1.0 - 0.5 * r2 + r2 * r2 * (4.166664568298827e-2 + r2 * (-1.388731625493765e-3 + r2 * 2.443315711809948e-5))
    q = k - 4.0 * jnp.floor(k * 0.25)
    swap = (q == 1.0) | (q == 3.0)
    sin_v = jnp.where(swap, c, s)
    cos_v = jnp.where(swap, s, c)
    sin_v = jnp.where(q >= 2.0, -sin_v, sin_v)
    cos_v = jnp.where((q == 1.0) | (q == 2.0), -cos_v, cos_v)
    return sin_v, cos_v


def inv_freq_row():
    i = np.arange(ROPE_DIM) % ROPE_HALF
    return (ROPE_BASE ** (-i / ROPE_HALF)).astype(np.float32).reshape(1, ROPE_DIM)


def merge_rows(blocks):
    stats = [t[:, QW:] for t in blocks]
    lane = lax.broadcasted_iota(jnp.int32, stats[0].shape, 1)
    top = functools.reduce(jnp.maximum, stats)
    factors = [jnp.exp(t - top) for t in stats]
    sums = [t * pltpu.roll(f, HEADS, 1) for t, f in zip(stats, factors)]
    out = jnp.where(lane < HEADS, top, functools.reduce(jnp.add, sums))
    vals = []
    for h in range(HEADS):
        terms = [t[:, h * HEAD_DIM:(h + 1) * HEAD_DIM] * f[:, h:h + 1] for t, f in zip(blocks, factors)]
        vals.append(functools.reduce(jnp.add, terms))
    return jnp.concatenate(vals, axis=1), out


def normalise(v, s):
    inv = 1.0 / s
    return jnp.concatenate([v[:, h * HEAD_DIM:(h + 1) * HEAD_DIM] * inv[:, HEADS + h:HEADS + h + 1] for h in range(HEADS)], axis=1)


class Places:
    def __init__(self):
        me = lax.axis_index('kv')
        self.core = me % 2
        self.x = (me // 2) % 2
        self.y = me // 4
        self.mate = me + 1 - 2 * self.core

    def flip(self, m):
        x = self.x + (m % 2) * (1 - 2 * self.x)
        y = self.y + (m // 2) * (1 - 2 * self.y)
        return x, y

    def peer(self, m):
        x, y = self.flip(m)
        return y * 4 + x * 2 + self.core

    def eighth(self, m, core):
        x, y = self.flip(m)
        return 32 * core + 16 * x + 8 * y


def send(src, dst, ss, rs, peer):
    return pltpu.make_async_remote_copy(src_ref=src, dst_ref=dst, send_sem=ss, recv_sem=rs,
                                        device_id={'kv': peer}, device_id_type=pl.DeviceIdType.MESH)


def al(v, m=8):
    return pl.multiple_of(v, m)


class Reduce:
    def __init__(self, places, part, r0, r1, own, s0, s1):
        self.p = places
        self.part, self.r0, self.r1, self.own, self.s0, self.s1 = part, r0, r1, own, s0, s1

    def pair_copy(self, c):
        src = al(c * CHUNK + 32 * (1 - self.p.core))
        return send(self.part.at[pl.ds(src, 32)], self.r0.at[pl.ds(al(c * 32), 32)], self.s0.at[0, c], self.s0.at[1, c], self.p.mate)

    def chip_copies(self, c):
        return [send(self.part.at[pl.ds(al(c * CHUNK + self.p.eighth(m, self.p.core)), 8)],
                     self.r1.at[pl.ds(al((c // 2) * 48 + 16 * (m - 1) + 8 * (c % 2)), 8)],
                     self.s1.at[0, 3 * c + m - 1], self.s1.at[1, 3 * c + m - 1], self.p.peer(m)) for m in (3, 1, 2)]

    def pair_step(self, c):
        self.pair_copy(c).wait_recv()
        rows = pl.ds(al(c * CHUNK + 32 * self.p.core), 32)
        v, s = merge_rows([self.part[rows, :], self.r0[pl.ds(al(c * 32), 32), :]])
        self.part[rows, :] = jnp.concatenate([v, s], axis=1)
        for cp in self.chip_copies(c):
            cp.start()

    def chip_step(self, c):
        @pl.when(c % 2 == 1)
        def _():
            for cp in self.chip_copies(c - 1) + self.chip_copies(c):
                cp.wait_recv()
            mine = jnp.concatenate([self.part[pl.ds(al(k * CHUNK + self.p.eighth(0, self.p.core)), 8), :] for k in (c - 1, c)], axis=0)
            v, s = merge_rows([mine] + [self.r1[pl.ds(al((c // 2) * 48 + 16 * n), 16), :] for n in range(3)])
            self.own[pl.ds(al((c - 1) * 8), 16), :] = normalise(v, s)

    def drain(self, c):
        self.pair_copy(c).wait_send()
        for cp in self.chip_copies(c):
            cp.wait_send()


class Attention:
    def __init__(self, off, kbuf, vbuf, q_v, kn_v, vn_v, p_col, js_col, part):
        self.refs = kbuf, vbuf, q_v, kn_v, vn_v, p_col, js_col, part
        self.sub = lax.broadcasted_iota(jnp.int32, (GROUP, 128), 0)
        self.lane = lax.broadcasted_iota(jnp.int32, (GROUP, 128), 1)
        self.slot_c = jnp.where((self.lane // SLOTS) == (self.sub % 2), (self.lane % SLOTS).astype(F32) + off.astype(F32), FAR)
        self.pick = [(self.sub // 2) == cc for cc in range(4)]
        self.iotas = [(lax.broadcasted_iota(jnp.int32, (16, HEAD_DIM), 0) + 16 * t).astype(F32).astype(BF16) for t in range(SLOTS // 16)]

    def rows(self, base):
        kbuf, vbuf, q_v, kn_v, vn_v, p_col, js_col, part = self.refs
        pick, iotas, lane, slot_c = self.pick, self.iotas, self.lane, self.slot_c

        def hits_of(b):
            js = jnp.broadcast_to(js_col[pl.ds(b, 1), :], (16, 128)).astype(BF16)
            js = jnp.concatenate([js, js], axis=1)
            return [io == js for io in iotas]

        def refresh(buf, new_ref, r0):
            out = []
            for i in range(GROUP):
                b = r0 + i
                hits = hits_of(b)
                fresh = jnp.broadcast_to(new_ref[pl.ds(b, 1), :], (16, HEAD_DIM)).astype(BF16)
                for t in range(SLOTS // 16):
                    piece = jnp.where(hits[t], fresh, buf[b, pl.ds(16 * t, 16), :])
                    buf[b, pl.ds(16 * t, 16), :] = piece
                    out.append(piece)
            return jnp.concatenate(out, axis=0)

        def scores(r0):
            rows = pl.ds(r0, GROUP)
            q = jnp.concatenate([q_v[rows, h * HEAD_DIM:(h + 1) * HEAD_DIM] for h in range(HEADS)], axis=0).astype(BF16)
            s = lax.dot_general(q, refresh(kbuf, kn_v, r0), (((1,), (1,)), ((), ())), preferred_element_type=F32)
            out = []
            for h in range(HEADS):
                sh = s[h * GROUP:(h + 1) * GROUP, :]
                c = sh[:, 384:512]
                for cc in range(3):
                    c = jnp.where(pick[cc], sh[:, cc * 128:(cc + 1) * 128], c)
                out.append(c)
            return out

        def soften(r0, cs):
            valid = slot_c <= p_col[pl.ds(r0, GROUP), :]
            stats = jnp.zeros((GROUP, 128), F32)
            ps = []
            for h in range(HEADS):
                c = jnp.where(valid, cs[h], NEG_LARGE)
                m = jnp.max(c, axis=1, keepdims=True)
                e = jnp.where(valid, jnp.exp(c - m), 0.0)
                l = jnp.sum(e, axis=1, keepdims=True)
                stats = jnp.where(lane == h, m, stats)
                stats = jnp.where(lane == HEADS + h, l, stats)
                ps.append(e)
            part[pl.ds(r0, GROUP), QW:PW] = stats
            return ps

        def values(r0, ps):
            pm = jnp.concatenate([jnp.concatenate([jnp.where(pick[cc], e, 0.0) for cc in range(4)], axis=1) for e in ps], axis=0).astype(BF16)
            o = jnp.dot(pm, refresh(vbuf, vn_v, r0), preferred_element_type=F32)
            rows = pl.ds(r0, GROUP)
            for h in range(HEADS):
                part[rows, h * HEAD_DIM:(h + 1) * HEAD_DIM] = o[h * GROUP:(h + 1) * GROUP, :]

        starts = [al(base + g * GROUP, GROUP) for g in range(CHUNK // GROUP)]
        cs = [scores(r0) for r0 in starts]
        ps = [soften(r0, c) for r0, c in zip(starts, cs)]
        for r0, e in zip(starts, ps):
            values(r0, e)


def chunk_rows(c):
    return pl.ds(pl.multiple_of(c * CHUNK, CHUNK), CHUNK)


def step_kernel(pos_hbm, freq_hbm, ns_hbm, sp_hbm, x_hbm, wq_hbm, wk_hbm, wv_hbm, k_hbm, v_hbm,
                own, kbuf, vbuf, sp_out,
                x_v, wq_v, wk_v, wv_v, n_v, q_v, kn_v, vn_v, p_col, js_col, cos_v, sin_v,
                part, r0, r1, pos_row, freq_ref, ns_ref, w_sem, k_sem, v_sem, s0, s1):
    p = Places()
    barrier = pltpu.get_barrier_semaphore()
    for peer in (p.mate, p.peer(1), p.peer(2), p.peer(3)):
        pl.semaphore_signal(barrier, inc=1, device_id={'kv': peer}, device_id_type=pl.DeviceIdType.MESH)
    off = lax.axis_index('kv') * SLOTS
    weights = ((x_hbm, x_v), (wk_hbm, wk_v), (wv_hbm, wv_v), (wq_hbm, wq_v), (sp_hbm, sp_out),
               (pos_hbm, pos_row), (freq_hbm, freq_ref), (ns_hbm, ns_ref))

    def w_in(n):
        return pltpu.make_async_copy(weights[n][0], weights[n][1], w_sem.at[n])

    def kv_in(c):
        return (pltpu.make_async_copy(k_hbm.at[chunk_rows(c)], kbuf.at[chunk_rows(c)], k_sem.at[c]),
                pltpu.make_async_copy(v_hbm.at[chunk_rows(c)], vbuf.at[chunk_rows(c)], v_sem.at[c]))

    for n in (5, 6, 7, 0, 1, 2, 3):
        w_in(n).start()
    for n in (5, 6, 7):
        w_in(n).wait()

    offf = off.astype(F32)

    @pl.loop(0, BATCH // 128)
    def _(t):
        rows = pl.ds(pl.multiple_of(t * 128, 128), 128)
        col = jnp.broadcast_to(pos_row[:, rows].astype(F32), (128, 128)).T
        p_col[rows, :] = col
        js = col - 512.0 * jnp.floor(col * (1.0 / 512.0)) - offf
        js_col[rows, :] = jnp.where((js >= 0.0) & (js < float(SLOTS)), js, -1.0)

    @pl.loop(0, BATCH // 64)
    def _(t):
        rows = pl.ds(pl.multiple_of(t * 64, 64), 64)
        s, c = sin_cos(p_col[rows, :] * freq_ref[...])
        lane = lax.broadcasted_iota(jnp.int32, (64, 128), 1)
        sin_v[rows, :] = jnp.where(lane < ROPE_HALF, -s, s)
        cos_v[rows, :] = c

    def rotate(t, rows):
        r = t[:, :ROPE_DIM]
        r = r * cos_v[rows, :] + pltpu.roll(r, ROPE_HALF, 1) * sin_v[rows, :]
        return jnp.concatenate([r, t[:, ROPE_DIM:]], axis=1)

    w_in(0).wait()
    for cp in kv_in(0):
        cp.start()
    gain = 1.0 + ns_ref[...].astype(F32).reshape(1, D_MODEL)

    @pl.loop(0, BATCH // 128)
    def _(i):
        rows = pl.ds(pl.multiple_of(i * 128, 128), 128)
        xf = x_v[rows, :].astype(F32)
        mean_sq = jnp.sum(xf * xf, axis=1, keepdims=True) * (1.0 / D_MODEL)
        n_v[rows, :] = (xf * lax.rsqrt(mean_sq + EPS) * gain).astype(BF16)

    for n in range(1, 4):
        w_in(n).wait()
    for c in range(1, AHEAD):
        for cp in kv_in(c):
            cp.start()
    red = Reduce(p, part, r0, r1, own, s0, s1)
    att = Attention(off, kbuf, vbuf, q_v, kn_v, vn_v, p_col, js_col, part)

    def attend(c):
        @pl.when(c + AHEAD < NCHUNK)
        def _():
            for cp in kv_in(c + AHEAD):
                cp.start()

        @pl.when(c == AHEAD)
        def _():
            w_in(4).start()

        @pl.when(c % (ROWS // CHUNK) == 0)
        def _():
            rows = pl.ds(al(c * CHUNK, ROWS), ROWS)
            kn_v[rows, :] = rotate(jnp.dot(n_v[rows, :], wk_v[...], preferred_element_type=F32), rows)
            vn_v[rows, :] = jnp.dot(n_v[rows, :], wv_v[...], preferred_element_type=F32)
            for h in range(HEADS):
                cols = pl.ds(h * HEAD_DIM, HEAD_DIM)
                qh = jnp.dot(n_v[rows, :], wq_v[:, cols], preferred_element_type=F32)
                q_v[rows, cols] = rotate(qh, rows) * SCORE_SCALE

        for cp in kv_in(c):
            cp.wait()
        att.rows(c * CHUNK)

        @pl.when(c == 0)
        def _():
            pl.semaphore_wait(barrier, 4)

        red.pair_copy(c).start()

    lags = ((0, attend), (1, red.pair_step), (4, red.chip_step))

    @pl.loop(0, NCHUNK + lags[-1][0])
    def _(i):
        for lag, body in lags:
            @pl.when((i >= lag) & (i < NCHUNK + lag))
            def _(lag=lag, body=body):
                body(i - lag)

    w_in(4).wait()
    p_all = pos_row[...]
    slot_ids = off + lax.broadcasted_iota(jnp.int32, (SLOTS, BATCH), 0)
    sp_out[...] = jnp.where(slot_ids == (p_all & 511), p_all, sp_out[...])

    @pl.loop(0, NCHUNK)
    def _(c):
        red.drain(c)


def out_kernel(own, from_x, from_y, from_d, x_v, wo_v, b_ref, out_ref, g, lsem, ssem, rsem):
    p = Places()
    barrier = pltpu.get_barrier_semaphore()
    pl.semaphore_signal(barrier, inc=1, device_id={'kv': p.mate}, device_id_type=pl.DeviceIdType.MESH)
    refs = (own, from_x, from_y, from_d)

    def copy(n):
        return send(refs[n], g.at[n], ssem.at[n], rsem.at[n], p.mate)

    pl.semaphore_wait(barrier, 1)
    for n in range(4):
        copy(n).start()
    bias = b_ref[...].astype(F32).reshape(1, D_MODEL)

    def emit(blocks, core):
        rows = [al(t * CHUNK + p.eighth(n, core)) for n in range(4) for t in range(NCHUNK)]
        o = jnp.concatenate([t[...].astype(BF16) for t in blocks], axis=0)
        xin = jnp.concatenate([x_v[pl.ds(r, 8), :].astype(F32) for r in rows], axis=0)
        y = xin + jnp.dot(o, wo_v[...], preferred_element_type=F32) + bias
        for t, r in enumerate(rows):
            out_ref[pl.ds(r, 8), :] = y[8 * t:8 * t + 8, :]

    emit(refs, p.core)
    for n in range(4):
        copy(n).wait_recv()
    emit([g.at[n] for n in range(4)], 1 - p.core)
    for n in range(4):
        copy(n).wait_send()


def solution(mesh):
    row_spec = P('dp', None)
    cache_spec = P('dp', 'kv', None)
    slot_spec = P('dp', 'kv')
    vec_spec = P(None)
    mat_spec = P(None, None)
    hbm = pl.BlockSpec(memory_space=pltpu.HBM)
    vmem = pl.BlockSpec(memory_space=pltpu.VMEM)

    def in_hbm(a):
        return pltpu.with_memory_space_constraint(a, pltpu.HBM)

    def local_step(x_in, positions, k_cache, v_cache, slot_pos, norm_scale, w_q, w_k, w_v, w_o, b_o):
        own, k_out, v_out, sp_t = pl.pallas_call(
            step_kernel,
            out_shape=(jax.ShapeDtypeStruct((BATCH // 8, QW), F32),
                       pltpu.VMEM((BATCH, SLOTS, HEAD_DIM), BF16),
                       pltpu.VMEM((BATCH, SLOTS, HEAD_DIM), BF16),
                       pltpu.VMEM((SLOTS, BATCH), jnp.int32)),
            in_specs=[hbm] * 10,
            out_specs=(vmem,) * 4,
            scratch_shapes=[
                pltpu.VMEM((BATCH, D_MODEL), BF16),
                pltpu.VMEM((D_MODEL, QW), BF16),
                pltpu.VMEM((D_MODEL, HEAD_DIM), BF16),
                pltpu.VMEM((D_MODEL, HEAD_DIM), BF16),
                pltpu.VMEM((BATCH, D_MODEL), BF16),
                pltpu.VMEM((BATCH, QW), F32),
                pltpu.VMEM((BATCH, HEAD_DIM), F32),
                pltpu.VMEM((BATCH, HEAD_DIM), F32),
                pltpu.VMEM((BATCH, 128), F32),
                pltpu.VMEM((BATCH, 128), F32),
                pltpu.VMEM((BATCH, 128), F32),
                pltpu.VMEM((BATCH, 128), F32),
                pltpu.VMEM((BATCH, PW), F32),
                pltpu.VMEM((NCHUNK * 32, PW), F32),
                pltpu.VMEM((NCHUNK * 24, PW), F32),
                pltpu.VMEM((1, BATCH), jnp.int32),
                pltpu.VMEM((1, ROPE_DIM), F32),
                pltpu.VMEM((D_MODEL,), BF16),
                pltpu.SemaphoreType.DMA((8,)),
                pltpu.SemaphoreType.DMA((NCHUNK,)),
                pltpu.SemaphoreType.DMA((NCHUNK,)),
                pltpu.SemaphoreType.DMA((2, NCHUNK)),
                pltpu.SemaphoreType.DMA((2, 3 * NCHUNK)),
            ],
            cost_estimate=pl.CostEstimate(flops=30_000_000_000, bytes_accessed=40_000_000, transcendentals=200_000),
            compiler_params=pltpu.CompilerParams(collective_id=0, has_side_effects=True, vmem_limit_bytes=20 * 1024 * 1024),
        )(*[in_hbm(a) for a in (positions.reshape(1, BATCH), jnp.asarray(inv_freq_row()), norm_scale, slot_pos.T, x_in, w_q, w_k, w_v, k_cache, v_cache)])
        far = [lax.ppermute(own, 'kv', [(i, i ^ m) for i in range(8)]) for m in (2, 4, 6)]
        x_out = pl.pallas_call(
            out_kernel,
            out_shape=jax.ShapeDtypeStruct((BATCH, D_MODEL), F32),
            in_specs=[vmem] * 7,
            out_specs=vmem,
            scratch_shapes=[
                pltpu.VMEM((4, BATCH // 8, QW), F32),
                pltpu.SemaphoreType.DMA,
                pltpu.SemaphoreType.DMA((4,)),
                pltpu.SemaphoreType.DMA((4,)),
            ],
            cost_estimate=pl.CostEstimate(flops=1_200_000_000, bytes_accessed=6_000_000, transcendentals=0),
            compiler_params=pltpu.CompilerParams(collective_id=1, has_side_effects=True, vmem_limit_bytes=20 * 1024 * 1024),
        )(own, *far, x_in, w_o, b_o)
        return x_out.astype(BF16), k_out, v_out, sp_t.T

    return jax.shard_map(
        local_step,
        mesh=mesh,
        in_specs=(row_spec, P('dp'), cache_spec, cache_spec, slot_spec, vec_spec, mat_spec, mat_spec, mat_spec, mat_spec, vec_spec),
        out_specs=(row_spec, cache_spec, cache_spec, slot_spec),
        check_vma=False)
```

```python
import functools

import jax
import jax.numpy as jnp
import numpy as np
from jax import lax
from jax.experimental import pallas as pl
from jax.experimental.pallas import tpu as pltpu
from jax.sharding import PartitionSpec as P

HEADS = 4
HEAD_DIM = 256
ROPE_DIM = 128
ROPE_HALF = ROPE_DIM // 2
ROPE_BASE = 10000.0
EPS = 1e-6
SCORE_SCALE = HEAD_DIM ** -0.5
NEG_LARGE = float(np.finfo(np.float32).min)
FAR = 1e9
F32 = jnp.float32
BF16 = jnp.bfloat16

BATCH = 512
D_MODEL = 1152
SLOTS = 64
QW = HEADS * HEAD_DIM
PW = QW + 128
GROUP = 8
STEP = 64
CHUNK = 64
AHEAD = 4
NCHUNK = BATCH // CHUNK
ROWS = 512


def sin_cos(theta):
    k = jnp.floor(theta * np.float32(2.0 / np.pi) + 0.5)
    r = theta - k * np.float32(1.5703125)
    r = r - k * np.float32(4.83751296997070312e-4)
    r = r - k * np.float32(7.54978995489188e-8)
    r2 = r * r
    s = r + r * r2 * (-1.6666654611e-1 + r2 * (8.3321608736e-3 + r2 * -1.9515295891e-4))
    c = 1.0 - 0.5 * r2 + r2 * r2 * (4.166664568298827e-2 + r2 * (-1.388731625493765e-3 + r2 * 2.443315711809948e-5))
    q = k - 4.0 * jnp.floor(k * 0.25)
    swap = (q == 1.0) | (q == 3.0)
    sin_v = jnp.where(swap, c, s)
    cos_v = jnp.where(swap, s, c)
    sin_v = jnp.where(q >= 2.0, -sin_v, sin_v)
    cos_v = jnp.where((q == 1.0) | (q == 2.0), -cos_v, cos_v)
    return sin_v, cos_v


def inv_freq_row():
    i = np.arange(ROPE_DIM) % ROPE_HALF
    return (ROPE_BASE ** (-i / ROPE_HALF)).astype(np.float32).reshape(1, ROPE_DIM)


def merge_rows(blocks):
    stats = [t[:, QW:] for t in blocks]
    lane = lax.broadcasted_iota(jnp.int32, stats[0].shape, 1)
    top = functools.reduce(jnp.maximum, stats)
    factors = [jnp.exp(t - top) for t in stats]
    sums = [t * pltpu.roll(f, HEADS, 1) for t, f in zip(stats, factors)]
    out = jnp.where(lane < HEADS, top, functools.reduce(jnp.add, sums))
    vals = []
    for h in range(HEADS):
        terms = [t[:, h * HEAD_DIM:(h + 1) * HEAD_DIM] * f[:, h:h + 1] for t, f in zip(blocks, factors)]
        vals.append(functools.reduce(jnp.add, terms))
    return jnp.concatenate(vals, axis=1), out


def normalise(v, s):
    inv = 1.0 / s
    return jnp.concatenate([v[:, h * HEAD_DIM:(h + 1) * HEAD_DIM] * inv[:, HEADS + h:HEADS + h + 1] for h in range(HEADS)], axis=1)


class Places:
    def __init__(self):
        me = lax.axis_index('kv')
        self.core = me % 2
        self.x = (me // 2) % 2
        self.y = me // 4
        self.mate = me + 1 - 2 * self.core

    def flip(self, m):
        x = self.x + (m % 2) * (1 - 2 * self.x)
        y = self.y + (m // 2) * (1 - 2 * self.y)
        return x, y

    def peer(self, m):
        x, y = self.flip(m)
        return y * 4 + x * 2 + self.core

    def eighth(self, m, core):
        x, y = self.flip(m)
        return 32 * core + 16 * x + 8 * y


def send(src, dst, ss, rs, peer):
    return pltpu.make_async_remote_copy(src_ref=src, dst_ref=dst, send_sem=ss, recv_sem=rs,
                                        device_id={'kv': peer}, device_id_type=pl.DeviceIdType.MESH)


def al(v, m=8):
    return pl.multiple_of(v, m)


class Reduce:
    def __init__(self, places, part, r0, r1, own, s0, s1):
        self.p = places
        self.part, self.r0, self.r1, self.own, self.s0, self.s1 = part, r0, r1, own, s0, s1

    def pair_copy(self, c):
        src = al(c * CHUNK + 32 * (1 - self.p.core))
        return send(self.part.at[pl.ds(src, 32)], self.r0.at[pl.ds(al(c * 32), 32)], self.s0.at[0, c], self.s0.at[1, c], self.p.mate)

    def chip_copies(self, c):
        return [send(self.part.at[pl.ds(al(c * CHUNK + self.p.eighth(m, self.p.core)), 8)],
                     self.r1.at[pl.ds(al((c // 2) * 48 + 16 * (m - 1) + 8 * (c % 2)), 8)],
                     self.s1.at[0, 3 * c + m - 1], self.s1.at[1, 3 * c + m - 1], self.p.peer(m)) for m in (3, 1, 2)]

    def pair_step(self, c):
        self.pair_copy(c).wait_recv()
        rows = pl.ds(al(c * CHUNK + 32 * self.p.core), 32)
        v, s = merge_rows([self.part[rows, :], self.r0[pl.ds(al(c * 32), 32), :]])
        self.part[rows, :] = jnp.concatenate([v, s], axis=1)
        for cp in self.chip_copies(c):
            cp.start()

    def chip_step(self, c):
        @pl.when(c % 2 == 1)
        def _():
            for cp in self.chip_copies(c - 1) + self.chip_copies(c):
                cp.wait_recv()
            mine = jnp.concatenate([self.part[pl.ds(al(k * CHUNK + self.p.eighth(0, self.p.core)), 8), :] for k in (c - 1, c)], axis=0)
            v, s = merge_rows([mine] + [self.r1[pl.ds(al((c // 2) * 48 + 16 * n), 16), :] for n in range(3)])
            self.own[pl.ds(al((c - 1) * 8), 16), :] = normalise(v, s)

    def drain(self, c):
        self.pair_copy(c).wait_send()
        for cp in self.chip_copies(c):
            cp.wait_send()


class Attention:
    def __init__(self, off, kbuf, vbuf, q_v, kn_v, vn_v, p_col, js_col, part):
        self.refs = kbuf, vbuf, q_v, kn_v, vn_v, p_col, js_col, part
        self.sub = lax.broadcasted_iota(jnp.int32, (GROUP, 128), 0)
        self.lane = lax.broadcasted_iota(jnp.int32, (GROUP, 128), 1)
        self.slot_c = jnp.where((self.lane // SLOTS) == (self.sub % 2), (self.lane % SLOTS).astype(F32) + off.astype(F32), FAR)
        self.pick = [(self.sub // 2) == cc for cc in range(4)]
        self.iotas = [(lax.broadcasted_iota(jnp.int32, (16, HEAD_DIM), 0) + 16 * t).astype(F32).astype(BF16) for t in range(SLOTS // 16)]

    def rows(self, base):
        kbuf, vbuf, q_v, kn_v, vn_v, p_col, js_col, part = self.refs
        pick, iotas, lane, slot_c = self.pick, self.iotas, self.lane, self.slot_c

        def hits_of(b):
            js = jnp.broadcast_to(js_col[pl.ds(b, 1), :], (16, 128)).astype(BF16)
            js = jnp.concatenate([js, js], axis=1)
            return [io == js for io in iotas]

        def refresh(buf, new_ref, r0):
            out = []
            for i in range(GROUP):
                b = r0 + i
                hits = hits_of(b)
                fresh = jnp.broadcast_to(new_ref[pl.ds(b, 1), :], (16, HEAD_DIM)).astype(BF16)
                for t in range(SLOTS // 16):
                    piece = jnp.where(hits[t], fresh, buf[b, pl.ds(16 * t, 16), :])
                    buf[b, pl.ds(16 * t, 16), :] = piece
                    out.append(piece)
            return jnp.concatenate(out, axis=0)

        def scores(r0):
            rows = pl.ds(r0, GROUP)
            q = jnp.concatenate([q_v[rows, h * HEAD_DIM:(h + 1) * HEAD_DIM] for h in range(HEADS)], axis=0).astype(BF16)
            s = lax.dot_general(q, refresh(kbuf, kn_v, r0), (((1,), (1,)), ((), ())), preferred_element_type=F32)
            out = []
            for h in range(HEADS):
                sh = s[h * GROUP:(h + 1) * GROUP, :]
                c = sh[:, 384:512]
                for cc in range(3):
                    c = jnp.where(pick[cc], sh[:, cc * 128:(cc + 1) * 128], c)
                out.append(c)
            return out

        def soften(r0, cs):
            valid = slot_c <= p_col[pl.ds(r0, GROUP), :]
            stats = jnp.zeros((GROUP, 128), F32)
            ps = []
            for h in range(HEADS):
                c = jnp.where(valid, cs[h], NEG_LARGE)
                m = jnp.max(c, axis=1, keepdims=True)
                e = jnp.where(valid, jnp.exp(c - m), 0.0)
                l = jnp.sum(e, axis=1, keepdims=True)
                stats = jnp.where(lane == h, m, stats)
                stats = jnp.where(lane == HEADS + h, l, stats)
                ps.append(e)
            part[pl.ds(r0, GROUP), QW:PW] = stats
            return ps

        def values(r0, ps):
            pm = jnp.concatenate([jnp.concatenate([jnp.where(pick[cc], e, 0.0) for cc in range(4)], axis=1) for e in ps], axis=0).astype(BF16)
            o = jnp.dot(pm, refresh(vbuf, vn_v, r0), preferred_element_type=F32)
            rows = pl.ds(r0, GROUP)
            for h in range(HEADS):
                part[rows, h * HEAD_DIM:(h + 1) * HEAD_DIM] = o[h * GROUP:(h + 1) * GROUP, :]

        starts = [al(base + g * GROUP, GROUP) for g in range(CHUNK // GROUP)]
        cs = [scores(r0) for r0 in starts]
        ps = [soften(r0, c) for r0, c in zip(starts, cs)]
        for r0, e in zip(starts, ps):
            values(r0, e)


def chunk_rows(c):
    return pl.ds(pl.multiple_of(c * CHUNK, CHUNK), CHUNK)


def step_kernel(pos_hbm, freq_hbm, ns_hbm, sp_hbm, x_hbm, wq_hbm, wk_hbm, wv_hbm, k_hbm, v_hbm,
                own, kbuf, vbuf, sp_out,
                x_v, wq_v, wk_v, wv_v, n_v, q_v, kn_v, vn_v, p_col, js_col, cos_v, sin_v,
                part, r0, r1, pos_row, freq_ref, ns_ref, w_sem, k_sem, v_sem, s0, s1):
    p = Places()
    barrier = pltpu.get_barrier_semaphore()
    for peer in (p.mate, p.peer(1), p.peer(2), p.peer(3)):
        pl.semaphore_signal(barrier, inc=1, device_id={'kv': peer}, device_id_type=pl.DeviceIdType.MESH)
    off = lax.axis_index('kv') * SLOTS
    weights = ((x_hbm, x_v), (wk_hbm, wk_v), (wv_hbm, wv_v), (wq_hbm, wq_v), (sp_hbm, sp_out),
               (pos_hbm, pos_row), (freq_hbm, freq_ref), (ns_hbm, ns_ref))

    def w_in(n):
        return pltpu.make_async_copy(weights[n][0], weights[n][1], w_sem.at[n])

    def kv_in(c):
        return (pltpu.make_async_copy(k_hbm.at[chunk_rows(c)], kbuf.at[chunk_rows(c)], k_sem.at[c]),
                pltpu.make_async_copy(v_hbm.at[chunk_rows(c)], vbuf.at[chunk_rows(c)], v_sem.at[c]))

    for n in (5, 6, 7, 0, 1, 2, 3):
        w_in(n).start()
    for n in (5, 6, 7):
        w_in(n).wait()

    offf = off.astype(F32)

    @pl.loop(0, BATCH // 128)
    def _(t):
        rows = pl.ds(pl.multiple_of(t * 128, 128), 128)
        col = jnp.broadcast_to(pos_row[:, rows].astype(F32), (128, 128)).T
        p_col[rows, :] = col
        js = col - 512.0 * jnp.floor(col * (1.0 / 512.0)) - offf
        js_col[rows, :] = jnp.where((js >= 0.0) & (js < float(SLOTS)), js, -1.0)

    @pl.loop(0, BATCH // 64)
    def _(t):
        rows = pl.ds(pl.multiple_of(t * 64, 64), 64)
        s, c = sin_cos(p_col[rows, :] * freq_ref[...])
        lane = lax.broadcasted_iota(jnp.int32, (64, 128), 1)
        sin_v[rows, :] = jnp.where(lane < ROPE_HALF, -s, s)
        cos_v[rows, :] = c

    def rotate(t, rows):
        r = t[:, :ROPE_DIM]
        r = r * cos_v[rows, :] + pltpu.roll(r, ROPE_HALF, 1) * sin_v[rows, :]
        return jnp.concatenate([r, t[:, ROPE_DIM:]], axis=1)

    w_in(0).wait()
    for cp in kv_in(0):
        cp.start()
    gain = 1.0 + ns_ref[...].astype(F32).reshape(1, D_MODEL)

    @pl.loop(0, BATCH // 128)
    def _(i):
        rows = pl.ds(pl.multiple_of(i * 128, 128), 128)
        xf = x_v[rows, :].astype(F32)
        mean_sq = jnp.sum(xf * xf, axis=1, keepdims=True) * (1.0 / D_MODEL)
        n_v[rows, :] = (xf * lax.rsqrt(mean_sq + EPS) * gain).astype(BF16)

    for n in range(1, 4):
        w_in(n).wait()
    for c in range(1, AHEAD):
        for cp in kv_in(c):
            cp.start()
    red = Reduce(p, part, r0, r1, own, s0, s1)
    att = Attention(off, kbuf, vbuf, q_v, kn_v, vn_v, p_col, js_col, part)

    def attend(c):
        @pl.when(c + AHEAD < NCHUNK)
        def _():
            for cp in kv_in(c + AHEAD):
                cp.start()

        @pl.when(c == AHEAD)
        def _():
            w_in(4).start()

        @pl.when(c % (ROWS // CHUNK) == 0)
        def _():
            rows = pl.ds(al(c * CHUNK, ROWS), ROWS)
            kn_v[rows, :] = rotate(jnp.dot(n_v[rows, :], wk_v[...], preferred_element_type=F32), rows)
            vn_v[rows, :] = jnp.dot(n_v[rows, :], wv_v[...], preferred_element_type=F32)
            for h in range(HEADS):
                cols = pl.ds(h * HEAD_DIM, HEAD_DIM)
                qh = jnp.dot(n_v[rows, :], wq_v[:, cols], preferred_element_type=F32)
                q_v[rows, cols] = rotate(qh, rows) * SCORE_SCALE

        for cp in kv_in(c):
            cp.wait()
        att.rows(c * CHUNK)

        @pl.when(c == 0)
        def _():
            pl.semaphore_wait(barrier, 4)

        red.pair_copy(c).start()

    lags = ((0, attend), (2, red.pair_step), (9, red.chip_step))

    @pl.loop(0, NCHUNK + lags[-1][0])
    def _(i):
        for lag, body in lags:
            @pl.when((i >= lag) & (i < NCHUNK + lag))
            def _(lag=lag, body=body):
                body(i - lag)

    w_in(4).wait()
    p_all = pos_row[...]
    slot_ids = off + lax.broadcasted_iota(jnp.int32, (SLOTS, BATCH), 0)
    sp_out[...] = jnp.where(slot_ids == (p_all & 511), p_all, sp_out[...])

    @pl.loop(0, NCHUNK)
    def _(c):
        red.drain(c)


def out_kernel(own, from_x, from_y, from_d, x_v, wo_v, b_ref, out_ref, g, lsem, ssem, rsem):
    p = Places()
    barrier = pltpu.get_barrier_semaphore()
    pl.semaphore_signal(barrier, inc=1, device_id={'kv': p.mate}, device_id_type=pl.DeviceIdType.MESH)
    refs = (own, from_x, from_y, from_d)

    def copy(n):
        return send(refs[n], g.at[n], ssem.at[n], rsem.at[n], p.mate)

    pl.semaphore_wait(barrier, 1)
    for n in range(4):
        copy(n).start()
    bias = b_ref[...].astype(F32).reshape(1, D_MODEL)

    def emit(blocks, core):
        rows = [al(t * CHUNK + p.eighth(n, core)) for n in range(4) for t in range(NCHUNK)]
        o = jnp.concatenate([t[...].astype(BF16) for t in blocks], axis=0)
        xin = jnp.concatenate([x_v[pl.ds(r, 8), :].astype(F32) for r in rows], axis=0)
        y = xin + jnp.dot(o, wo_v[...], preferred_element_type=F32) + bias
        for t, r in enumerate(rows):
            out_ref[pl.ds(r, 8), :] = y[8 * t:8 * t + 8, :]

    emit(refs, p.core)
    for n in range(4):
        copy(n).wait_recv()
    emit([g.at[n] for n in range(4)], 1 - p.core)
    for n in range(4):
        copy(n).wait_send()


def solution(mesh):
    row_spec = P('dp', None)
    cache_spec = P('dp', 'kv', None)
    slot_spec = P('dp', 'kv')
    vec_spec = P(None)
    mat_spec = P(None, None)
    hbm = pl.BlockSpec(memory_space=pltpu.HBM)
    vmem = pl.BlockSpec(memory_space=pltpu.VMEM)

    def in_hbm(a):
        return pltpu.with_memory_space_constraint(a, pltpu.HBM)

    def local_step(x_in, positions, k_cache, v_cache, slot_pos, norm_scale, w_q, w_k, w_v, w_o, b_o):
        own, k_out, v_out, sp_t = pl.pallas_call(
            step_kernel,
            out_shape=(jax.ShapeDtypeStruct((BATCH // 8, QW), F32),
                       pltpu.VMEM((BATCH, SLOTS, HEAD_DIM), BF16),
                       pltpu.VMEM((BATCH, SLOTS, HEAD_DIM), BF16),
                       pltpu.VMEM((SLOTS, BATCH), jnp.int32)),
            in_specs=[hbm] * 10,
            out_specs=(vmem,) * 4,
            scratch_shapes=[
                pltpu.VMEM((BATCH, D_MODEL), BF16),
                pltpu.VMEM((D_MODEL, QW), BF16),
                pltpu.VMEM((D_MODEL, HEAD_DIM), BF16),
                pltpu.VMEM((D_MODEL, HEAD_DIM), BF16),
                pltpu.VMEM((BATCH, D_MODEL), BF16),
                pltpu.VMEM((BATCH, QW), F32),
                pltpu.VMEM((BATCH, HEAD_DIM), F32),
                pltpu.VMEM((BATCH, HEAD_DIM), F32),
                pltpu.VMEM((BATCH, 128), F32),
                pltpu.VMEM((BATCH, 128), F32),
                pltpu.VMEM((BATCH, 128), F32),
                pltpu.VMEM((BATCH, 128), F32),
                pltpu.VMEM((BATCH, PW), F32),
                pltpu.VMEM((NCHUNK * 32, PW), F32),
                pltpu.VMEM((NCHUNK * 24, PW), F32),
                pltpu.VMEM((1, BATCH), jnp.int32),
                pltpu.VMEM((1, ROPE_DIM), F32),
                pltpu.VMEM((D_MODEL,), BF16),
                pltpu.SemaphoreType.DMA((8,)),
                pltpu.SemaphoreType.DMA((NCHUNK,)),
                pltpu.SemaphoreType.DMA((NCHUNK,)),
                pltpu.SemaphoreType.DMA((2, NCHUNK)),
                pltpu.SemaphoreType.DMA((2, 3 * NCHUNK)),
            ],
            cost_estimate=pl.CostEstimate(flops=30_000_000_000, bytes_accessed=40_000_000, transcendentals=200_000),
            compiler_params=pltpu.CompilerParams(collective_id=0, has_side_effects=True, vmem_limit_bytes=20 * 1024 * 1024),
        )(*[in_hbm(a) for a in (positions.reshape(1, BATCH), jnp.asarray(inv_freq_row()), norm_scale, slot_pos.T, x_in, w_q, w_k, w_v, k_cache, v_cache)])
        far = [lax.ppermute(own, 'kv', [(i, i ^ m) for i in range(8)]) for m in (2, 4, 6)]
        x_out = pl.pallas_call(
            out_kernel,
            out_shape=jax.ShapeDtypeStruct((BATCH, D_MODEL), F32),
            in_specs=[vmem] * 7,
            out_specs=vmem,
            scratch_shapes=[
                pltpu.VMEM((4, BATCH // 8, QW), F32),
                pltpu.SemaphoreType.DMA,
                pltpu.SemaphoreType.DMA((4,)),
                pltpu.SemaphoreType.DMA((4,)),
            ],
            cost_estimate=pl.CostEstimate(flops=1_200_000_000, bytes_accessed=6_000_000, transcendentals=0),
            compiler_params=pltpu.CompilerParams(collective_id=1, has_side_effects=True, vmem_limit_bytes=20 * 1024 * 1024),
        )(own, *far, x_in, w_o, b_o)
        return x_out.astype(BF16), k_out, v_out, sp_t.T

    return jax.shard_map(
        local_step,
        mesh=mesh,
        in_specs=(row_spec, P('dp'), cache_spec, cache_spec, slot_spec, vec_spec, mat_spec, mat_spec, mat_spec, mat_spec, vec_spec),
        out_specs=(row_spec, cache_spec, cache_spec, slot_spec),
        check_vma=False)
```

```python
import functools

import jax
import jax.numpy as jnp
import numpy as np
from jax import lax
from jax.experimental import pallas as pl
from jax.experimental.pallas import tpu as pltpu
from jax.sharding import PartitionSpec as P

HEADS = 4
HEAD_DIM = 256
ROPE_DIM = 128
ROPE_HALF = ROPE_DIM // 2
ROPE_BASE = 10000.0
EPS = 1e-6
SCORE_SCALE = HEAD_DIM ** -0.5
NEG_LARGE = float(np.finfo(np.float32).min)
FAR = 1e9
F32 = jnp.float32
BF16 = jnp.bfloat16

BATCH = 512
D_MODEL = 1152
SLOTS = 64
QW = HEADS * HEAD_DIM
PW = QW + 128
GROUP = 8
STEP = 64
CHUNK = 64
NCHUNK = BATCH // CHUNK
ROWS = 512


def sin_cos(theta):
    k = jnp.floor(theta * np.float32(2.0 / np.pi) + 0.5)
    r = theta - k * np.float32(1.5703125)
    r = r - k * np.float32(4.83751296997070312e-4)
    r = r - k * np.float32(7.54978995489188e-8)
    r2 = r * r
    s = r + r * r2 * (-1.6666654611e-1 + r2 * (8.3321608736e-3 + r2 * -1.9515295891e-4))
    c = 1.0 - 0.5 * r2 + r2 * r2 * (4.166664568298827e-2 + r2 * (-1.388731625493765e-3 + r2 * 2.443315711809948e-5))
    q = k - 4.0 * jnp.floor(k * 0.25)
    swap = (q == 1.0) | (q == 3.0)
    sin_v = jnp.where(swap, c, s)
    cos_v = jnp.where(swap, s, c)
    sin_v = jnp.where(q >= 2.0, -sin_v, sin_v)
    cos_v = jnp.where((q == 1.0) | (q == 2.0), -cos_v, cos_v)
    return sin_v, cos_v


def inv_freq_row():
    i = np.arange(ROPE_DIM) % ROPE_HALF
    return (ROPE_BASE ** (-i / ROPE_HALF)).astype(np.float32).reshape(1, ROPE_DIM)


def merge_rows(blocks):
    stats = [t[:, QW:] for t in blocks]
    lane = lax.broadcasted_iota(jnp.int32, stats[0].shape, 1)
    top = functools.reduce(jnp.maximum, stats)
    factors = [jnp.exp(t - top) for t in stats]
    sums = [t * pltpu.roll(f, HEADS, 1) for t, f in zip(stats, factors)]
    out = jnp.where(lane < HEADS, top, functools.reduce(jnp.add, sums))
    vals = []
    for h in range(HEADS):
        terms = [t[:, h * HEAD_DIM:(h + 1) * HEAD_DIM] * f[:, h:h + 1] for t, f in zip(blocks, factors)]
        vals.append(functools.reduce(jnp.add, terms))
    return jnp.concatenate(vals, axis=1), out


def normalise(v, s):
    inv = 1.0 / s
    return jnp.concatenate([v[:, h * HEAD_DIM:(h + 1) * HEAD_DIM] * inv[:, HEADS + h:HEADS + h + 1] for h in range(HEADS)], axis=1)


class Places:
    def __init__(self):
        me = lax.axis_index('kv')
        self.core = me % 2
        self.x = (me // 2) % 2
        self.y = me // 4
        self.mate = me + 1 - 2 * self.core

    def flip(self, m):
        x = self.x + (m % 2) * (1 - 2 * self.x)
        y = self.y + (m // 2) * (1 - 2 * self.y)
        return x, y

    def peer(self, m):
        x, y = self.flip(m)
        return y * 4 + x * 2 + self.core

    def eighth(self, m, core):
        x, y = self.flip(m)
        return 32 * core + 16 * x + 8 * y


def send(src, dst, ss, rs, peer):
    return pltpu.make_async_remote_copy(src_ref=src, dst_ref=dst, send_sem=ss, recv_sem=rs,
                                        device_id={'kv': peer}, device_id_type=pl.DeviceIdType.MESH)


def al(v, m=8):
    return pl.multiple_of(v, m)


class Reduce:
    def __init__(self, places, part, r0, r1, own, s0, s1):
        self.p = places
        self.part, self.r0, self.r1, self.own, self.s0, self.s1 = part, r0, r1, own, s0, s1

    def pair_copy(self, c):
        src = al(c * CHUNK + 32 * (1 - self.p.core))
        return send(self.part.at[pl.ds(src, 32)], self.r0.at[pl.ds(al(c * 32), 32)], self.s0.at[0, c], self.s0.at[1, c], self.p.mate)

    def chip_copies(self, c):
        return [send(self.part.at[pl.ds(al(c * CHUNK + self.p.eighth(m, self.p.core)), 8)],
                     self.r1.at[pl.ds(al((c // 2) * 48 + 16 * (m - 1) + 8 * (c % 2)), 8)],
                     self.s1.at[0, 3 * c + m - 1], self.s1.at[1, 3 * c + m - 1], self.p.peer(m)) for m in (3, 1, 2)]

    def pair_step(self, c):
        self.pair_copy(c).wait_recv()
        rows = pl.ds(al(c * CHUNK + 32 * self.p.core), 32)
        v, s = merge_rows([self.part[rows, :], self.r0[pl.ds(al(c * 32), 32), :]])
        self.part[rows, :] = jnp.concatenate([v, s], axis=1)
        for cp in self.chip_copies(c):
            cp.start()

    def chip_step(self, c):
        @pl.when(c % 2 == 1)
        def _():
            for cp in self.chip_copies(c - 1) + self.chip_copies(c):
                cp.wait_recv()
            mine = jnp.concatenate([self.part[pl.ds(al(k * CHUNK + self.p.eighth(0, self.p.core)), 8), :] for k in (c - 1, c)], axis=0)
            v, s = merge_rows([mine] + [self.r1[pl.ds(al((c // 2) * 48 + 16 * n), 16), :] for n in range(3)])
            self.own[pl.ds(al((c - 1) * 8), 16), :] = normalise(v, s)

    def drain(self, c):
        self.pair_copy(c).wait_send()
        for cp in self.chip_copies(c):
            cp.wait_send()


class Attention:
    def __init__(self, off, kbuf, vbuf, q_v, kn_v, vn_v, p_col, js_col, part):
        self.refs = kbuf, vbuf, q_v, kn_v, vn_v, p_col, js_col, part
        self.sub = lax.broadcasted_iota(jnp.int32, (GROUP, 128), 0)
        self.lane = lax.broadcasted_iota(jnp.int32, (GROUP, 128), 1)
        self.slot_c = jnp.where((self.lane // SLOTS) == (self.sub % 2), (self.lane % SLOTS).astype(F32) + off.astype(F32), FAR)
        self.pick = [(self.sub // 2) == cc for cc in range(4)]
        self.iotas = [(lax.broadcasted_iota(jnp.int32, (16, HEAD_DIM), 0) + 16 * t).astype(F32).astype(BF16) for t in range(SLOTS // 16)]

    def rows(self, base):
        kbuf, vbuf, q_v, kn_v, vn_v, p_col, js_col, part = self.refs
        pick, iotas, lane, slot_c = self.pick, self.iotas, self.lane, self.slot_c

        def hits_of(b):
            js = jnp.broadcast_to(js_col[pl.ds(b, 1), :], (16, 128)).astype(BF16)
            js = jnp.concatenate([js, js], axis=1)
            return [io == js for io in iotas]

        def refresh(buf, new_ref, r0):
            out = []
            for i in range(GROUP):
                b = r0 + i
                hits = hits_of(b)
                fresh = jnp.broadcast_to(new_ref[pl.ds(b, 1), :], (16, HEAD_DIM)).astype(BF16)
                for t in range(SLOTS // 16):
                    piece = jnp.where(hits[t], fresh, buf[b, pl.ds(16 * t, 16), :])
                    buf[b, pl.ds(16 * t, 16), :] = piece
                    out.append(piece)
            return jnp.concatenate(out, axis=0)

        def scores(r0):
            rows = pl.ds(r0, GROUP)
            q = jnp.concatenate([q_v[rows, h * HEAD_DIM:(h + 1) * HEAD_DIM] for h in range(HEADS)], axis=0).astype(BF16)
            s = lax.dot_general(q, refresh(kbuf, kn_v, r0), (((1,), (1,)), ((), ())), preferred_element_type=F32)
            out = []
            for h in range(HEADS):
                sh = s[h * GROUP:(h + 1) * GROUP, :]
                c = sh[:, 384:512]
                for cc in range(3):
                    c = jnp.where(pick[cc], sh[:, cc * 128:(cc + 1) * 128], c)
                out.append(c)
            return out

        def soften(r0, cs):
            valid = slot_c <= p_col[pl.ds(r0, GROUP), :]
            stats = jnp.zeros((GROUP, 128), F32)
            ps = []
            for h in range(HEADS):
                c = jnp.where(valid, cs[h], NEG_LARGE)
                m = jnp.max(c, axis=1, keepdims=True)
                e = jnp.where(valid, jnp.exp(c - m), 0.0)
                l = jnp.sum(e, axis=1, keepdims=True)
                stats = jnp.where(lane == h, m, stats)
                stats = jnp.where(lane == HEADS + h, l, stats)
                ps.append(e)
            part[pl.ds(r0, GROUP), QW:PW] = stats
            return ps

        def values(r0, ps):
            pm = jnp.concatenate([jnp.concatenate([jnp.where(pick[cc], e, 0.0) for cc in range(4)], axis=1) for e in ps], axis=0).astype(BF16)
            o = jnp.dot(pm, refresh(vbuf, vn_v, r0), preferred_element_type=F32)
            rows = pl.ds(r0, GROUP)
            for h in range(HEADS):
                part[rows, h * HEAD_DIM:(h + 1) * HEAD_DIM] = o[h * GROUP:(h + 1) * GROUP, :]

        starts = [al(base + g * GROUP, GROUP) for g in range(CHUNK // GROUP)]
        cs = [scores(r0) for r0 in starts]
        ps = [soften(r0, c) for r0, c in zip(starts, cs)]
        for r0, e in zip(starts, ps):
            values(r0, e)


def chunk_rows(c):
    return pl.ds(pl.multiple_of(c * CHUNK, CHUNK), CHUNK)


def step_kernel(pos_hbm, freq_hbm, ns_hbm, sp_hbm, x_hbm, wq_hbm, wk_hbm, wv_hbm, k_hbm, v_hbm,
                own, kbuf, vbuf, sp_out,
                x_v, wq_v, wk_v, wv_v, n_v, q_v, kn_v, vn_v, p_col, js_col, cos_v, sin_v,
                part, r0, r1, pos_row, freq_ref, ns_ref, w_sem, k_sem, v_sem, s0, s1):
    p = Places()
    barrier = pltpu.get_barrier_semaphore()
    for peer in (p.mate, p.peer(1), p.peer(2), p.peer(3)):
        pl.semaphore_signal(barrier, inc=1, device_id={'kv': peer}, device_id_type=pl.DeviceIdType.MESH)
    off = lax.axis_index('kv') * SLOTS
    weights = ((x_hbm, x_v), (wk_hbm, wk_v), (wv_hbm, wv_v), (wq_hbm, wq_v), (sp_hbm, sp_out),
               (pos_hbm, pos_row), (freq_hbm, freq_ref), (ns_hbm, ns_ref))

    def w_in(n):
        return pltpu.make_async_copy(weights[n][0], weights[n][1], w_sem.at[n])

    def kv_in(c):
        return (pltpu.make_async_copy(k_hbm.at[chunk_rows(c)], kbuf.at[chunk_rows(c)], k_sem.at[c]),
                pltpu.make_async_copy(v_hbm.at[chunk_rows(c)], vbuf.at[chunk_rows(c)], v_sem.at[c]))

    for n in (5, 6, 7, 0, 1, 2, 3):
        w_in(n).start()
    for n in (5, 6, 7):
        w_in(n).wait()

    offf = off.astype(F32)

    @pl.loop(0, BATCH // 128)
    def _(t):
        rows = pl.ds(pl.multiple_of(t * 128, 128), 128)
        col = jnp.broadcast_to(pos_row[:, rows].astype(F32), (128, 128)).T
        p_col[rows, :] = col
        js = col - 512.0 * jnp.floor(col * (1.0 / 512.0)) - offf
        js_col[rows, :] = jnp.where((js >= 0.0) & (js < float(SLOTS)), js, -1.0)

    @pl.loop(0, BATCH // 64)
    def _(t):
        rows = pl.ds(pl.multiple_of(t * 64, 64), 64)
        s, c = sin_cos(p_col[rows, :] * freq_ref[...])
        lane = lax.broadcasted_iota(jnp.int32, (64, 128), 1)
        sin_v[rows, :] = jnp.where(lane < ROPE_HALF, -s, s)
        cos_v[rows, :] = c

    def rotate(t, rows):
        r = t[:, :ROPE_DIM]
        r = r * cos_v[rows, :] + pltpu.roll(r, ROPE_HALF, 1) * sin_v[rows, :]
        return jnp.concatenate([r, t[:, ROPE_DIM:]], axis=1)

    w_in(0).wait()
    for cp in kv_in(0) + kv_in(1):
        cp.start()
    gain = 1.0 + ns_ref[...].astype(F32).reshape(1, D_MODEL)

    @pl.loop(0, BATCH // 128)
    def _(i):
        rows = pl.ds(pl.multiple_of(i * 128, 128), 128)
        xf = x_v[rows, :].astype(F32)
        mean_sq = jnp.sum(xf * xf, axis=1, keepdims=True) * (1.0 / D_MODEL)
        n_v[rows, :] = (xf * lax.rsqrt(mean_sq + EPS) * gain).astype(BF16)

    for n in range(1, 4):
        w_in(n).wait()
    for c in range(2, NCHUNK):
        for cp in kv_in(c):
            cp.start()
    red = Reduce(p, part, r0, r1, own, s0, s1)
    att = Attention(off, kbuf, vbuf, q_v, kn_v, vn_v, p_col, js_col, part)

    def attend(c):
        @pl.when(c == NCHUNK // 2)
        def _():
            w_in(4).start()

        @pl.when(c % (ROWS // CHUNK) == 0)
        def _():
            rows = pl.ds(al(c * CHUNK, ROWS), ROWS)
            kn_v[rows, :] = rotate(jnp.dot(n_v[rows, :], wk_v[...], preferred_element_type=F32), rows)
            vn_v[rows, :] = jnp.dot(n_v[rows, :], wv_v[...], preferred_element_type=F32)
            for h in range(HEADS):
                cols = pl.ds(h * HEAD_DIM, HEAD_DIM)
                qh = jnp.dot(n_v[rows, :], wq_v[:, cols], preferred_element_type=F32)
                q_v[rows, cols] = rotate(qh, rows) * SCORE_SCALE

        for cp in kv_in(c):
            cp.wait()
        att.rows(c * CHUNK)

        @pl.when(c == 0)
        def _():
            pl.semaphore_wait(barrier, 4)

        red.pair_copy(c).start()

    lags = ((0, attend), (1, red.pair_step), (6, red.chip_step))

    @pl.loop(0, NCHUNK + lags[-1][0])
    def _(i):
        for lag, body in lags:
            @pl.when((i >= lag) & (i < NCHUNK + lag))
            def _(lag=lag, body=body):
                body(i - lag)

    w_in(4).wait()
    p_all = pos_row[...]
    slot_ids = off + lax.broadcasted_iota(jnp.int32, (SLOTS, BATCH), 0)
    sp_out[...] = jnp.where(slot_ids == (p_all & 511), p_all, sp_out[...])

    @pl.loop(0, NCHUNK)
    def _(c):
        red.drain(c)


def out_kernel(own, from_x, from_y, from_d, x_v, wo_v, b_ref, out_ref, g, lsem, ssem, rsem):
    p = Places()
    barrier = pltpu.get_barrier_semaphore()
    pl.semaphore_signal(barrier, inc=1, device_id={'kv': p.mate}, device_id_type=pl.DeviceIdType.MESH)
    refs = (own, from_x, from_y, from_d)

    def copy(n):
        return send(refs[n], g.at[n], ssem.at[n], rsem.at[n], p.mate)

    pl.semaphore_wait(barrier, 1)
    for n in range(4):
        copy(n).start()
    bias = b_ref[...].astype(F32).reshape(1, D_MODEL)

    def emit(blocks, core):
        rows = [al(t * CHUNK + p.eighth(n, core)) for n in range(4) for t in range(NCHUNK)]
        o = jnp.concatenate([t[...].astype(BF16) for t in blocks], axis=0)
        xin = jnp.concatenate([x_v[pl.ds(r, 8), :].astype(F32) for r in rows], axis=0)
        y = xin + jnp.dot(o, wo_v[...], preferred_element_type=F32) + bias
        for t, r in enumerate(rows):
            out_ref[pl.ds(r, 8), :] = y[8 * t:8 * t + 8, :]

    emit(refs, p.core)
    for n in range(4):
        copy(n).wait_recv()
    emit([g.at[n] for n in range(4)], 1 - p.core)
    for n in range(4):
        copy(n).wait_send()


def solution(mesh):
    row_spec = P('dp', None)
    cache_spec = P('dp', 'kv', None)
    slot_spec = P('dp', 'kv')
    vec_spec = P(None)
    mat_spec = P(None, None)
    hbm = pl.BlockSpec(memory_space=pltpu.HBM)
    vmem = pl.BlockSpec(memory_space=pltpu.VMEM)

    def in_hbm(a):
        return pltpu.with_memory_space_constraint(a, pltpu.HBM)

    def local_step(x_in, positions, k_cache, v_cache, slot_pos, norm_scale, w_q, w_k, w_v, w_o, b_o):
        own, k_out, v_out, sp_t = pl.pallas_call(
            step_kernel,
            out_shape=(jax.ShapeDtypeStruct((BATCH // 8, QW), F32),
                       pltpu.VMEM((BATCH, SLOTS, HEAD_DIM), BF16),
                       pltpu.VMEM((BATCH, SLOTS, HEAD_DIM), BF16),
                       pltpu.VMEM((SLOTS, BATCH), jnp.int32)),
            in_specs=[hbm] * 10,
            out_specs=(vmem,) * 4,
            scratch_shapes=[
                pltpu.VMEM((BATCH, D_MODEL), BF16),
                pltpu.VMEM((D_MODEL, QW), BF16),
                pltpu.VMEM((D_MODEL, HEAD_DIM), BF16),
                pltpu.VMEM((D_MODEL, HEAD_DIM), BF16),
                pltpu.VMEM((BATCH, D_MODEL), BF16),
                pltpu.VMEM((BATCH, QW), F32),
                pltpu.VMEM((BATCH, HEAD_DIM), F32),
                pltpu.VMEM((BATCH, HEAD_DIM), F32),
                pltpu.VMEM((BATCH, 128), F32),
                pltpu.VMEM((BATCH, 128), F32),
                pltpu.VMEM((BATCH, 128), F32),
                pltpu.VMEM((BATCH, 128), F32),
                pltpu.VMEM((BATCH, PW), F32),
                pltpu.VMEM((NCHUNK * 32, PW), F32),
                pltpu.VMEM((NCHUNK * 24, PW), F32),
                pltpu.VMEM((1, BATCH), jnp.int32),
                pltpu.VMEM((1, ROPE_DIM), F32),
                pltpu.VMEM((D_MODEL,), BF16),
                pltpu.SemaphoreType.DMA((8,)),
                pltpu.SemaphoreType.DMA((NCHUNK,)),
                pltpu.SemaphoreType.DMA((NCHUNK,)),
                pltpu.SemaphoreType.DMA((2, NCHUNK)),
                pltpu.SemaphoreType.DMA((2, 3 * NCHUNK)),
            ],
            cost_estimate=pl.CostEstimate(flops=30_000_000_000, bytes_accessed=40_000_000, transcendentals=200_000),
            compiler_params=pltpu.CompilerParams(collective_id=0, has_side_effects=True, vmem_limit_bytes=20 * 1024 * 1024),
        )(*[in_hbm(a) for a in (positions.reshape(1, BATCH), jnp.asarray(inv_freq_row()), norm_scale, slot_pos.T, x_in, w_q, w_k, w_v, k_cache, v_cache)])
        far = [lax.ppermute(own, 'kv', [(i, i ^ m) for i in range(8)]) for m in (2, 4, 6)]
        x_out = pl.pallas_call(
            out_kernel,
            out_shape=jax.ShapeDtypeStruct((BATCH, D_MODEL), F32),
            in_specs=[vmem] * 7,
            out_specs=vmem,
            scratch_shapes=[
                pltpu.VMEM((4, BATCH // 8, QW), F32),
                pltpu.SemaphoreType.DMA,
                pltpu.SemaphoreType.DMA((4,)),
                pltpu.SemaphoreType.DMA((4,)),
            ],
            cost_estimate=pl.CostEstimate(flops=1_200_000_000, bytes_accessed=6_000_000, transcendentals=0),
            compiler_params=pltpu.CompilerParams(collective_id=1, has_side_effects=True, vmem_limit_bytes=20 * 1024 * 1024),
        )(own, *far, x_in, w_o, b_o)
        return x_out.astype(BF16), k_out, v_out, sp_t.T

    return jax.shard_map(
        local_step,
        mesh=mesh,
        in_specs=(row_spec, P('dp'), cache_spec, cache_spec, slot_spec, vec_spec, mat_spec, mat_spec, mat_spec, mat_spec, vec_spec),
        out_specs=(row_spec, cache_spec, cache_spec, slot_spec),
        check_vma=False)
```

```python
import functools

import jax
import jax.numpy as jnp
import numpy as np
from jax import lax
from jax.experimental import pallas as pl
from jax.experimental.pallas import tpu as pltpu
from jax.sharding import PartitionSpec as P

HEADS = 4
HEAD_DIM = 256
ROPE_DIM = 128
ROPE_HALF = ROPE_DIM // 2
ROPE_BASE = 10000.0
EPS = 1e-6
SCORE_SCALE = HEAD_DIM ** -0.5
NEG_LARGE = float(np.finfo(np.float32).min)
FAR = 1e9
F32 = jnp.float32
BF16 = jnp.bfloat16

BATCH = 512
D_MODEL = 1152
SLOTS = 64
QW = HEADS * HEAD_DIM
PW = QW + 128
GROUP = 8
HALF = 32
STEP = 64
CHUNK = 64
NCHUNK = BATCH // CHUNK
ROWS = 512


def sin_cos(theta):
    k = jnp.floor(theta * np.float32(2.0 / np.pi) + 0.5)
    r = theta - k * np.float32(1.5703125)
    r = r - k * np.float32(4.83751296997070312e-4)
    r = r - k * np.float32(7.54978995489188e-8)
    r2 = r * r
    s = r + r * r2 * (-1.6666654611e-1 + r2 * (8.3321608736e-3 + r2 * -1.9515295891e-4))
    c = 1.0 - 0.5 * r2 + r2 * r2 * (4.166664568298827e-2 + r2 * (-1.388731625493765e-3 + r2 * 2.443315711809948e-5))
    q = k - 4.0 * jnp.floor(k * 0.25)
    swap = (q == 1.0) | (q == 3.0)
    sin_v = jnp.where(swap, c, s)
    cos_v = jnp.where(swap, s, c)
    sin_v = jnp.where(q >= 2.0, -sin_v, sin_v)
    cos_v = jnp.where((q == 1.0) | (q == 2.0), -cos_v, cos_v)
    return sin_v, cos_v


def inv_freq_row():
    i = np.arange(ROPE_DIM) % ROPE_HALF
    return (ROPE_BASE ** (-i / ROPE_HALF)).astype(np.float32).reshape(1, ROPE_DIM)


def merge_rows(blocks):
    stats = [t[:, QW:] for t in blocks]
    lane = lax.broadcasted_iota(jnp.int32, stats[0].shape, 1)
    top = functools.reduce(jnp.maximum, stats)
    factors = [jnp.exp(t - top) for t in stats]
    sums = [t * pltpu.roll(f, HEADS, 1) for t, f in zip(stats, factors)]
    out = jnp.where(lane < HEADS, top, functools.reduce(jnp.add, sums))
    vals = []
    for h in range(HEADS):
        terms = [t[:, h * HEAD_DIM:(h + 1) * HEAD_DIM] * f[:, h:h + 1] for t, f in zip(blocks, factors)]
        vals.append(functools.reduce(jnp.add, terms))
    return jnp.concatenate(vals, axis=1), out


def normalise(v, s):
    inv = 1.0 / s
    return jnp.concatenate([v[:, h * HEAD_DIM:(h + 1) * HEAD_DIM] * inv[:, HEADS + h:HEADS + h + 1] for h in range(HEADS)], axis=1)


class Places:
    def __init__(self):
        me = lax.axis_index('kv')
        self.core = me % 2
        self.x = (me // 2) % 2
        self.y = me // 4
        self.mate = me + 1 - 2 * self.core

    def flip(self, m):
        x = self.x + (m % 2) * (1 - 2 * self.x)
        y = self.y + (m // 2) * (1 - 2 * self.y)
        return x, y

    def peer(self, m):
        x, y = self.flip(m)
        return y * 4 + x * 2 + self.core

    def eighth(self, m, core):
        x, y = self.flip(m)
        return 32 * core + 16 * x + 8 * y


def send(src, dst, ss, rs, peer):
    return pltpu.make_async_remote_copy(src_ref=src, dst_ref=dst, send_sem=ss, recv_sem=rs,
                                        device_id={'kv': peer}, device_id_type=pl.DeviceIdType.MESH)


def al(v, m=8):
    return pl.multiple_of(v, m)


class Reduce:
    def __init__(self, places, part, r0, r1, own, s0, s1):
        self.p = places
        self.part, self.r0, self.r1, self.own, self.s0, self.s1 = part, r0, r1, own, s0, s1

    def pair_copy(self, c):
        src = al(c * CHUNK + 32 * (1 - self.p.core))
        return send(self.part.at[pl.ds(src, 32)], self.r0.at[pl.ds(al(c * 32), 32)], self.s0.at[0, c], self.s0.at[1, c], self.p.mate)

    def chip_copies(self, c):
        return [send(self.part.at[pl.ds(al(c * CHUNK + self.p.eighth(m, self.p.core)), 8)],
                     self.r1.at[pl.ds(al((c // 2) * 48 + 16 * (m - 1) + 8 * (c % 2)), 8)],
                     self.s1.at[0, 3 * c + m - 1], self.s1.at[1, 3 * c + m - 1], self.p.peer(m)) for m in (3, 1, 2)]

    def pair_step(self, c):
        self.pair_copy(c).wait_recv()
        rows = pl.ds(al(c * CHUNK + 32 * self.p.core), 32)
        v, s = merge_rows([self.part[rows, :], self.r0[pl.ds(al(c * 32), 32), :]])
        self.part[rows, :] = jnp.concatenate([v, s], axis=1)
        for cp in self.chip_copies(c):
            cp.start()

    def chip_step(self, c):
        @pl.when(c % 2 == 1)
        def _():
            for cp in self.chip_copies(c - 1) + self.chip_copies(c):
                cp.wait_recv()
            mine = jnp.concatenate([self.part[pl.ds(al(k * CHUNK + self.p.eighth(0, self.p.core)), 8), :] for k in (c - 1, c)], axis=0)
            v, s = merge_rows([mine] + [self.r1[pl.ds(al((c // 2) * 48 + 16 * n), 16), :] for n in range(3)])
            self.own[pl.ds(al((c - 1) * 8), 16), :] = normalise(v, s)

    def drain(self, c):
        self.pair_copy(c).wait_send()
        for cp in self.chip_copies(c):
            cp.wait_send()


class Attention:
    def __init__(self, off, kbuf, vbuf, q_v, kn_v, vn_v, p_col, js_col, part):
        self.refs = kbuf, vbuf, q_v, kn_v, vn_v, p_col, js_col, part
        self.sub = lax.broadcasted_iota(jnp.int32, (GROUP, 128), 0)
        self.lane = lax.broadcasted_iota(jnp.int32, (GROUP, 128), 1)
        self.slot_c = jnp.where((self.lane // SLOTS) == (self.sub % 2), (self.lane % SLOTS).astype(F32) + off.astype(F32), FAR)
        self.pick = [(self.sub // 2) == cc for cc in range(4)]
        self.iotas = [(lax.broadcasted_iota(jnp.int32, (16, HEAD_DIM), 0) + 16 * t).astype(F32).astype(BF16) for t in range(SLOTS // 16)]

    def rows(self, base):
        kbuf, vbuf, q_v, kn_v, vn_v, p_col, js_col, part = self.refs
        pick, iotas, lane, slot_c = self.pick, self.iotas, self.lane, self.slot_c

        def hits_of(b):
            js = jnp.broadcast_to(js_col[pl.ds(b, 1), :], (16, 128)).astype(BF16)
            js = jnp.concatenate([js, js], axis=1)
            return [io == js for io in iotas]

        def refresh(buf, new_ref, r0):
            out = []
            for i in range(GROUP):
                b = r0 + i
                hits = hits_of(b)
                fresh = jnp.broadcast_to(new_ref[pl.ds(b, 1), :], (16, HEAD_DIM)).astype(BF16)
                for t in range(SLOTS // 16):
                    piece = jnp.where(hits[t], fresh, buf[b, pl.ds(16 * t, 16), :])
                    buf[b, pl.ds(16 * t, 16), :] = piece
                    out.append(piece)
            return jnp.concatenate(out, axis=0)

        def scores(r0):
            rows = pl.ds(r0, GROUP)
            q = jnp.concatenate([q_v[rows, h * HEAD_DIM:(h + 1) * HEAD_DIM] for h in range(HEADS)], axis=0).astype(BF16)
            s = lax.dot_general(q, refresh(kbuf, kn_v, r0), (((1,), (1,)), ((), ())), preferred_element_type=F32)
            out = []
            for h in range(HEADS):
                sh = s[h * GROUP:(h + 1) * GROUP, :]
                c = sh[:, 384:512]
                for cc in range(3):
                    c = jnp.where(pick[cc], sh[:, cc * 128:(cc + 1) * 128], c)
                out.append(c)
            return out

        def soften(r0, cs):
            valid = slot_c <= p_col[pl.ds(r0, GROUP), :]
            stats = jnp.zeros((GROUP, 128), F32)
            ps = []
            for h in range(HEADS):
                c = jnp.where(valid, cs[h], NEG_LARGE)
                m = jnp.max(c, axis=1, keepdims=True)
                e = jnp.where(valid, jnp.exp(c - m), 0.0)
                l = jnp.sum(e, axis=1, keepdims=True)
                stats = jnp.where(lane == h, m, stats)
                stats = jnp.where(lane == HEADS + h, l, stats)
                ps.append(e)
            part[pl.ds(r0, GROUP), QW:PW] = stats
            return ps

        def values(r0, ps):
            pm = jnp.concatenate([jnp.concatenate([jnp.where(pick[cc], e, 0.0) for cc in range(4)], axis=1) for e in ps], axis=0).astype(BF16)
            o = jnp.dot(pm, refresh(vbuf, vn_v, r0), preferred_element_type=F32)
            rows = pl.ds(r0, GROUP)
            for h in range(HEADS):
                part[rows, h * HEAD_DIM:(h + 1) * HEAD_DIM] = o[h * GROUP:(h + 1) * GROUP, :]

        starts = [al(base + g * GROUP, GROUP) for g in range(HALF // GROUP)]
        cs = [scores(r0) for r0 in starts]
        ps = [soften(r0, c) for r0, c in zip(starts, cs)]
        for r0, e in zip(starts, ps):
            values(r0, e)


def chunk_rows(c):
    return pl.ds(pl.multiple_of(c * CHUNK, CHUNK), CHUNK)


def step_kernel(pos_hbm, freq_hbm, ns_hbm, sp_hbm, x_hbm, wq_hbm, wk_hbm, wv_hbm, wo_hbm, k_hbm, v_hbm,
                own, kbuf, vbuf, sp_out, x_v, wo_v,
                wq_v, wk_v, wv_v, n_v, q_v, kn_v, vn_v, p_col, js_col, cos_v, sin_v,
                part, r0, r1, pos_row, freq_ref, ns_ref, w_sem, k_sem, v_sem, s0, s1):
    p = Places()
    barrier = pltpu.get_barrier_semaphore()
    for peer in (p.mate, p.peer(1), p.peer(2), p.peer(3)):
        pl.semaphore_signal(barrier, inc=1, device_id={'kv': peer}, device_id_type=pl.DeviceIdType.MESH)
    off = lax.axis_index('kv') * SLOTS
    weights = ((x_hbm, x_v), (wk_hbm, wk_v), (wv_hbm, wv_v), (wq_hbm, wq_v), (sp_hbm, sp_out),
               (pos_hbm, pos_row), (freq_hbm, freq_ref), (ns_hbm, ns_ref), (wo_hbm, wo_v))

    def w_in(n):
        return pltpu.make_async_copy(weights[n][0], weights[n][1], w_sem.at[n])

    def kv_in(c):
        return (pltpu.make_async_copy(k_hbm.at[chunk_rows(c)], kbuf.at[chunk_rows(c)], k_sem.at[c]),
                pltpu.make_async_copy(v_hbm.at[chunk_rows(c)], vbuf.at[chunk_rows(c)], v_sem.at[c]))

    for n in (5, 6, 7, 0, 1, 2, 3):
        w_in(n).start()
    for n in (5, 6, 7):
        w_in(n).wait()

    offf = off.astype(F32)

    @pl.loop(0, BATCH // 128)
    def _(t):
        rows = pl.ds(pl.multiple_of(t * 128, 128), 128)
        col = jnp.broadcast_to(pos_row[:, rows].astype(F32), (128, 128)).T
        p_col[rows, :] = col
        js = col - 512.0 * jnp.floor(col * (1.0 / 512.0)) - offf
        js_col[rows, :] = jnp.where((js >= 0.0) & (js < float(SLOTS)), js, -1.0)

    @pl.loop(0, BATCH // 64)
    def _(t):
        rows = pl.ds(pl.multiple_of(t * 64, 64), 64)
        s, c = sin_cos(p_col[rows, :] * freq_ref[...])
        lane = lax.broadcasted_iota(jnp.int32, (64, 128), 1)
        sin_v[rows, :] = jnp.where(lane < ROPE_HALF, -s, s)
        cos_v[rows, :] = c

    def rotate(t, rows):
        r = t[:, :ROPE_DIM]
        r = r * cos_v[rows, :] + pltpu.roll(r, ROPE_HALF, 1) * sin_v[rows, :]
        return jnp.concatenate([r, t[:, ROPE_DIM:]], axis=1)

    w_in(0).wait()
    for cp in kv_in(0) + kv_in(1):
        cp.start()
    gain = 1.0 + ns_ref[...].astype(F32).reshape(1, D_MODEL)

    @pl.loop(0, BATCH // 128)
    def _(i):
        rows = pl.ds(pl.multiple_of(i * 128, 128), 128)
        xf = x_v[rows, :].astype(F32)
        mean_sq = jnp.sum(xf * xf, axis=1, keepdims=True) * (1.0 / D_MODEL)
        n_v[rows, :] = (xf * lax.rsqrt(mean_sq + EPS) * gain).astype(BF16)

    for n in range(1, 4):
        w_in(n).wait()
    for c in range(2, NCHUNK):
        for cp in kv_in(c):
            cp.start()
    red = Reduce(p, part, r0, r1, own, s0, s1)
    att = Attention(off, kbuf, vbuf, q_v, kn_v, vn_v, p_col, js_col, part)

    def attend(c):
        @pl.when(c == NCHUNK - 1)
        def _():
            w_in(4).start()
            w_in(8).start()

        @pl.when(c % (ROWS // CHUNK) == 0)
        def _():
            rows = pl.ds(al(c * CHUNK, ROWS), ROWS)
            kn_v[rows, :] = rotate(jnp.dot(n_v[rows, :], wk_v[...], preferred_element_type=F32), rows)
            vn_v[rows, :] = jnp.dot(n_v[rows, :], wv_v[...], preferred_element_type=F32)
            for h in range(HEADS):
                cols = pl.ds(h * HEAD_DIM, HEAD_DIM)
                qh = jnp.dot(n_v[rows, :], wq_v[:, cols], preferred_element_type=F32)
                q_v[rows, cols] = rotate(qh, rows) * SCORE_SCALE

        for cp in kv_in(c):
            cp.wait()
        att.rows(c * CHUNK + HALF * (1 - p.core))

        @pl.when(c == 0)
        def _():
            pl.semaphore_wait(barrier, 4)

        red.pair_copy(c).start()
        att.rows(c * CHUNK + HALF * p.core)

    lags = ((0, attend), (1, red.pair_step), (6, red.chip_step))

    @pl.loop(0, NCHUNK + lags[-1][0])
    def _(i):
        for lag, body in lags:
            @pl.when((i >= lag) & (i < NCHUNK + lag))
            def _(lag=lag, body=body):
                body(i - lag)

    w_in(4).wait()
    w_in(8).wait()
    p_all = pos_row[...]
    slot_ids = off + lax.broadcasted_iota(jnp.int32, (SLOTS, BATCH), 0)
    sp_out[...] = jnp.where(slot_ids == (p_all & 511), p_all, sp_out[...])

    @pl.loop(0, NCHUNK)
    def _(c):
        red.drain(c)


def out_kernel(own, from_x, from_y, from_d, x_v, wo_v, b_ref, out_ref, g, lsem, ssem, rsem):
    p = Places()
    barrier = pltpu.get_barrier_semaphore()
    pl.semaphore_signal(barrier, inc=1, device_id={'kv': p.mate}, device_id_type=pl.DeviceIdType.MESH)
    refs = (own, from_x, from_y, from_d)

    def copy(n):
        return send(refs[n], g.at[n], ssem.at[n], rsem.at[n], p.mate)

    pl.semaphore_wait(barrier, 1)
    for n in range(4):
        copy(n).start()
    bias = b_ref[...].astype(F32).reshape(1, D_MODEL)

    def emit(blocks, core):
        rows = [al(t * CHUNK + p.eighth(n, core)) for n in range(4) for t in range(NCHUNK)]
        o = jnp.concatenate([t[...].astype(BF16) for t in blocks], axis=0)
        xin = jnp.concatenate([x_v[pl.ds(r, 8), :].astype(F32) for r in rows], axis=0)
        y = xin + jnp.dot(o, wo_v[...], preferred_element_type=F32) + bias
        for t, r in enumerate(rows):
            out_ref[pl.ds(r, 8), :] = y[8 * t:8 * t + 8, :]

    emit(refs, p.core)
    for n in range(4):
        copy(n).wait_recv()
    emit([g.at[n] for n in range(4)], 1 - p.core)
    for n in range(4):
        copy(n).wait_send()


def solution(mesh):
    row_spec = P('dp', None)
    cache_spec = P('dp', 'kv', None)
    slot_spec = P('dp', 'kv')
    vec_spec = P(None)
    mat_spec = P(None, None)
    hbm = pl.BlockSpec(memory_space=pltpu.HBM)
    vmem = pl.BlockSpec(memory_space=pltpu.VMEM)

    def in_hbm(a):
        return pltpu.with_memory_space_constraint(a, pltpu.HBM)

    def local_step(x_in, positions, k_cache, v_cache, slot_pos, norm_scale, w_q, w_k, w_v, w_o, b_o):
        own, k_out, v_out, sp_t, x_keep, wo_keep = pl.pallas_call(
            step_kernel,
            out_shape=(jax.ShapeDtypeStruct((BATCH // 8, QW), F32),
                       pltpu.VMEM((BATCH, SLOTS, HEAD_DIM), BF16),
                       pltpu.VMEM((BATCH, SLOTS, HEAD_DIM), BF16),
                       pltpu.VMEM((SLOTS, BATCH), jnp.int32),
                       pltpu.VMEM((BATCH, D_MODEL), BF16),
                       pltpu.VMEM((QW, D_MODEL), BF16)),
            in_specs=[hbm] * 11,
            out_specs=(vmem,) * 6,
            scratch_shapes=[
                pltpu.VMEM((D_MODEL, QW), BF16),
                pltpu.VMEM((D_MODEL, HEAD_DIM), BF16),
                pltpu.VMEM((D_MODEL, HEAD_DIM), BF16),
                pltpu.VMEM((BATCH, D_MODEL), BF16),
                pltpu.VMEM((BATCH, QW), F32),
                pltpu.VMEM((BATCH, HEAD_DIM), F32),
                pltpu.VMEM((BATCH, HEAD_DIM), F32),
                pltpu.VMEM((BATCH, 128), F32),
                pltpu.VMEM((BATCH, 128), F32),
                pltpu.VMEM((BATCH, 128), F32),
                pltpu.VMEM((BATCH, 128), F32),
                pltpu.VMEM((BATCH, PW), F32),
                pltpu.VMEM((NCHUNK * 32, PW), F32),
                pltpu.VMEM((NCHUNK * 24, PW), F32),
                pltpu.VMEM((1, BATCH), jnp.int32),
                pltpu.VMEM((1, ROPE_DIM), F32),
                pltpu.VMEM((D_MODEL,), BF16),
                pltpu.SemaphoreType.DMA((9,)),
                pltpu.SemaphoreType.DMA((NCHUNK,)),
                pltpu.SemaphoreType.DMA((NCHUNK,)),
                pltpu.SemaphoreType.DMA((2, NCHUNK)),
                pltpu.SemaphoreType.DMA((2, 3 * NCHUNK)),
            ],
            cost_estimate=pl.CostEstimate(flops=30_000_000_000, bytes_accessed=40_000_000, transcendentals=200_000),
            compiler_params=pltpu.CompilerParams(collective_id=0, has_side_effects=True, vmem_limit_bytes=18 * 1024 * 1024),
        )(*[in_hbm(a) for a in (positions.reshape(1, BATCH), jnp.asarray(inv_freq_row()), norm_scale, slot_pos.T, x_in, w_q, w_k, w_v, w_o, k_cache, v_cache)])
        far = [lax.ppermute(own, 'kv', [(i, i ^ m) for i in range(8)]) for m in (2, 4, 6)]
        x_out = pl.pallas_call(
            out_kernel,
            out_shape=jax.ShapeDtypeStruct((BATCH, D_MODEL), F32),
            in_specs=[vmem] * 7,
            out_specs=vmem,
            scratch_shapes=[
                pltpu.VMEM((4, BATCH // 8, QW), F32),
                pltpu.SemaphoreType.DMA,
                pltpu.SemaphoreType.DMA((4,)),
                pltpu.SemaphoreType.DMA((4,)),
            ],
            cost_estimate=pl.CostEstimate(flops=1_200_000_000, bytes_accessed=6_000_000, transcendentals=0),
            compiler_params=pltpu.CompilerParams(collective_id=1, has_side_effects=True, vmem_limit_bytes=18 * 1024 * 1024),
        )(own, *far, x_keep, wo_keep, b_o)
        return x_out.astype(BF16), k_out, v_out, sp_t.T

    return jax.shard_map(
        local_step,
        mesh=mesh,
        in_specs=(row_spec, P('dp'), cache_spec, cache_spec, slot_spec, vec_spec, mat_spec, mat_spec, mat_spec, mat_spec, vec_spec),
        out_specs=(row_spec, cache_spec, cache_spec, slot_spec),
        check_vma=False)
```

```python
import functools

import jax
import jax.numpy as jnp
import numpy as np
from jax import lax
from jax.experimental import pallas as pl
from jax.experimental.pallas import tpu as pltpu
from jax.sharding import PartitionSpec as P

HEADS = 4
HEAD_DIM = 256
ROPE_DIM = 128
ROPE_HALF = ROPE_DIM // 2
ROPE_BASE = 10000.0
EPS = 1e-6
SCORE_SCALE = HEAD_DIM ** -0.5
NEG_LARGE = float(np.finfo(np.float32).min)
FAR = 1e9
F32 = jnp.float32
BF16 = jnp.bfloat16

BATCH = 512
D_MODEL = 1152
SLOTS = 64
QW = HEADS * HEAD_DIM
PW = QW + 128
GROUP = 8
HALF = 32
STEP = 64
CHUNK = 64
NCHUNK = BATCH // CHUNK
ROWS = 512


def sin_cos(theta):
    k = jnp.floor(theta * np.float32(2.0 / np.pi) + 0.5)
    r = theta - k * np.float32(1.5703125)
    r = r - k * np.float32(4.83751296997070312e-4)
    r = r - k * np.float32(7.54978995489188e-8)
    r2 = r * r
    s = r + r * r2 * (-1.6666654611e-1 + r2 * (8.3321608736e-3 + r2 * -1.9515295891e-4))
    c = 1.0 - 0.5 * r2 + r2 * r2 * (4.166664568298827e-2 + r2 * (-1.388731625493765e-3 + r2 * 2.443315711809948e-5))
    q = k - 4.0 * jnp.floor(k * 0.25)
    swap = (q == 1.0) | (q == 3.0)
    sin_v = jnp.where(swap, c, s)
    cos_v = jnp.where(swap, s, c)
    sin_v = jnp.where(q >= 2.0, -sin_v, sin_v)
    cos_v = jnp.where((q == 1.0) | (q == 2.0), -cos_v, cos_v)
    return sin_v, cos_v


def inv_freq_row():
    i = np.arange(ROPE_DIM) % ROPE_HALF
    return (ROPE_BASE ** (-i / ROPE_HALF)).astype(np.float32).reshape(1, ROPE_DIM)


def merge_rows(blocks):
    stats = [t[:, QW:] for t in blocks]
    lane = lax.broadcasted_iota(jnp.int32, stats[0].shape, 1)
    top = functools.reduce(jnp.maximum, stats)
    factors = [jnp.exp(t - top) for t in stats]
    sums = [t * pltpu.roll(f, HEADS, 1) for t, f in zip(stats, factors)]
    out = jnp.where(lane < HEADS, top, functools.reduce(jnp.add, sums))
    vals = []
    for h in range(HEADS):
        terms = [t[:, h * HEAD_DIM:(h + 1) * HEAD_DIM] * f[:, h:h + 1] for t, f in zip(blocks, factors)]
        vals.append(functools.reduce(jnp.add, terms))
    return jnp.concatenate(vals, axis=1), out


def normalise(v, s):
    inv = 1.0 / s
    return jnp.concatenate([v[:, h * HEAD_DIM:(h + 1) * HEAD_DIM] * inv[:, HEADS + h:HEADS + h + 1] for h in range(HEADS)], axis=1)


class Places:
    def __init__(self):
        me = lax.axis_index('kv')
        self.core = me % 2
        self.x = (me // 2) % 2
        self.y = me // 4
        self.mate = me + 1 - 2 * self.core

    def flip(self, m):
        x = self.x + (m % 2) * (1 - 2 * self.x)
        y = self.y + (m // 2) * (1 - 2 * self.y)
        return x, y

    def peer(self, m):
        x, y = self.flip(m)
        return y * 4 + x * 2 + self.core

    def eighth(self, m, core):
        x, y = self.flip(m)
        return 32 * core + 16 * x + 8 * y


def send(src, dst, ss, rs, peer):
    return pltpu.make_async_remote_copy(src_ref=src, dst_ref=dst, send_sem=ss, recv_sem=rs,
                                        device_id={'kv': peer}, device_id_type=pl.DeviceIdType.MESH)


def al(v, m=8):
    return pl.multiple_of(v, m)


class Reduce:
    def __init__(self, places, part, r0, r1, own, s0, s1):
        self.p = places
        self.part, self.r0, self.r1, self.own, self.s0, self.s1 = part, r0, r1, own, s0, s1

    def pair_copy(self, c):
        src = al(c * CHUNK + 32 * (1 - self.p.core))
        return send(self.part.at[pl.ds(src, 32)], self.r0.at[pl.ds(al(c * 32), 32)], self.s0.at[0, c], self.s0.at[1, c], self.p.mate)

    def chip_copies(self, c):
        return [send(self.part.at[pl.ds(al(c * CHUNK + self.p.eighth(m, self.p.core)), 8)],
                     self.r1.at[pl.ds(al((c // 2) * 48 + 16 * (m - 1) + 8 * (c % 2)), 8)],
                     self.s1.at[0, 3 * c + m - 1], self.s1.at[1, 3 * c + m - 1], self.p.peer(m)) for m in (3, 1, 2)]

    def pair_step(self, c):
        self.pair_copy(c).wait_recv()
        rows = pl.ds(al(c * CHUNK + 32 * self.p.core), 32)
        v, s = merge_rows([self.part[rows, :], self.r0[pl.ds(al(c * 32), 32), :]])
        self.part[rows, :] = jnp.concatenate([v, s], axis=1)
        for cp in self.chip_copies(c):
            cp.start()

    def chip_step(self, c):
        @pl.when(c % 2 == 1)
        def _():
            for cp in self.chip_copies(c - 1) + self.chip_copies(c):
                cp.wait_recv()
            mine = jnp.concatenate([self.part[pl.ds(al(k * CHUNK + self.p.eighth(0, self.p.core)), 8), :] for k in (c - 1, c)], axis=0)
            v, s = merge_rows([mine] + [self.r1[pl.ds(al((c // 2) * 48 + 16 * n), 16), :] for n in range(3)])
            self.own[pl.ds(al((c - 1) * 8), 16), :] = normalise(v, s)

    def drain(self, c):
        self.pair_copy(c).wait_send()
        for cp in self.chip_copies(c):
            cp.wait_send()


class Attention:
    def __init__(self, off, kbuf, vbuf, q_v, kn_v, vn_v, p_col, js_col, part):
        self.refs = kbuf, vbuf, q_v, kn_v, vn_v, p_col, js_col, part
        self.sub = lax.broadcasted_iota(jnp.int32, (GROUP, 128), 0)
        self.lane = lax.broadcasted_iota(jnp.int32, (GROUP, 128), 1)
        self.slot_c = jnp.where((self.lane // SLOTS) == (self.sub % 2), (self.lane % SLOTS).astype(F32) + off.astype(F32), FAR)
        self.pick = [(self.sub // 2) == cc for cc in range(4)]
        self.iotas = [(lax.broadcasted_iota(jnp.int32, (16, HEAD_DIM), 0) + 16 * t).astype(F32).astype(BF16) for t in range(SLOTS // 16)]

    def rows(self, base, count):
        kbuf, vbuf, q_v, kn_v, vn_v, p_col, js_col, part = self.refs
        pick, iotas, lane, slot_c = self.pick, self.iotas, self.lane, self.slot_c

        def hits_of(b):
            js = jnp.broadcast_to(js_col[pl.ds(b, 1), :], (16, 128)).astype(BF16)
            js = jnp.concatenate([js, js], axis=1)
            return [io == js for io in iotas]

        def refresh(buf, new_ref, r0):
            out = []
            for i in range(GROUP):
                b = r0 + i
                hits = hits_of(b)
                fresh = jnp.broadcast_to(new_ref[pl.ds(b, 1), :], (16, HEAD_DIM)).astype(BF16)
                for t in range(SLOTS // 16):
                    piece = jnp.where(hits[t], fresh, buf[b, pl.ds(16 * t, 16), :])
                    buf[b, pl.ds(16 * t, 16), :] = piece
                    out.append(piece)
            return jnp.concatenate(out, axis=0)

        def scores(r0):
            rows = pl.ds(r0, GROUP)
            q = jnp.concatenate([q_v[rows, h * HEAD_DIM:(h + 1) * HEAD_DIM] for h in range(HEADS)], axis=0).astype(BF16)
            s = lax.dot_general(q, refresh(kbuf, kn_v, r0), (((1,), (1,)), ((), ())), preferred_element_type=F32)
            out = []
            for h in range(HEADS):
                sh = s[h * GROUP:(h + 1) * GROUP, :]
                c = sh[:, 384:512]
                for cc in range(3):
                    c = jnp.where(pick[cc], sh[:, cc * 128:(cc + 1) * 128], c)
                out.append(c)
            return out

        def soften(r0, cs):
            valid = slot_c <= p_col[pl.ds(r0, GROUP), :]
            stats = jnp.zeros((GROUP, 128), F32)
            ps = []
            for h in range(HEADS):
                c = jnp.where(valid, cs[h], NEG_LARGE)
                m = jnp.max(c, axis=1, keepdims=True)
                e = jnp.where(valid, jnp.exp(c - m), 0.0)
                l = jnp.sum(e, axis=1, keepdims=True)
                stats = jnp.where(lane == h, m, stats)
                stats = jnp.where(lane == HEADS + h, l, stats)
                ps.append(e)
            part[pl.ds(r0, GROUP), QW:PW] = stats
            return ps

        def values(r0, ps):
            pm = jnp.concatenate([jnp.concatenate([jnp.where(pick[cc], e, 0.0) for cc in range(4)], axis=1) for e in ps], axis=0).astype(BF16)
            o = jnp.dot(pm, refresh(vbuf, vn_v, r0), preferred_element_type=F32)
            rows = pl.ds(r0, GROUP)
            for h in range(HEADS):
                part[rows, h * HEAD_DIM:(h + 1) * HEAD_DIM] = o[h * GROUP:(h + 1) * GROUP, :]

        starts = [al(base + g * GROUP, GROUP) for g in range(count // GROUP)]
        cs = [scores(r0) for r0 in starts]
        ps = [soften(r0, c) for r0, c in zip(starts, cs)]
        for r0, e in zip(starts, ps):
            values(r0, e)


def chunk_rows(c):
    return pl.ds(pl.multiple_of(c * CHUNK, CHUNK), CHUNK)


def step_kernel(pos_hbm, freq_hbm, ns_hbm, sp_hbm, x_hbm, wq_hbm, wk_hbm, wv_hbm, wo_hbm, k_hbm, v_hbm,
                own, kbuf, vbuf, sp_out, x_v, wo_v,
                wq_v, wk_v, wv_v, n_v, q_v, kn_v, vn_v, p_col, js_col, cos_v, sin_v,
                part, r0, r1, pos_row, freq_ref, ns_ref, w_sem, k_sem, v_sem, s0, s1):
    p = Places()
    barrier = pltpu.get_barrier_semaphore()
    for peer in (p.mate, p.peer(1), p.peer(2), p.peer(3)):
        pl.semaphore_signal(barrier, inc=1, device_id={'kv': peer}, device_id_type=pl.DeviceIdType.MESH)
    off = lax.axis_index('kv') * SLOTS
    weights = ((x_hbm, x_v), (wk_hbm, wk_v), (wv_hbm, wv_v), (wq_hbm, wq_v), (sp_hbm, sp_out),
               (pos_hbm, pos_row), (freq_hbm, freq_ref), (ns_hbm, ns_ref), (wo_hbm, wo_v))

    def w_in(n):
        return pltpu.make_async_copy(weights[n][0], weights[n][1], w_sem.at[n])

    def kv_in(c):
        return (pltpu.make_async_copy(k_hbm.at[chunk_rows(c)], kbuf.at[chunk_rows(c)], k_sem.at[c]),
                pltpu.make_async_copy(v_hbm.at[chunk_rows(c)], vbuf.at[chunk_rows(c)], v_sem.at[c]))

    for n in (5, 6, 7, 0, 1, 2, 3):
        w_in(n).start()
    for n in (5, 6, 7):
        w_in(n).wait()

    offf = off.astype(F32)

    @pl.loop(0, BATCH // 128)
    def _(t):
        rows = pl.ds(pl.multiple_of(t * 128, 128), 128)
        col = jnp.broadcast_to(pos_row[:, rows].astype(F32), (128, 128)).T
        p_col[rows, :] = col
        js = col - 512.0 * jnp.floor(col * (1.0 / 512.0)) - offf
        js_col[rows, :] = jnp.where((js >= 0.0) & (js < float(SLOTS)), js, -1.0)

    @pl.loop(0, BATCH // 64)
    def _(t):
        rows = pl.ds(pl.multiple_of(t * 64, 64), 64)
        s, c = sin_cos(p_col[rows, :] * freq_ref[...])
        lane = lax.broadcasted_iota(jnp.int32, (64, 128), 1)
        sin_v[rows, :] = jnp.where(lane < ROPE_HALF, -s, s)
        cos_v[rows, :] = c

    def rotate(t, rows):
        r = t[:, :ROPE_DIM]
        r = r * cos_v[rows, :] + pltpu.roll(r, ROPE_HALF, 1) * sin_v[rows, :]
        return jnp.concatenate([r, t[:, ROPE_DIM:]], axis=1)

    w_in(0).wait()
    for cp in kv_in(0) + kv_in(1):
        cp.start()
    gain = 1.0 + ns_ref[...].astype(F32).reshape(1, D_MODEL)

    @pl.loop(0, BATCH // 128)
    def _(i):
        rows = pl.ds(pl.multiple_of(i * 128, 128), 128)
        xf = x_v[rows, :].astype(F32)
        mean_sq = jnp.sum(xf * xf, axis=1, keepdims=True) * (1.0 / D_MODEL)
        n_v[rows, :] = (xf * lax.rsqrt(mean_sq + EPS) * gain).astype(BF16)

    for n in range(1, 4):
        w_in(n).wait()
    for c in range(2, NCHUNK):
        for cp in kv_in(c):
            cp.start()
    red = Reduce(p, part, r0, r1, own, s0, s1)
    att = Attention(off, kbuf, vbuf, q_v, kn_v, vn_v, p_col, js_col, part)

    def attend(c):
        @pl.when(c == NCHUNK - 1)
        def _():
            w_in(4).start()
            w_in(8).start()

        @pl.when(c % (ROWS // CHUNK) == 0)
        def _():
            rows = pl.ds(al(c * CHUNK, ROWS), ROWS)
            kn_v[rows, :] = rotate(jnp.dot(n_v[rows, :], wk_v[...], preferred_element_type=F32), rows)
            vn_v[rows, :] = jnp.dot(n_v[rows, :], wv_v[...], preferred_element_type=F32)
            for h in range(HEADS):
                cols = pl.ds(h * HEAD_DIM, HEAD_DIM)
                qh = jnp.dot(n_v[rows, :], wq_v[:, cols], preferred_element_type=F32)
                q_v[rows, cols] = rotate(qh, rows) * SCORE_SCALE

        for cp in kv_in(c):
            cp.wait()
        @pl.when(c < NCHUNK - 1)
        def _():
            att.rows(c * CHUNK, CHUNK)

        @pl.when(c == NCHUNK - 1)
        def _():
            att.rows(c * CHUNK + HALF * (1 - p.core), HALF)

        @pl.when(c == 0)
        def _():
            pl.semaphore_wait(barrier, 4)

        red.pair_copy(c).start()

        @pl.when(c == NCHUNK - 1)
        def _():
            att.rows(c * CHUNK + HALF * p.core, HALF)

    lags = ((0, attend), (1, red.pair_step), (6, red.chip_step))

    @pl.loop(0, NCHUNK + lags[-1][0])
    def _(i):
        for lag, body in lags:
            @pl.when((i >= lag) & (i < NCHUNK + lag))
            def _(lag=lag, body=body):
                body(i - lag)

    w_in(4).wait()
    w_in(8).wait()
    p_all = pos_row[...]
    slot_ids = off + lax.broadcasted_iota(jnp.int32, (SLOTS, BATCH), 0)
    sp_out[...] = jnp.where(slot_ids == (p_all & 511), p_all, sp_out[...])

    @pl.loop(0, NCHUNK)
    def _(c):
        red.drain(c)


def out_kernel(own, from_x, from_y, from_d, x_v, wo_v, b_ref, out_ref, g, lsem, ssem, rsem):
    p = Places()
    barrier = pltpu.get_barrier_semaphore()
    pl.semaphore_signal(barrier, inc=1, device_id={'kv': p.mate}, device_id_type=pl.DeviceIdType.MESH)
    refs = (own, from_x, from_y, from_d)

    def copy(n):
        return send(refs[n], g.at[n], ssem.at[n], rsem.at[n], p.mate)

    pl.semaphore_wait(barrier, 1)
    for n in range(4):
        copy(n).start()
    bias = b_ref[...].astype(F32).reshape(1, D_MODEL)

    def emit(blocks, core):
        rows = [al(t * CHUNK + p.eighth(n, core)) for n in range(4) for t in range(NCHUNK)]
        o = jnp.concatenate([t[...].astype(BF16) for t in blocks], axis=0)
        xin = jnp.concatenate([x_v[pl.ds(r, 8), :].astype(F32) for r in rows], axis=0)
        y = xin + jnp.dot(o, wo_v[...], preferred_element_type=F32) + bias
        for t, r in enumerate(rows):
            out_ref[pl.ds(r, 8), :] = y[8 * t:8 * t + 8, :].astype(BF16)

    emit(refs, p.core)
    for n in range(4):
        copy(n).wait_recv()
    emit([g.at[n] for n in range(4)], 1 - p.core)
    for n in range(4):
        copy(n).wait_send()


def solution(mesh):
    row_spec = P('dp', None)
    cache_spec = P('dp', 'kv', None)
    slot_spec = P('dp', 'kv')
    vec_spec = P(None)
    mat_spec = P(None, None)
    hbm = pl.BlockSpec(memory_space=pltpu.HBM)
    vmem = pl.BlockSpec(memory_space=pltpu.VMEM)

    def in_hbm(a):
        return pltpu.with_memory_space_constraint(a, pltpu.HBM)

    def local_step(x_in, positions, k_cache, v_cache, slot_pos, norm_scale, w_q, w_k, w_v, w_o, b_o):
        own, k_out, v_out, sp_t, x_keep, wo_keep = pl.pallas_call(
            step_kernel,
            out_shape=(jax.ShapeDtypeStruct((BATCH // 8, QW), F32),
                       pltpu.VMEM((BATCH, SLOTS, HEAD_DIM), BF16),
                       pltpu.VMEM((BATCH, SLOTS, HEAD_DIM), BF16),
                       pltpu.VMEM((SLOTS, BATCH), jnp.int32),
                       pltpu.VMEM((BATCH, D_MODEL), BF16),
                       pltpu.VMEM((QW, D_MODEL), BF16)),
            in_specs=[hbm] * 11,
            out_specs=(vmem,) * 6,
            scratch_shapes=[
                pltpu.VMEM((D_MODEL, QW), BF16),
                pltpu.VMEM((D_MODEL, HEAD_DIM), BF16),
                pltpu.VMEM((D_MODEL, HEAD_DIM), BF16),
                pltpu.VMEM((BATCH, D_MODEL), BF16),
                pltpu.VMEM((BATCH, QW), F32),
                pltpu.VMEM((BATCH, HEAD_DIM), F32),
                pltpu.VMEM((BATCH, HEAD_DIM), F32),
                pltpu.VMEM((BATCH, 128), F32),
                pltpu.VMEM((BATCH, 128), F32),
                pltpu.VMEM((BATCH, 128), F32),
                pltpu.VMEM((BATCH, 128), F32),
                pltpu.VMEM((BATCH, PW), F32),
                pltpu.VMEM((NCHUNK * 32, PW), F32),
                pltpu.VMEM((NCHUNK * 24, PW), F32),
                pltpu.VMEM((1, BATCH), jnp.int32),
                pltpu.VMEM((1, ROPE_DIM), F32),
                pltpu.VMEM((D_MODEL,), BF16),
                pltpu.SemaphoreType.DMA((9,)),
                pltpu.SemaphoreType.DMA((NCHUNK,)),
                pltpu.SemaphoreType.DMA((NCHUNK,)),
                pltpu.SemaphoreType.DMA((2, NCHUNK)),
                pltpu.SemaphoreType.DMA((2, 3 * NCHUNK)),
            ],
            cost_estimate=pl.CostEstimate(flops=30_000_000_000, bytes_accessed=40_000_000, transcendentals=200_000),
            compiler_params=pltpu.CompilerParams(collective_id=0, has_side_effects=True, vmem_limit_bytes=18 * 1024 * 1024),
        )(*[in_hbm(a) for a in (positions.reshape(1, BATCH), jnp.asarray(inv_freq_row()), norm_scale, slot_pos.T, x_in, w_q, w_k, w_v, w_o, k_cache, v_cache)])
        far = [lax.ppermute(own, 'kv', [(i, i ^ m) for i in range(8)]) for m in (2, 4, 6)]
        x_out = pl.pallas_call(
            out_kernel,
            out_shape=jax.ShapeDtypeStruct((BATCH, D_MODEL), BF16),
            in_specs=[vmem] * 7,
            out_specs=vmem,
            scratch_shapes=[
                pltpu.VMEM((4, BATCH // 8, QW), F32),
                pltpu.SemaphoreType.DMA,
                pltpu.SemaphoreType.DMA((4,)),
                pltpu.SemaphoreType.DMA((4,)),
            ],
            cost_estimate=pl.CostEstimate(flops=1_200_000_000, bytes_accessed=6_000_000, transcendentals=0),
            compiler_params=pltpu.CompilerParams(collective_id=1, has_side_effects=True, vmem_limit_bytes=18 * 1024 * 1024),
        )(own, *far, x_keep, wo_keep, b_o)
        return x_out, k_out, v_out, sp_t.T

    return jax.shard_map(
        local_step,
        mesh=mesh,
        in_specs=(row_spec, P('dp'), cache_spec, cache_spec, slot_spec, vec_spec, mat_spec, mat_spec, mat_spec, mat_spec, vec_spec),
        out_specs=(row_spec, cache_spec, cache_spec, slot_spec),
        check_vma=False)
```

```python
import functools

import jax
import jax.numpy as jnp
import numpy as np
from jax import lax
from jax.experimental import pallas as pl
from jax.experimental.pallas import tpu as pltpu
from jax.sharding import PartitionSpec as P

HEADS = 4
HEAD_DIM = 256
ROPE_DIM = 128
ROPE_HALF = ROPE_DIM // 2
ROPE_BASE = 10000.0
EPS = 1e-6
SCORE_SCALE = HEAD_DIM ** -0.5
NEG_LARGE = float(np.finfo(np.float32).min)
FAR = 1e9
F32 = jnp.float32
BF16 = jnp.bfloat16

BATCH = 512
D_MODEL = 1152
SLOTS = 64
QW = HEADS * HEAD_DIM
PW = QW + 128
GROUP = 8
HALF = 32
STEP = 64
CHUNK = 64
NCHUNK = BATCH // CHUNK
ROWS = 256


def sin_cos(theta):
    k = jnp.floor(theta * np.float32(2.0 / np.pi) + 0.5)
    r = theta - k * np.float32(1.5703125)
    r = r - k * np.float32(4.83751296997070312e-4)
    r = r - k * np.float32(7.54978995489188e-8)
    r2 = r * r
    s = r + r * r2 * (-1.6666654611e-1 + r2 * (8.3321608736e-3 + r2 * -1.9515295891e-4))
    c = 1.0 - 0.5 * r2 + r2 * r2 * (4.166664568298827e-2 + r2 * (-1.388731625493765e-3 + r2 * 2.443315711809948e-5))
    q = k - 4.0 * jnp.floor(k * 0.25)
    swap = (q == 1.0) | (q == 3.0)
    sin_v = jnp.where(swap, c, s)
    cos_v = jnp.where(swap, s, c)
    sin_v = jnp.where(q >= 2.0, -sin_v, sin_v)
    cos_v = jnp.where((q == 1.0) | (q == 2.0), -cos_v, cos_v)
    return sin_v, cos_v


def inv_freq_row():
    i = np.arange(ROPE_DIM) % ROPE_HALF
    return (ROPE_BASE ** (-i / ROPE_HALF)).astype(np.float32).reshape(1, ROPE_DIM)


def merge_rows(blocks):
    stats = [t[:, QW:] for t in blocks]
    lane = lax.broadcasted_iota(jnp.int32, stats[0].shape, 1)
    top = functools.reduce(jnp.maximum, stats)
    factors = [jnp.exp(t - top) for t in stats]
    sums = [t * pltpu.roll(f, HEADS, 1) for t, f in zip(stats, factors)]
    out = jnp.where(lane < HEADS, top, functools.reduce(jnp.add, sums))
    vals = []
    for h in range(HEADS):
        terms = [t[:, h * HEAD_DIM:(h + 1) * HEAD_DIM] * f[:, h:h + 1] for t, f in zip(blocks, factors)]
        vals.append(functools.reduce(jnp.add, terms))
    return jnp.concatenate(vals, axis=1), out


def normalise(v, s):
    inv = 1.0 / s
    return jnp.concatenate([v[:, h * HEAD_DIM:(h + 1) * HEAD_DIM] * inv[:, HEADS + h:HEADS + h + 1] for h in range(HEADS)], axis=1)


class Places:
    def __init__(self):
        me = lax.axis_index('kv')
        self.core = me % 2
        self.x = (me // 2) % 2
        self.y = me // 4
        self.mate = me + 1 - 2 * self.core

    def flip(self, m):
        x = self.x + (m % 2) * (1 - 2 * self.x)
        y = self.y + (m // 2) * (1 - 2 * self.y)
        return x, y

    def peer(self, m):
        x, y = self.flip(m)
        return y * 4 + x * 2 + self.core

    def eighth(self, m, core):
        x, y = self.flip(m)
        return 32 * core + 16 * x + 8 * y


def send(src, dst, ss, rs, peer):
    return pltpu.make_async_remote_copy(src_ref=src, dst_ref=dst, send_sem=ss, recv_sem=rs,
                                        device_id={'kv': peer}, device_id_type=pl.DeviceIdType.MESH)


def al(v, m=8):
    return pl.multiple_of(v, m)


class Reduce:
    def __init__(self, places, part, r0, r1, own, s0, s1):
        self.p = places
        self.part, self.r0, self.r1, self.own, self.s0, self.s1 = part, r0, r1, own, s0, s1

    def pair_copy(self, c):
        src = al(c * CHUNK + 32 * (1 - self.p.core))
        return send(self.part.at[pl.ds(src, 32)], self.r0.at[pl.ds(al(c * 32), 32)], self.s0.at[0, c], self.s0.at[1, c], self.p.mate)

    def chip_copies(self, c):
        return [send(self.part.at[pl.ds(al(c * CHUNK + self.p.eighth(m, self.p.core)), 8)],
                     self.r1.at[pl.ds(al((c // 2) * 48 + 16 * (m - 1) + 8 * (c % 2)), 8)],
                     self.s1.at[0, 3 * c + m - 1], self.s1.at[1, 3 * c + m - 1], self.p.peer(m)) for m in (3, 1, 2)]

    def pair_step(self, c):
        self.pair_copy(c).wait_recv()
        rows = pl.ds(al(c * CHUNK + 32 * self.p.core), 32)
        v, s = merge_rows([self.part[rows, :], self.r0[pl.ds(al(c * 32), 32), :]])
        self.part[rows, :] = jnp.concatenate([v, s], axis=1)
        for cp in self.chip_copies(c):
            cp.start()

    def chip_step(self, c):
        @pl.when(c % 2 == 1)
        def _():
            for cp in self.chip_copies(c - 1) + self.chip_copies(c):
                cp.wait_recv()
            mine = jnp.concatenate([self.part[pl.ds(al(k * CHUNK + self.p.eighth(0, self.p.core)), 8), :] for k in (c - 1, c)], axis=0)
            v, s = merge_rows([mine] + [self.r1[pl.ds(al((c // 2) * 48 + 16 * n), 16), :] for n in range(3)])
            self.own[pl.ds(al((c - 1) * 8), 16), :] = normalise(v, s)

    def drain(self, c):
        self.pair_copy(c).wait_send()
        for cp in self.chip_copies(c):
            cp.wait_send()


class Attention:
    def __init__(self, off, kbuf, vbuf, q_v, kn_v, vn_v, p_col, js_col, part):
        self.refs = kbuf, vbuf, q_v, kn_v, vn_v, p_col, js_col, part
        self.sub = lax.broadcasted_iota(jnp.int32, (GROUP, 128), 0)
        self.lane = lax.broadcasted_iota(jnp.int32, (GROUP, 128), 1)
        self.slot_c = jnp.where((self.lane // SLOTS) == (self.sub % 2), (self.lane % SLOTS).astype(F32) + off.astype(F32), FAR)
        self.pick = [(self.sub // 2) == cc for cc in range(4)]
        self.iotas = [(lax.broadcasted_iota(jnp.int32, (16, HEAD_DIM), 0) + 16 * t).astype(F32).astype(BF16) for t in range(SLOTS // 16)]

    def rows(self, base, count):
        kbuf, vbuf, q_v, kn_v, vn_v, p_col, js_col, part = self.refs
        pick, iotas, lane, slot_c = self.pick, self.iotas, self.lane, self.slot_c

        def hits_of(b):
            js = jnp.broadcast_to(js_col[pl.ds(b, 1), :], (16, 128)).astype(BF16)
            js = jnp.concatenate([js, js], axis=1)
            return [io == js for io in iotas]

        def refresh(buf, new_ref, r0):
            out = []
            for i in range(GROUP):
                b = r0 + i
                hits = hits_of(b)
                fresh = jnp.broadcast_to(new_ref[pl.ds(b, 1), :], (16, HEAD_DIM)).astype(BF16)
                for t in range(SLOTS // 16):
                    piece = jnp.where(hits[t], fresh, buf[b, pl.ds(16 * t, 16), :])
                    buf[b, pl.ds(16 * t, 16), :] = piece
                    out.append(piece)
            return jnp.concatenate(out, axis=0)

        def scores(r0):
            rows = pl.ds(r0, GROUP)
            q = jnp.concatenate([q_v[rows, h * HEAD_DIM:(h + 1) * HEAD_DIM] for h in range(HEADS)], axis=0).astype(BF16)
            s = lax.dot_general(q, refresh(kbuf, kn_v, r0), (((1,), (1,)), ((), ())), preferred_element_type=F32)
            out = []
            for h in range(HEADS):
                sh = s[h * GROUP:(h + 1) * GROUP, :]
                c = sh[:, 384:512]
                for cc in range(3):
                    c = jnp.where(pick[cc], sh[:, cc * 128:(cc + 1) * 128], c)
                out.append(c)
            return out

        def soften(r0, cs):
            valid = slot_c <= p_col[pl.ds(r0, GROUP), :]
            stats = jnp.zeros((GROUP, 128), F32)
            ps = []
            for h in range(HEADS):
                c = jnp.where(valid, cs[h], NEG_LARGE)
                m = jnp.max(c, axis=1, keepdims=True)
                e = jnp.where(valid, jnp.exp(c - m), 0.0)
                l = jnp.sum(e, axis=1, keepdims=True)
                stats = jnp.where(lane == h, m, stats)
                stats = jnp.where(lane == HEADS + h, l, stats)
                ps.append(e)
            part[pl.ds(r0, GROUP), QW:PW] = stats
            return ps

        def values(r0, ps):
            pm = jnp.concatenate([jnp.concatenate([jnp.where(pick[cc], e, 0.0) for cc in range(4)], axis=1) for e in ps], axis=0).astype(BF16)
            o = jnp.dot(pm, refresh(vbuf, vn_v, r0), preferred_element_type=F32)
            rows = pl.ds(r0, GROUP)
            for h in range(HEADS):
                part[rows, h * HEAD_DIM:(h + 1) * HEAD_DIM] = o[h * GROUP:(h + 1) * GROUP, :]

        starts = [al(base + g * GROUP, GROUP) for g in range(count // GROUP)]
        cs = [scores(r0) for r0 in starts]
        ps = [soften(r0, c) for r0, c in zip(starts, cs)]
        for r0, e in zip(starts, ps):
            values(r0, e)


def chunk_rows(c):
    return pl.ds(pl.multiple_of(c * CHUNK, CHUNK), CHUNK)


def step_kernel(pos_hbm, freq_hbm, ns_hbm, sp_hbm, x_hbm, wq_hbm, wk_hbm, wv_hbm, wo_hbm, k_hbm, v_hbm,
                own, kbuf, vbuf, sp_out, x_v, wo_v,
                wq_v, wk_v, wv_v, n_v, q_v, kn_v, vn_v, p_col, js_col, cos_v, sin_v,
                part, r0, r1, pos_row, freq_ref, ns_ref, w_sem, k_sem, v_sem, s0, s1):
    p = Places()
    barrier = pltpu.get_barrier_semaphore()
    for peer in (p.mate, p.peer(1), p.peer(2), p.peer(3)):
        pl.semaphore_signal(barrier, inc=1, device_id={'kv': peer}, device_id_type=pl.DeviceIdType.MESH)
    off = lax.axis_index('kv') * SLOTS
    weights = ((x_hbm, x_v), (wk_hbm, wk_v), (wv_hbm, wv_v), (wq_hbm, wq_v), (sp_hbm, sp_out),
               (pos_hbm, pos_row), (freq_hbm, freq_ref), (ns_hbm, ns_ref), (wo_hbm, wo_v))

    def w_in(n):
        return pltpu.make_async_copy(weights[n][0], weights[n][1], w_sem.at[n])

    def kv_in(c):
        return (pltpu.make_async_copy(k_hbm.at[chunk_rows(c)], kbuf.at[chunk_rows(c)], k_sem.at[c]),
                pltpu.make_async_copy(v_hbm.at[chunk_rows(c)], vbuf.at[chunk_rows(c)], v_sem.at[c]))

    for n in (5, 6, 7, 0, 1, 2, 3):
        w_in(n).start()
    for n in (5, 6, 7):
        w_in(n).wait()

    offf = off.astype(F32)

    @pl.loop(0, BATCH // 128)
    def _(t):
        rows = pl.ds(pl.multiple_of(t * 128, 128), 128)
        col = jnp.broadcast_to(pos_row[:, rows].astype(F32), (128, 128)).T
        p_col[rows, :] = col
        js = col - 512.0 * jnp.floor(col * (1.0 / 512.0)) - offf
        js_col[rows, :] = jnp.where((js >= 0.0) & (js < float(SLOTS)), js, -1.0)

    @pl.loop(0, BATCH // 64)
    def _(t):
        rows = pl.ds(pl.multiple_of(t * 64, 64), 64)
        s, c = sin_cos(p_col[rows, :] * freq_ref[...])
        lane = lax.broadcasted_iota(jnp.int32, (64, 128), 1)
        sin_v[rows, :] = jnp.where(lane < ROPE_HALF, -s, s)
        cos_v[rows, :] = c

    def rotate(t, rows):
        r = t[:, :ROPE_DIM]
        r = r * cos_v[rows, :] + pltpu.roll(r, ROPE_HALF, 1) * sin_v[rows, :]
        return jnp.concatenate([r, t[:, ROPE_DIM:]], axis=1)

    w_in(0).wait()
    for cp in kv_in(0) + kv_in(1):
        cp.start()
    gain = 1.0 + ns_ref[...].astype(F32).reshape(1, D_MODEL)

    @pl.loop(0, BATCH // 128)
    def _(i):
        rows = pl.ds(pl.multiple_of(i * 128, 128), 128)
        xf = x_v[rows, :].astype(F32)
        mean_sq = jnp.sum(xf * xf, axis=1, keepdims=True) * (1.0 / D_MODEL)
        n_v[rows, :] = (xf * lax.rsqrt(mean_sq + EPS) * gain).astype(BF16)

    for n in range(1, 4):
        w_in(n).wait()
    for c in range(2, NCHUNK):
        for cp in kv_in(c):
            cp.start()
    red = Reduce(p, part, r0, r1, own, s0, s1)
    att = Attention(off, kbuf, vbuf, q_v, kn_v, vn_v, p_col, js_col, part)

    def attend(c):
        @pl.when(c == NCHUNK - 1)
        def _():
            w_in(4).start()
            w_in(8).start()

        @pl.when(c % (ROWS // CHUNK) == 0)
        def _():
            rows = pl.ds(al(c * CHUNK, ROWS), ROWS)
            kn_v[rows, :] = rotate(jnp.dot(n_v[rows, :], wk_v[...], preferred_element_type=F32), rows)
            vn_v[rows, :] = jnp.dot(n_v[rows, :], wv_v[...], preferred_element_type=F32)
            for h in range(HEADS):
                cols = pl.ds(h * HEAD_DIM, HEAD_DIM)
                qh = jnp.dot(n_v[rows, :], wq_v[:, cols], preferred_element_type=F32)
                q_v[rows, cols] = rotate(qh, rows) * SCORE_SCALE

        for cp in kv_in(c):
            cp.wait()
        @pl.when(c < NCHUNK - 1)
        def _():
            att.rows(c * CHUNK, CHUNK)

        @pl.when(c == NCHUNK - 1)
        def _():
            att.rows(c * CHUNK + HALF * (1 - p.core), HALF)

        @pl.when(c == 0)
        def _():
            pl.semaphore_wait(barrier, 4)

        red.pair_copy(c).start()

        @pl.when(c == NCHUNK - 1)
        def _():
            att.rows(c * CHUNK + HALF * p.core, HALF)

    lags = ((0, attend), (1, red.pair_step), (6, red.chip_step))

    @pl.loop(0, NCHUNK + lags[-1][0])
    def _(i):
        for lag, body in lags:
            @pl.when((i >= lag) & (i < NCHUNK + lag))
            def _(lag=lag, body=body):
                body(i - lag)

    w_in(4).wait()
    w_in(8).wait()
    p_all = pos_row[...]
    slot_ids = off + lax.broadcasted_iota(jnp.int32, (SLOTS, BATCH), 0)
    sp_out[...] = jnp.where(slot_ids == (p_all & 511), p_all, sp_out[...])

    @pl.loop(0, NCHUNK)
    def _(c):
        red.drain(c)


def out_kernel(own, from_x, from_y, from_d, x_v, wo_v, b_ref, out_ref, g, lsem, ssem, rsem):
    p = Places()
    barrier = pltpu.get_barrier_semaphore()
    pl.semaphore_signal(barrier, inc=1, device_id={'kv': p.mate}, device_id_type=pl.DeviceIdType.MESH)
    refs = (own, from_x, from_y, from_d)

    def copy(n):
        return send(refs[n], g.at[n], ssem.at[n], rsem.at[n], p.mate)

    pl.semaphore_wait(barrier, 1)
    for n in range(4):
        copy(n).start()
    bias = b_ref[...].astype(F32).reshape(1, D_MODEL)

    def emit(blocks, chips, core):
        rows = [al(t * CHUNK + p.eighth(n, core)) for n in chips for t in range(NCHUNK)]
        o = jnp.concatenate([t[...].astype(BF16) for t in blocks], axis=0)
        xin = jnp.concatenate([x_v[pl.ds(r, 8), :].astype(F32) for r in rows], axis=0)
        y = xin + jnp.dot(o, wo_v[...], preferred_element_type=F32) + bias
        for t, r in enumerate(rows):
            out_ref[pl.ds(r, 8), :] = y[8 * t:8 * t + 8, :].astype(BF16)

    emit(refs, range(4), p.core)
    for first in (0, 2):
        pair = (first, first + 1)
        for n in pair:
            copy(n).wait_recv()
        emit([g.at[n] for n in pair], pair, 1 - p.core)
    for n in range(4):
        copy(n).wait_send()


def solution(mesh):
    row_spec = P('dp', None)
    cache_spec = P('dp', 'kv', None)
    slot_spec = P('dp', 'kv')
    vec_spec = P(None)
    mat_spec = P(None, None)
    hbm = pl.BlockSpec(memory_space=pltpu.HBM)
    vmem = pl.BlockSpec(memory_space=pltpu.VMEM)

    def in_hbm(a):
        return pltpu.with_memory_space_constraint(a, pltpu.HBM)

    def local_step(x_in, positions, k_cache, v_cache, slot_pos, norm_scale, w_q, w_k, w_v, w_o, b_o):
        own, k_out, v_out, sp_t, x_keep, wo_keep = pl.pallas_call(
            step_kernel,
            out_shape=(jax.ShapeDtypeStruct((BATCH // 8, QW), F32),
                       pltpu.VMEM((BATCH, SLOTS, HEAD_DIM), BF16),
                       pltpu.VMEM((BATCH, SLOTS, HEAD_DIM), BF16),
                       pltpu.VMEM((SLOTS, BATCH), jnp.int32),
                       pltpu.VMEM((BATCH, D_MODEL), BF16),
                       pltpu.VMEM((QW, D_MODEL), BF16)),
            in_specs=[hbm] * 11,
            out_specs=(vmem,) * 6,
            scratch_shapes=[
                pltpu.VMEM((D_MODEL, QW), BF16),
                pltpu.VMEM((D_MODEL, HEAD_DIM), BF16),
                pltpu.VMEM((D_MODEL, HEAD_DIM), BF16),
                pltpu.VMEM((BATCH, D_MODEL), BF16),
                pltpu.VMEM((BATCH, QW), F32),
                pltpu.VMEM((BATCH, HEAD_DIM), F32),
                pltpu.VMEM((BATCH, HEAD_DIM), F32),
                pltpu.VMEM((BATCH, 128), F32),
                pltpu.VMEM((BATCH, 128), F32),
                pltpu.VMEM((BATCH, 128), F32),
                pltpu.VMEM((BATCH, 128), F32),
                pltpu.VMEM((BATCH, PW), F32),
                pltpu.VMEM((NCHUNK * 32, PW), F32),
                pltpu.VMEM((NCHUNK * 24, PW), F32),
                pltpu.VMEM((1, BATCH), jnp.int32),
                pltpu.VMEM((1, ROPE_DIM), F32),
                pltpu.VMEM((D_MODEL,), BF16),
                pltpu.SemaphoreType.DMA((9,)),
                pltpu.SemaphoreType.DMA((NCHUNK,)),
                pltpu.SemaphoreType.DMA((NCHUNK,)),
                pltpu.SemaphoreType.DMA((2, NCHUNK)),
                pltpu.SemaphoreType.DMA((2, 3 * NCHUNK)),
            ],
            cost_estimate=pl.CostEstimate(flops=30_000_000_000, bytes_accessed=40_000_000, transcendentals=200_000),
            compiler_params=pltpu.CompilerParams(collective_id=0, has_side_effects=True, vmem_limit_bytes=18 * 1024 * 1024),
        )(*[in_hbm(a) for a in (positions.reshape(1, BATCH), jnp.asarray(inv_freq_row()), norm_scale, slot_pos.T, x_in, w_q, w_k, w_v, w_o, k_cache, v_cache)])
        far = [lax.ppermute(own, 'kv', [(i, i ^ m) for i in range(8)]) for m in (2, 4, 6)]
        x_out = pl.pallas_call(
            out_kernel,
            out_shape=jax.ShapeDtypeStruct((BATCH, D_MODEL), BF16),
            in_specs=[vmem] * 7,
            out_specs=vmem,
            scratch_shapes=[
                pltpu.VMEM((4, BATCH // 8, QW), F32),
                pltpu.SemaphoreType.DMA,
                pltpu.SemaphoreType.DMA((4,)),
                pltpu.SemaphoreType.DMA((4,)),
            ],
            cost_estimate=pl.CostEstimate(flops=1_200_000_000, bytes_accessed=6_000_000, transcendentals=0),
            compiler_params=pltpu.CompilerParams(collective_id=1, has_side_effects=True, vmem_limit_bytes=18 * 1024 * 1024),
        )(own, *far, x_keep, wo_keep, b_o)
        return x_out, k_out, v_out, sp_t.T

    return jax.shard_map(
        local_step,
        mesh=mesh,
        in_specs=(row_spec, P('dp'), cache_spec, cache_spec, slot_spec, vec_spec, mat_spec, mat_spec, mat_spec, mat_spec, vec_spec),
        out_specs=(row_spec, cache_spec, cache_spec, slot_spec),
        check_vma=False)
```

```python
import functools

import jax
import jax.numpy as jnp
import numpy as np
from jax import lax
from jax.experimental import pallas as pl
from jax.experimental.pallas import tpu as pltpu
from jax.sharding import PartitionSpec as P

HEADS = 4
HEAD_DIM = 256
ROPE_DIM = 128
ROPE_HALF = ROPE_DIM // 2
ROPE_BASE = 10000.0
EPS = 1e-6
SCORE_SCALE = HEAD_DIM ** -0.5
NEG_LARGE = float(np.finfo(np.float32).min)
FAR = 1e9
F32 = jnp.float32
BF16 = jnp.bfloat16

BATCH = 512
D_MODEL = 1152
SLOTS = 64
QW = HEADS * HEAD_DIM
PW = QW + 128
GROUP = 8
HALF = 32
STEP = 64
CHUNK = 64
NCHUNK = BATCH // CHUNK
ROWS = 256


def sin_cos(theta):
    k = jnp.floor(theta * np.float32(2.0 / np.pi) + 0.5)
    r = theta - k * np.float32(1.5703125)
    r = r - k * np.float32(4.83751296997070312e-4)
    r = r - k * np.float32(7.54978995489188e-8)
    r2 = r * r
    s = r + r * r2 * (-1.6666654611e-1 + r2 * (8.3321608736e-3 + r2 * -1.9515295891e-4))
    c = 1.0 - 0.5 * r2 + r2 * r2 * (4.166664568298827e-2 + r2 * (-1.388731625493765e-3 + r2 * 2.443315711809948e-5))
    q = k - 4.0 * jnp.floor(k * 0.25)
    swap = (q == 1.0) | (q == 3.0)
    sin_v = jnp.where(swap, c, s)
    cos_v = jnp.where(swap, s, c)
    sin_v = jnp.where(q >= 2.0, -sin_v, sin_v)
    cos_v = jnp.where((q == 1.0) | (q == 2.0), -cos_v, cos_v)
    return sin_v, cos_v


def inv_freq_row():
    i = np.arange(ROPE_DIM) % ROPE_HALF
    return (ROPE_BASE ** (-i / ROPE_HALF)).astype(np.float32).reshape(1, ROPE_DIM)


def merge_rows(blocks):
    stats = [t[:, QW:] for t in blocks]
    lane = lax.broadcasted_iota(jnp.int32, stats[0].shape, 1)
    top = functools.reduce(jnp.maximum, stats)
    factors = [jnp.exp(t - top) for t in stats]
    sums = [t * pltpu.roll(f, HEADS, 1) for t, f in zip(stats, factors)]
    out = jnp.where(lane < HEADS, top, functools.reduce(jnp.add, sums))
    vals = []
    for h in range(HEADS):
        terms = [t[:, h * HEAD_DIM:(h + 1) * HEAD_DIM] * f[:, h:h + 1] for t, f in zip(blocks, factors)]
        vals.append(functools.reduce(jnp.add, terms))
    return jnp.concatenate(vals, axis=1), out


def normalise(v, s):
    inv = 1.0 / s
    return jnp.concatenate([v[:, h * HEAD_DIM:(h + 1) * HEAD_DIM] * inv[:, HEADS + h:HEADS + h + 1] for h in range(HEADS)], axis=1)


class Places:
    def __init__(self):
        me = lax.axis_index('kv')
        self.core = me % 2
        self.x = (me // 2) % 2
        self.y = me // 4
        self.mate = me + 1 - 2 * self.core

    def flip(self, m):
        x = self.x + (m % 2) * (1 - 2 * self.x)
        y = self.y + (m // 2) * (1 - 2 * self.y)
        return x, y

    def peer(self, m):
        x, y = self.flip(m)
        return y * 4 + x * 2 + self.core

    def eighth(self, m, core):
        x, y = self.flip(m)
        return 32 * core + 16 * x + 8 * y


def send(src, dst, ss, rs, peer):
    return pltpu.make_async_remote_copy(src_ref=src, dst_ref=dst, send_sem=ss, recv_sem=rs,
                                        device_id={'kv': peer}, device_id_type=pl.DeviceIdType.MESH)


def al(v, m=8):
    return pl.multiple_of(v, m)


class Reduce:
    def __init__(self, places, part, r0, r1, own, s0, s1):
        self.p = places
        self.part, self.r0, self.r1, self.own, self.s0, self.s1 = part, r0, r1, own, s0, s1

    def pair_copy(self, c):
        src = al(c * CHUNK + 32 * (1 - self.p.core))
        return send(self.part.at[pl.ds(src, 32)], self.r0.at[pl.ds(al(c * 32), 32)], self.s0.at[0, c], self.s0.at[1, c], self.p.mate)

    def chip_copies(self, c):
        return [send(self.part.at[pl.ds(al(c * CHUNK + self.p.eighth(m, self.p.core)), 8)],
                     self.r1.at[pl.ds(al((c // 2) * 48 + 16 * (m - 1) + 8 * (c % 2)), 8)],
                     self.s1.at[0, 3 * c + m - 1], self.s1.at[1, 3 * c + m - 1], self.p.peer(m)) for m in (3, 1, 2)]

    def pair_step(self, c):
        self.pair_copy(c).wait_recv()
        rows = pl.ds(al(c * CHUNK + 32 * self.p.core), 32)
        v, s = merge_rows([self.part[rows, :], self.r0[pl.ds(al(c * 32), 32), :]])
        self.part[rows, :] = jnp.concatenate([v, s], axis=1)
        for cp in self.chip_copies(c):
            cp.start()

    def chip_step(self, c):
        @pl.when(c % 2 == 1)
        def _():
            for cp in self.chip_copies(c - 1) + self.chip_copies(c):
                cp.wait_recv()
            mine = jnp.concatenate([self.part[pl.ds(al(k * CHUNK + self.p.eighth(0, self.p.core)), 8), :] for k in (c - 1, c)], axis=0)
            v, s = merge_rows([mine] + [self.r1[pl.ds(al((c // 2) * 48 + 16 * n), 16), :] for n in range(3)])
            self.own[pl.ds(al((c - 1) * 8), 16), :] = normalise(v, s)

    def drain(self, c):
        self.pair_copy(c).wait_send()
        for cp in self.chip_copies(c):
            cp.wait_send()


class Attention:
    def __init__(self, off, kbuf, vbuf, q_v, kn_v, vn_v, p_col, js_col, part):
        self.refs = kbuf, vbuf, q_v, kn_v, vn_v, p_col, js_col, part
        self.sub = lax.broadcasted_iota(jnp.int32, (GROUP, 128), 0)
        self.lane = lax.broadcasted_iota(jnp.int32, (GROUP, 128), 1)
        self.slot_c = jnp.where((self.lane // SLOTS) == (self.sub % 2), (self.lane % SLOTS).astype(F32) + off.astype(F32), FAR)
        self.pick = [(self.sub // 2) == cc for cc in range(4)]
        self.iotas = [(lax.broadcasted_iota(jnp.int32, (16, HEAD_DIM), 0) + 16 * t).astype(F32).astype(BF16) for t in range(SLOTS // 16)]

    def rows(self, base, count):
        kbuf, vbuf, q_v, kn_v, vn_v, p_col, js_col, part = self.refs
        pick, iotas, lane, slot_c = self.pick, self.iotas, self.lane, self.slot_c

        def hits_of(b):
            js = jnp.broadcast_to(js_col[pl.ds(b, 1), :], (16, 128)).astype(BF16)
            js = jnp.concatenate([js, js], axis=1)
            return [io == js for io in iotas]

        def refresh(buf, new_ref, r0):
            out = []
            for i in range(GROUP):
                b = r0 + i
                hits = hits_of(b)
                fresh = jnp.broadcast_to(new_ref[pl.ds(b, 1), :], (16, HEAD_DIM)).astype(BF16)
                for t in range(SLOTS // 16):
                    piece = jnp.where(hits[t], fresh, buf[b, pl.ds(16 * t, 16), :])
                    buf[b, pl.ds(16 * t, 16), :] = piece
                    out.append(piece)
            return jnp.concatenate(out, axis=0)

        def scores(r0):
            rows = pl.ds(r0, GROUP)
            q = jnp.concatenate([q_v[rows, h * HEAD_DIM:(h + 1) * HEAD_DIM] for h in range(HEADS)], axis=0).astype(BF16)
            s = lax.dot_general(q, refresh(kbuf, kn_v, r0), (((1,), (1,)), ((), ())), preferred_element_type=F32)
            out = []
            for h in range(HEADS):
                sh = s[h * GROUP:(h + 1) * GROUP, :]
                c = sh[:, 384:512]
                for cc in range(3):
                    c = jnp.where(pick[cc], sh[:, cc * 128:(cc + 1) * 128], c)
                out.append(c)
            return out

        def soften(r0, cs):
            valid = slot_c <= p_col[pl.ds(r0, GROUP), :]
            stats = jnp.zeros((GROUP, 128), F32)
            ps = []
            for h in range(HEADS):
                c = jnp.where(valid, cs[h], NEG_LARGE)
                m = jnp.max(c, axis=1, keepdims=True)
                e = jnp.where(valid, jnp.exp(c - m), 0.0)
                l = jnp.sum(e, axis=1, keepdims=True)
                stats = jnp.where(lane == h, m, stats)
                stats = jnp.where(lane == HEADS + h, l, stats)
                ps.append(e)
            part[pl.ds(r0, GROUP), QW:PW] = stats
            return ps

        def values(r0, ps):
            pm = jnp.concatenate([jnp.concatenate([jnp.where(pick[cc], e, 0.0) for cc in range(4)], axis=1) for e in ps], axis=0).astype(BF16)
            o = jnp.dot(pm, refresh(vbuf, vn_v, r0), preferred_element_type=F32)
            rows = pl.ds(r0, GROUP)
            for h in range(HEADS):
                part[rows, h * HEAD_DIM:(h + 1) * HEAD_DIM] = o[h * GROUP:(h + 1) * GROUP, :]

        starts = [al(base + g * GROUP, GROUP) for g in range(count // GROUP)]
        cs = [scores(r0) for r0 in starts]
        ps = [soften(r0, c) for r0, c in zip(starts, cs)]
        for r0, e in zip(starts, ps):
            values(r0, e)


def chunk_rows(c):
    return pl.ds(pl.multiple_of(c * CHUNK, CHUNK), CHUNK)


def step_kernel(pos_hbm, freq_hbm, ns_hbm, sp_hbm, x_hbm, wq_hbm, wk_hbm, wv_hbm, wo_hbm, k_hbm, v_hbm,
                own, kbuf, vbuf, sp_out, x_v, wo_v,
                wq_v, wk_v, wv_v, n_v, q_v, kn_v, vn_v, p_col, js_col, cos_v, sin_v,
                part, r0, r1, pos_row, freq_ref, ns_ref, w_sem, k_sem, v_sem, s0, s1):
    p = Places()
    barrier = pltpu.get_barrier_semaphore()
    for peer in (p.mate, p.peer(1), p.peer(2), p.peer(3)):
        pl.semaphore_signal(barrier, inc=1, device_id={'kv': peer}, device_id_type=pl.DeviceIdType.MESH)
    off = lax.axis_index('kv') * SLOTS
    weights = ((x_hbm, x_v), (wk_hbm, wk_v), (wv_hbm, wv_v), (wq_hbm, wq_v), (sp_hbm, sp_out),
               (pos_hbm, pos_row), (freq_hbm, freq_ref), (ns_hbm, ns_ref), (wo_hbm, wo_v))

    def w_in(n):
        return pltpu.make_async_copy(weights[n][0], weights[n][1], w_sem.at[n])

    def kv_in(c):
        return (pltpu.make_async_copy(k_hbm.at[chunk_rows(c)], kbuf.at[chunk_rows(c)], k_sem.at[c]),
                pltpu.make_async_copy(v_hbm.at[chunk_rows(c)], vbuf.at[chunk_rows(c)], v_sem.at[c]))

    for n in (5, 6, 7, 0, 1, 2, 3):
        w_in(n).start()
    for n in (5, 6, 7):
        w_in(n).wait()

    offf = off.astype(F32)

    @pl.loop(0, BATCH // 128)
    def _(t):
        rows = pl.ds(pl.multiple_of(t * 128, 128), 128)
        col = jnp.broadcast_to(pos_row[:, rows].astype(F32), (128, 128)).T
        p_col[rows, :] = col
        js = col - 512.0 * jnp.floor(col * (1.0 / 512.0)) - offf
        js_col[rows, :] = jnp.where((js >= 0.0) & (js < float(SLOTS)), js, -1.0)

    @pl.loop(0, BATCH // 64)
    def _(t):
        rows = pl.ds(pl.multiple_of(t * 64, 64), 64)
        s, c = sin_cos(p_col[rows, :] * freq_ref[...])
        lane = lax.broadcasted_iota(jnp.int32, (64, 128), 1)
        sin_v[rows, :] = jnp.where(lane < ROPE_HALF, -s, s)
        cos_v[rows, :] = c

    def rotate(t, rows):
        r = t[:, :ROPE_DIM]
        r = r * cos_v[rows, :] + pltpu.roll(r, ROPE_HALF, 1) * sin_v[rows, :]
        return jnp.concatenate([r, t[:, ROPE_DIM:]], axis=1)

    w_in(0).wait()
    for cp in kv_in(0) + kv_in(1):
        cp.start()
    gain = 1.0 + ns_ref[...].astype(F32).reshape(1, D_MODEL)

    @pl.loop(0, BATCH // 128)
    def _(i):
        rows = pl.ds(pl.multiple_of(i * 128, 128), 128)
        xf = x_v[rows, :].astype(F32)
        mean_sq = jnp.sum(xf * xf, axis=1, keepdims=True) * (1.0 / D_MODEL)
        n_v[rows, :] = (xf * lax.rsqrt(mean_sq + EPS) * gain).astype(BF16)

    for n in range(1, 4):
        w_in(n).wait()
    for c in range(2, NCHUNK):
        for cp in kv_in(c):
            cp.start()
    red = Reduce(p, part, r0, r1, own, s0, s1)
    att = Attention(off, kbuf, vbuf, q_v, kn_v, vn_v, p_col, js_col, part)

    def attend(c):
        @pl.when(c % (ROWS // CHUNK) == 0)
        def _():
            rows = pl.ds(al(c * CHUNK, ROWS), ROWS)
            kn_v[rows, :] = rotate(jnp.dot(n_v[rows, :], wk_v[...], preferred_element_type=F32), rows)
            vn_v[rows, :] = jnp.dot(n_v[rows, :], wv_v[...], preferred_element_type=F32)
            for h in range(HEADS):
                cols = pl.ds(h * HEAD_DIM, HEAD_DIM)
                qh = jnp.dot(n_v[rows, :], wq_v[:, cols], preferred_element_type=F32)
                q_v[rows, cols] = rotate(qh, rows) * SCORE_SCALE

        for cp in kv_in(c):
            cp.wait()

        @pl.when(c == NCHUNK - 1)
        def _():
            w_in(4).start()
            w_in(8).start()
        @pl.when(c < NCHUNK - 1)
        def _():
            att.rows(c * CHUNK, CHUNK)

        @pl.when(c == NCHUNK - 1)
        def _():
            att.rows(c * CHUNK + HALF * (1 - p.core), HALF)

        @pl.when(c == 0)
        def _():
            pl.semaphore_wait(barrier, 4)

        red.pair_copy(c).start()

        @pl.when(c == NCHUNK - 1)
        def _():
            att.rows(c * CHUNK + HALF * p.core, HALF)

    lags = ((0, attend), (1, red.pair_step), (6, red.chip_step))

    @pl.loop(0, NCHUNK + lags[-1][0])
    def _(i):
        for lag, body in lags:
            @pl.when((i >= lag) & (i < NCHUNK + lag))
            def _(lag=lag, body=body):
                body(i - lag)

    w_in(4).wait()
    w_in(8).wait()
    p_all = pos_row[...]
    slot_ids = off + lax.broadcasted_iota(jnp.int32, (SLOTS, BATCH), 0)
    sp_out[...] = jnp.where(slot_ids == (p_all & 511), p_all, sp_out[...])

    @pl.loop(0, NCHUNK)
    def _(c):
        red.drain(c)


def out_kernel(own, from_x, from_y, from_d, x_v, wo_v, b_ref, out_ref, g, lsem, ssem, rsem):
    p = Places()
    barrier = pltpu.get_barrier_semaphore()
    pl.semaphore_signal(barrier, inc=1, device_id={'kv': p.mate}, device_id_type=pl.DeviceIdType.MESH)
    refs = (own, from_x, from_y, from_d)

    def copy(n):
        return send(refs[n], g.at[n], ssem.at[n], rsem.at[n], p.mate)

    pl.semaphore_wait(barrier, 1)
    for n in range(4):
        copy(n).start()
    bias = b_ref[...].astype(F32).reshape(1, D_MODEL)

    def emit(blocks, chips, core):
        rows = [al(t * CHUNK + p.eighth(n, core)) for n in chips for t in range(NCHUNK)]
        o = jnp.concatenate([t[...].astype(BF16) for t in blocks], axis=0)
        xin = jnp.concatenate([x_v[pl.ds(r, 8), :].astype(F32) for r in rows], axis=0)
        y = xin + jnp.dot(o, wo_v[...], preferred_element_type=F32) + bias
        for t, r in enumerate(rows):
            out_ref[pl.ds(r, 8), :] = y[8 * t:8 * t + 8, :].astype(BF16)

    emit(refs, range(4), p.core)
    for first in (0, 2):
        pair = (first, first + 1)
        for n in pair:
            copy(n).wait_recv()
        emit([g.at[n] for n in pair], pair, 1 - p.core)
    for n in range(4):
        copy(n).wait_send()


def solution(mesh):
    row_spec = P('dp', None)
    cache_spec = P('dp', 'kv', None)
    slot_spec = P('dp', 'kv')
    vec_spec = P(None)
    mat_spec = P(None, None)
    hbm = pl.BlockSpec(memory_space=pltpu.HBM)
    vmem = pl.BlockSpec(memory_space=pltpu.VMEM)

    def in_hbm(a):
        return pltpu.with_memory_space_constraint(a, pltpu.HBM)

    def local_step(x_in, positions, k_cache, v_cache, slot_pos, norm_scale, w_q, w_k, w_v, w_o, b_o):
        own, k_out, v_out, sp_t, x_keep, wo_keep = pl.pallas_call(
            step_kernel,
            out_shape=(jax.ShapeDtypeStruct((BATCH // 8, QW), F32),
                       pltpu.VMEM((BATCH, SLOTS, HEAD_DIM), BF16),
                       pltpu.VMEM((BATCH, SLOTS, HEAD_DIM), BF16),
                       pltpu.VMEM((SLOTS, BATCH), jnp.int32),
                       pltpu.VMEM((BATCH, D_MODEL), BF16),
                       pltpu.VMEM((QW, D_MODEL), BF16)),
            in_specs=[hbm] * 11,
            out_specs=(vmem,) * 6,
            scratch_shapes=[
                pltpu.VMEM((D_MODEL, QW), BF16),
                pltpu.VMEM((D_MODEL, HEAD_DIM), BF16),
                pltpu.VMEM((D_MODEL, HEAD_DIM), BF16),
                pltpu.VMEM((BATCH, D_MODEL), BF16),
                pltpu.VMEM((BATCH, QW), F32),
                pltpu.VMEM((BATCH, HEAD_DIM), F32),
                pltpu.VMEM((BATCH, HEAD_DIM), F32),
                pltpu.VMEM((BATCH, 128), F32),
                pltpu.VMEM((BATCH, 128), F32),
                pltpu.VMEM((BATCH, 128), F32),
                pltpu.VMEM((BATCH, 128), F32),
                pltpu.VMEM((BATCH, PW), F32),
                pltpu.VMEM((NCHUNK * 32, PW), F32),
                pltpu.VMEM((NCHUNK * 24, PW), F32),
                pltpu.VMEM((1, BATCH), jnp.int32),
                pltpu.VMEM((1, ROPE_DIM), F32),
                pltpu.VMEM((D_MODEL,), BF16),
                pltpu.SemaphoreType.DMA((9,)),
                pltpu.SemaphoreType.DMA((NCHUNK,)),
                pltpu.SemaphoreType.DMA((NCHUNK,)),
                pltpu.SemaphoreType.DMA((2, NCHUNK)),
                pltpu.SemaphoreType.DMA((2, 3 * NCHUNK)),
            ],
            cost_estimate=pl.CostEstimate(flops=30_000_000_000, bytes_accessed=40_000_000, transcendentals=200_000),
            compiler_params=pltpu.CompilerParams(collective_id=0, has_side_effects=True, vmem_limit_bytes=18 * 1024 * 1024),
        )(*[in_hbm(a) for a in (positions.reshape(1, BATCH), jnp.asarray(inv_freq_row()), norm_scale, slot_pos.T, x_in, w_q, w_k, w_v, w_o, k_cache, v_cache)])
        far = [lax.ppermute(own, 'kv', [(i, i ^ m) for i in range(8)]) for m in (2, 4, 6)]
        x_out = pl.pallas_call(
            out_kernel,
            out_shape=jax.ShapeDtypeStruct((BATCH, D_MODEL), BF16),
            in_specs=[vmem] * 7,
            out_specs=vmem,
            scratch_shapes=[
                pltpu.VMEM((4, BATCH // 8, QW), F32),
                pltpu.SemaphoreType.DMA,
                pltpu.SemaphoreType.DMA((4,)),
                pltpu.SemaphoreType.DMA((4,)),
            ],
            cost_estimate=pl.CostEstimate(flops=1_200_000_000, bytes_accessed=6_000_000, transcendentals=0),
            compiler_params=pltpu.CompilerParams(collective_id=1, has_side_effects=True, vmem_limit_bytes=18 * 1024 * 1024),
        )(own, *far, x_keep, wo_keep, b_o)
        return x_out, k_out, v_out, sp_t.T

    return jax.shard_map(
        local_step,
        mesh=mesh,
        in_specs=(row_spec, P('dp'), cache_spec, cache_spec, slot_spec, vec_spec, mat_spec, mat_spec, mat_spec, mat_spec, vec_spec),
        out_specs=(row_spec, cache_spec, cache_spec, slot_spec),
        check_vma=False)
```
